32 devices in a mesh: tp: 4 (over z), dp: 8 (over y, x, core).
Axes of the slice: x: 2, y: 2, z: 4, core: 2. Of those that a mesh axis runs over, the one named last changes fastest.
Arguments:
- tokens: int32 [32, 448], P('dp')
- labels: int32 [32, 448], P('dp')
- lossmask: int32 [32, 448], P('dp')
- hidden: bfloat16 [32, 448, 1280], P('dp')
- grad_x0: bfloat16 [32, 448, 1280], P('dp')
- embed_table: bfloat16 [51968, 1280], P('tp')
- pos_table: bfloat16 [448, 1280], replicated
- ln_gain: float32 [1280], replicated
- ln_bias: float32 [1280], replicated
Outputs:
- output 1: float32 [], replicated
- output 2: bfloat16 [32, 448, 1280], P('dp')
- output 3: bfloat16 [32, 448, 1280], P('dp')
- output 4: float32 [51968, 1280], P('tp')
- output 5: float32 [448, 1280], replicated
All inputs are finite; a program needn't handle non-finite values.
Results may differ from the reference program's by a relative error of at most 0.001.
Values sent between devices are 32-bit elements.
A program may use at most 1 GiB of HBM per device.

```python
import jax
import jax.numpy as jnp
import math
from jax import lax

BATCH_ALL = 32
TEXT_CTX = 448
D_MODEL = 1280
VOCAB_ROWS = 51968


def layer_norm(h_f32, ln_gain, ln_bias):
    mean_val = jnp.mean(h_f32, axis=-1, keepdims=True)
    centered = h_f32 - mean_val
    var_val = jnp.mean(centered * centered, axis=-1, keepdims=True)
    return centered * lax.rsqrt(var_val + 1e-5) * ln_gain + ln_bias


def setup_inputs(seed: int = 0) -> dict:
    rng_keys = jax.random.split(jax.random.key(seed), 9)
    pos_ids = jnp.arange(TEXT_CTX, dtype=jnp.int32)[None, :]
    tokens = jax.random.randint(rng_keys[0], (BATCH_ALL, TEXT_CTX), 0, VOCAB_ROWS, dtype=jnp.int32)
    tokens = tokens.at[0, 0].set(0).at[0, 1].set(VOCAB_ROWS - 1)
    labels = jax.random.randint(rng_keys[1], (BATCH_ALL, TEXT_CTX), 0, VOCAB_ROWS, dtype=jnp.int32)
    labels = labels.at[0, 0].set(VOCAB_ROWS - 1).at[0, 1].set(0)
    prompt_len = jax.random.randint(rng_keys[2], (BATCH_ALL, 1), 1, (3 * TEXT_CTX) // 4 + 1, dtype=jnp.int32)
    lossmask = (pos_ids >= prompt_len).astype(jnp.int32)
    row_scale = 1.5 / math.sqrt(D_MODEL)
    embed_table = (jax.random.normal(rng_keys[3], (VOCAB_ROWS, D_MODEL), jnp.float32) * row_scale).astype(jnp.bfloat16)
    pos_table = (jax.random.normal(rng_keys[4], (TEXT_CTX, D_MODEL), jnp.float32) * row_scale).astype(jnp.bfloat16)
    signal = (math.log(VOCAB_ROWS) + 1.5) / (1.5 * math.sqrt(D_MODEL))
    target_dir = jnp.take(embed_table, labels, axis=0).astype(jnp.float32) / row_scale
    noise = jax.random.normal(rng_keys[5], (BATCH_ALL, TEXT_CTX, D_MODEL), jnp.float32)
    hidden = (noise + signal * target_dir).astype(jnp.bfloat16)
    grad_x0 = (jax.random.normal(rng_keys[6], (BATCH_ALL, TEXT_CTX, D_MODEL), jnp.float32) / (BATCH_ALL * TEXT_CTX)).astype(jnp.bfloat16)
    ln_gain = 1.0 + 0.2 * jax.random.normal(rng_keys[7], (D_MODEL,), jnp.float32)
    ln_bias = 0.3 * jax.random.normal(rng_keys[8], (D_MODEL,), jnp.float32)
    return {'tokens': tokens, 'labels': labels, 'lossmask': lossmask, 'hidden': hidden, 'grad_x0': grad_x0, 'embed_table': embed_table, 'pos_table': pos_table, 'ln_gain': ln_gain, 'ln_bias': ln_bias}


def reference(tokens, labels, lossmask, hidden, grad_x0, embed_table, pos_table, ln_gain, ln_bias):
    embed_out = (jnp.take(embed_table, tokens, axis=0).astype(jnp.float32) + pos_table.astype(jnp.float32)[None]).astype(jnp.bfloat16)
    mask_f = lossmask.astype(jnp.float32)
    mask_count = jnp.sum(mask_f)
    vocab_ids = jnp.arange(VOCAB_ROWS, dtype=jnp.int32)

    def seq_step(carry, seq_in):
        embed_acc, loss_acc = carry
        tok_seq, lab_seq, mask_seq, hid_seq, dx_seq = seq_in
        z_f32, norm_vjp = jax.vjp(lambda h_in: layer_norm(h_in, ln_gain, ln_bias), hid_seq.astype(jnp.float32))
        z_bf16 = z_f32.astype(jnp.bfloat16)
        logits = jnp.dot(z_bf16, embed_table.T, preferred_element_type=jnp.float32)
        row_max = jnp.max(logits, axis=-1, keepdims=True)
        log_norm = row_max[:, 0] + jnp.log(jnp.sum(jnp.exp(logits - row_max), axis=-1))
        hit = vocab_ids[None, :] == lab_seq[:, None]
        lab_logit = jnp.sum(jnp.where(hit, logits, 0.0), axis=-1)
        tok_nll = log_norm - lab_logit
        prob_tok = jnp.exp(logits - log_norm[:, None])
        weight = mask_seq / mask_count
        g_bf16 = ((prob_tok - hit.astype(jnp.float32)) * weight[:, None]).astype(jnp.bfloat16)
        grad_z = jnp.dot(g_bf16, embed_table, preferred_element_type=jnp.float32)
        grad_h = norm_vjp(grad_z)[0].astype(jnp.bfloat16)
        embed_acc = embed_acc + jnp.dot(g_bf16.T, z_bf16, preferred_element_type=jnp.float32) + jax.ops.segment_sum(dx_seq.astype(jnp.float32), tok_seq, num_segments=VOCAB_ROWS)
        loss_acc = loss_acc + jnp.sum(mask_seq * tok_nll)
        return (embed_acc, loss_acc), grad_h

    init = (jnp.zeros((VOCAB_ROWS, D_MODEL), jnp.float32), jnp.zeros((), jnp.float32))
    (grad_embed, loss_sum), grad_hidden = lax.scan(seq_step, init, (tokens, labels, mask_f, hidden, grad_x0))
    mean_loss = loss_sum / mask_count
    grad_pos = jnp.sum(grad_x0.astype(jnp.float32), axis=0)
    return (mean_loss, embed_out, grad_hidden, grad_embed, grad_pos)
```

```python
import functools

import jax
import jax.numpy as jnp
from jax import lax
from jax.experimental import pallas as pl
from jax.experimental.pallas import tpu as pltpu
from jax.sharding import PartitionSpec as P

MESH = pl.DeviceIdType.MESH
F32 = jnp.float32
BF16 = jnp.bfloat16
NT = (((1,), (1,)), ((), ()))
TN = (((0,), (0,)), ((), ()))
RING = 4
SLOTS = 8
VMEM_LIMIT = 66_000_000


def sizes(tokens, vocab_loc):
    if vocab_loc % 448 == 0 and tokens % 1792 == 0:
        return 448, 256, 56
    return 64, 128, 8


def stats_kernel(chunk, tile, hidden, gain, bias, lab, embed, zb, stats, m_ref, s_ref, l_ref):
    step = pl.program_id(0)
    tokens = hidden.shape[0]
    tiles = tokens // tile

    @pl.when(step == 0)
    def _():
        def norm(j, carry):
            rows = pl.ds(pl.multiple_of(j * tile, tile), tile)
            h = hidden[rows, :].astype(F32)
            centered = h - jnp.mean(h, axis=-1, keepdims=True)
            var = jnp.mean(centered * centered, axis=-1, keepdims=True)
            zb[rows, :] = (centered * lax.rsqrt(var + 1e-5) * gain[...] + bias[...]).astype(BF16)
            return carry
        lax.fori_loop(0, tiles, norm, 0)
        m_ref[...] = jnp.full_like(m_ref, -jnp.inf)
        s_ref[...] = jnp.zeros_like(s_ref)
        l_ref[...] = jnp.zeros_like(l_ref)

    e = embed[...]
    ids = lax.broadcasted_iota(jnp.int32, (chunk, tile), 0) + step * chunk
    for j in range(tiles):
        cols = slice(j * tile, (j + 1) * tile)
        logits = lax.dot_general(e, zb[cols, :], NT, preferred_element_type=F32)
        m_old = m_ref[:, cols]
        m_new = jnp.maximum(m_old, jnp.max(logits, axis=0, keepdims=True))
        m_ref[:, cols] = m_new
        s_ref[:, cols] = s_ref[:, cols] * jnp.exp(m_old - m_new) + jnp.sum(jnp.exp(logits - m_new), axis=0, keepdims=True)
        l_ref[:, cols] += jnp.sum(jnp.where(ids == lab[:, cols], logits, 0.0), axis=0, keepdims=True)

    @pl.when(step == pl.num_programs(0) - 1)
    def _():
        stats[0:1, :] = m_ref[...] + jnp.log(s_ref[...])
        stats[1:2, :] = l_ref[...]


def token_stats(hidden, gain, bias, lab, embed, chunk, tile):
    tokens, d = hidden.shape
    steps = embed.shape[0] // chunk
    whole = lambda shape: pl.BlockSpec(shape, lambda i: (0, 0))
    return pl.pallas_call(
        functools.partial(stats_kernel, chunk, tile),
        grid=(steps,),
        out_shape=(jax.ShapeDtypeStruct((tokens, d), BF16), jax.ShapeDtypeStruct((2, tokens), F32)),
        in_specs=[whole((tokens, d)), whole((1, d)), whole((1, d)), whole((1, tokens)),
                  pl.BlockSpec((chunk, d), lambda i: (i, 0))],
        out_specs=(whole((tokens, d)), whole((2, tokens))),
        scratch_shapes=[pltpu.VMEM((1, tokens), F32)] * 3,
        compiler_params=pltpu.CompilerParams(vmem_limit_bytes=VMEM_LIMIT),
        cost_estimate=pl.CostEstimate(flops=2 * tokens * d * embed.shape[0], bytes_accessed=2 * embed.size,
                                      transcendentals=tokens * embed.shape[0]),
        name='token_stats',
    )(hidden, gain, bias, lab, embed)


def grad_kernel(ntp, chunk, tile, zrows,
                zb, dx, lse, wgt, lab, tok, embed,
                out, gz, own, d2d, rs_r, rs_l,
                ebuf, gt, oh, acc, gbuf, ld_own, ld_d2d, s1, s2, fin, rs1, rs2, zin_r, zin_l, zout_r, zout_l, zfin,
                e_sem, own_sem, d2d_s, d2d_r, ld_sem, rs1_s, rs1_r, rs2_s, rs2_r, fin_s, ag1_r, ag2_r, fwd_s, part_r,
                zld, zrs_sr, zrs_sl, zrs_rr, zrs_rl, zfin_s, zag_rr, zag_rl, zfw_r, zfw_l):
    tokens, d = zb.shape
    vocab_loc = embed.shape[0]
    nc = vocab_loc // chunk
    tiles = tokens // tile
    ntile = 256 if d % 256 == 0 and d > 256 else 128
    half, quarter, eighth = chunk // 2, chunk // 4, chunk // 8
    dp, z = lax.axis_index('dp'), lax.axis_index('tp')
    core = lax.rem(dp, 2)
    xpos = lax.rem(lax.div(dp, 2), 2)
    ypos = lax.div(dp, 4)
    partner = dp + 1 - 2 * core
    x_nbr = dp + 2 - 4 * xpos
    y_nbr = dp + 4 - 8 * ypos

    def place(k):
        odd = lax.rem(k, 2)
        n1 = x_nbr + (y_nbr - x_nbr) * odd
        n2 = y_nbr + (x_nbr - y_nbr) * odd
        a1 = xpos + (ypos - xpos) * odd
        a2 = ypos + (xpos - ypos) * odd
        return n1, n2, a1, a2

    def rdma(src, dst, ssem, rsem, dev):
        return pltpu.make_async_remote_copy(src_ref=src, dst_ref=dst, send_sem=ssem, recv_sem=rsem,
                                            device_id={'dp': dev}, device_id_type=MESH)

    def zdma(src, dst, ssem, rsem, dev):
        return pltpu.make_async_remote_copy(src_ref=src, dst_ref=dst, send_sem=ssem, recv_sem=rsem,
                                            device_id={'tp': dev}, device_id_type=MESH)

    def rows8(start, n):
        return pl.ds(pl.multiple_of(start, 8), n)

    def valid(k, limit=None):
        return (k >= 0) & (k < (nc if limit is None else limit))

    def e_copy(k):
        return pltpu.make_async_copy(embed.at[rows8(k * chunk, chunk)], ebuf.at[lax.rem(k, 2)], e_sem.at[lax.rem(k, 2)])

    def own_copy(k):
        b = lax.rem(k, 2)
        return pltpu.make_async_copy(gbuf.at[b, rows8(core * half, half)], own.at[k], own_sem.at[b])

    def d2d_copy(k):
        b = lax.rem(k, 2)
        return rdma(gbuf.at[b, rows8((1 - core) * half, half)], d2d.at[k], d2d_s.at[b], d2d_r.at[k], partner)

    def rs1_copy(k):
        n1, _, a1, _ = place(k)
        b, r = lax.rem(k, RING), lax.rem(k, SLOTS)
        return rdma(s1.at[b, rows8((1 - a1) * quarter, quarter)], rs1.at[r], rs1_s.at[b], rs1_r.at[r], n1)

    def rs2_copy(k):
        _, n2, _, a2 = place(k)
        b, r = lax.rem(k, RING), lax.rem(k, SLOTS)
        return rdma(s2.at[b, rows8((1 - a2) * eighth, eighth)], rs2.at[r], rs2_s.at[b], rs2_r.at[r], n2)

    def fin_copies(k):
        n1, n2, a1, a2 = place(k)
        b = lax.rem(k, RING)
        dst = out.at[rows8(k * chunk + core * half + a1 * quarter + a2 * eighth, eighth)]
        src = fin.at[b]
        return (pltpu.make_async_copy(src, dst, fin_s.at[0, b]),
                rdma(src, dst, fin_s.at[1, b], ag1_r.at[k], n2),
                rdma(src, dst, fin_s.at[2, b], ag2_r.at[0, k], n1),
                rdma(src, dst, fin_s.at[3, b], part_r.at[0, k], partner))

    def fwd_copies(k):
        n1, _, a1, a2 = place(k)
        b = lax.rem(k, RING)
        ref = out.at[rows8(k * chunk + core * half + a1 * quarter + (1 - a2) * eighth, eighth)]
        return (rdma(ref, ref, fwd_s.at[0, b], ag2_r.at[1, k], n1),
                rdma(ref, ref, fwd_s.at[1, b], part_r.at[1, k], partner))

    def last_copy(k):
        _, _, a1, _ = place(k)
        ref = out.at[rows8(k * chunk + core * half + (1 - a1) * quarter, quarter)]
        return rdma(ref, ref, fwd_s.at[2, lax.rem(k, RING)], part_r.at[2, k], partner)

    def compute(k, carry):
        slot = lax.rem(k, 2)
        e_copy(k).wait()

        @pl.when(k + 1 < nc)
        def _():
            e_copy(k + 1).start()

        ids = lax.broadcasted_iota(jnp.int32, (chunk, tile), 0) + k * chunk

        def per_tile(j, c):
            cols = pl.ds(pl.multiple_of(j * tile, tile), tile)
            e = ebuf[slot]
            logits = lax.dot_general(e, zb[cols, :], NT, preferred_element_type=F32)
            hit = jnp.where(ids == lab[j], 1.0, 0.0)
            g = ((jnp.exp(logits - lse[j]) - hit) * wgt[j]).astype(BF16)
            gt[:, cols] = g
            oh[:, cols] = jnp.where(ids == tok[j], 1.0, 0.0).astype(BF16)
            acc[cols, :] += lax.dot_general(g, e, TN, preferred_element_type=F32)
            return c
        lax.fori_loop(0, tiles, per_tile, 0)

        @pl.when(k >= 1)
        def _():
            own_copy(k - 1).wait()
            d2d_copy(k - 1).wait_send()

        def per_cols(n, c):
            cols = pl.ds(pl.multiple_of(n * ntile, ntile), ntile)
            gbuf[slot, :, cols] = (jnp.dot(gt[...], zb[:, cols], preferred_element_type=F32)
                                   + jnp.dot(oh[...], dx[:, cols], preferred_element_type=F32))
            return c
        lax.fori_loop(0, d // ntile, per_cols, 0)
        own_copy(k).start()
        d2d_copy(k).start()

        @pl.when(k == nc - 1)
        def _():
            own_copy(k).wait()
            d2d_copy(k).wait_send()
        return carry

    def load_start(k):
        d2d_copy(k).wait_recv()
        pltpu.make_async_copy(own.at[k], ld_own, ld_sem.at[0]).start()
        pltpu.make_async_copy(d2d.at[k], ld_d2d, ld_sem.at[1]).start()

    def stage_a(k):
        pltpu.make_async_copy(own.at[k], ld_own, ld_sem.at[0]).wait()
        pltpu.make_async_copy(d2d.at[k], ld_d2d, ld_sem.at[1]).wait()

        @pl.when(k >= RING)
        def _():
            rs1_copy(k - RING).wait_send()
        b = lax.rem(k, RING)

        def add(i, c):
            r = rows8(i * eighth, eighth)
            s1[b, r, :] = ld_own[r, :] + ld_d2d[r, :]
            return c
        lax.fori_loop(0, half // eighth, add, 0)
        rs1_copy(k).start()

    def stage_b(k):
        _, _, a1, _ = place(k)
        rs1_copy(k).wait_recv()

        @pl.when(k >= RING)
        def _():
            rs2_copy(k - RING).wait_send()
        b, r = lax.rem(k, RING), lax.rem(k, SLOTS)

        def add(i, c):
            s2[b, rows8(i * eighth, eighth), :] = (s1[b, rows8(a1 * quarter + i * eighth, eighth), :]
                                                   + rs1[r, rows8(i * eighth, eighth), :])
            return c
        lax.fori_loop(0, quarter // eighth, add, 0)
        rs2_copy(k).start()

    def stage_c(k):
        _, _, _, a2 = place(k)
        rs2_copy(k).wait_recv()

        @pl.when(k >= RING)
        def _():
            for i, c in enumerate(fin_copies(k - RING)):
                c.wait() if i == 0 else c.wait_send()
        b, r = lax.rem(k, RING), lax.rem(k, SLOTS)
        fin[b] = s2[b, rows8(a2 * eighth, eighth), :] + rs2[r]
        for c in fin_copies(k):
            c.start()

    def stage_d(k):
        fin_copies(k)[1].wait_recv()

        @pl.when(k >= RING)
        def _():
            for c in fwd_copies(k - RING):
                c.wait_send()
        for c in fwd_copies(k):
            c.start()

    def stage_e(k):
        fin_copies(k)[2].wait_recv()
        fwd_copies(k)[0].wait_recv()

        @pl.when(k >= RING)
        def _():
            last_copy(k - RING).wait_send()
        last_copy(k).start()

    def stage_f(k):
        fin_copies(k)[3].wait_recv()
        fwd_copies(k)[1].wait_recv()
        last_copy(k).wait_recv()

    nb = tokens // ntp // zrows
    qrows = tokens // ntp

    def zacc(q, b):
        return pl.multiple_of(q * qrows + b * zrows, 8)

    def right_copy(b, i, src=None):
        n = ntp - 1 - i
        s = zout_r.at[lax.rem(b, 2), pl.ds(i, n)] if src is None else src
        return zdma(s, rs_r.at[b, pl.ds(i, n)], zrs_sr.at[lax.rem(b, 2)], zrs_rr.at[b], i + 1)

    def left_copy(b, i):
        return zdma(zout_l.at[lax.rem(b, 2), pl.ds(0, i)], rs_l.at[b, pl.ds(0, i)], zrs_sl.at[lax.rem(b, 2)],
                    zrs_rl.at[b], i - 1)

    def z_right(b):
        for i in range(ntp - 1):
            @pl.when(z == i)
            def _(i=i):
                n = ntp - 1 - i
                if i > 0:
                    right_copy(b, i - 1).wait_recv()
                    load = pltpu.make_async_copy(rs_r.at[b, pl.ds(i, n)], zin_r.at[pl.ds(i, n)], zld.at[0])
                    load.start()
                    load.wait()

                @pl.when(b >= 2)
                def _():
                    right_copy(b - 2, i).wait_send()
                for q in range(i + 1, ntp):
                    mine = acc[pl.ds(zacc(q, b), zrows), :]
                    zout_r[lax.rem(b, 2), q - 1] = mine if i == 0 else zin_r[q - 1] + mine
                right_copy(b, i).start()

    def z_left(b):
        for i in range(1, ntp):
            @pl.when(z == i)
            def _(i=i):
                if i < ntp - 1:
                    left_copy(b, i + 1).wait_recv()
                    load = pltpu.make_async_copy(rs_l.at[b, pl.ds(0, i)], zin_l.at[pl.ds(0, i)], zld.at[0])
                    load.start()
                    load.wait()

                @pl.when(b >= 2)
                def _():
                    left_copy(b - 2, i).wait_send()
                for q in range(i):
                    mine = acc[pl.ds(zacc(q, b), zrows), :]
                    zout_l[lax.rem(b, 2), q] = mine if i == ntp - 1 else zin_l[q] + mine
                left_copy(b, i).start()

    def zfin_copies(b):
        s = lax.rem(b, 2)
        dst = gz.at[rows8(z * qrows + b * zrows, zrows)]
        return (pltpu.make_async_copy(zfin.at[s], dst, zfin_s.at[0, s]),
                zdma(zfin.at[s], dst, zfin_s.at[1, s], zag_rr.at[b, 0], z + 1),
                zdma(zfin.at[s], dst, zfin_s.at[2, s], zag_rl.at[b, 0], z - 1))

    def z_final(b):
        for i in range(ntp):
            @pl.when(z == i)
            def _(i=i):
                if i > 0:
                    right_copy(b, i - 1).wait_recv() if i == ntp - 1 else None
                    load = pltpu.make_async_copy(rs_r.at[b, i - 1], zin_r.at[i - 1], zld.at[0])
                    load.start()
                    load.wait()
                if i < ntp - 1:
                    left_copy(b, i + 1).wait_recv() if i == 0 else None
                    load = pltpu.make_async_copy(rs_l.at[b, i], zin_l.at[i], zld.at[0])
                    load.start()
                    load.wait()
                z_wait_fin(b - 2, b >= 2)
                total = acc[pl.ds(zacc(i, b), zrows), :]
                if i > 0:
                    total = zin_r[i - 1] + total
                if i < ntp - 1:
                    total = total + zin_l[i]
                zfin[lax.rem(b, 2)] = total
        copies = zfin_copies(b)
        copies[0].start()

        @pl.when(z < ntp - 1)
        def _():
            copies[1].start()

        @pl.when(z > 0)
        def _():
            copies[2].start()

    def z_wait_fin(b, cond):
        @pl.when(cond)
        def _():
            copies = zfin_copies(b)
            copies[0].wait()

            @pl.when(z < ntp - 1)
            def _():
                copies[1].wait_send()

            @pl.when(z > 0)
            def _():
                copies[2].wait_send()

    def zag(b, h, sign, ssem, rsem):
        ref = gz.at[rows8((z - sign * h) * qrows + b * zrows, zrows)]
        return zdma(ref, ref, ssem.at[b, h - 1], rsem.at[b, h], z + sign)

    def z_hop(b, h):
        ref_r = gz.at[rows8((z - h) * qrows + b * zrows, zrows)]
        ref_l = gz.at[rows8((z + h) * qrows + b * zrows, zrows)]

        @pl.when(z >= h)
        def _():
            zdma(ref_r, ref_r, zfw_r.at[b, 0], zag_rr.at[b, h - 1], z).wait_recv()
            if h < ntp - 1:
                @pl.when(z < ntp - 1)
                def _():
                    zag(b, h, 1, zfw_r, zag_rr).start()

        @pl.when(z + h <= ntp - 1)
        def _():
            zdma(ref_l, ref_l, zfw_l.at[b, 0], zag_rl.at[b, h - 1], z).wait_recv()
            if h < ntp - 1:
                @pl.when(z > 0)
                def _():
                    zag(b, h, -1, zfw_l, zag_rl).start()

    lead = min(8, nc)

    def cs(t):
        late = t - lead
        c = lead + lax.div(late * 3, 2)
        return jnp.minimum(jnp.where(t <= lead, t, c), nc)

    z_start = lead + -(-(nc - lead) * 2 // 3)
    ticks = max(nc + 13, z_start + nb + 2 * ntp)
    acc[...] = jnp.zeros_like(acc)
    e_copy(0).start()

    def tick(t, carry):
        ka = t - 2

        @pl.when(valid(ka))
        def _():
            load_start(ka)
        lax.fori_loop(cs(t), cs(t + 1), compute, 0)
        for stage, lag in ((stage_e, 10), (stage_d, 8), (stage_c, 6), (stage_b, 4), (stage_a, 2), (stage_f, 12)):
            @pl.when(valid(t - lag))
            def _(stage=stage, lag=lag):
                stage(t - lag)
        zt = t - z_start

        @pl.when(valid(zt - z, nb))
        def _():
            z_right(zt - z)

        @pl.when(valid(zt - (ntp - 1 - z), nb))
        def _():
            z_left(zt - (ntp - 1 - z))

        @pl.when(valid(zt - (ntp - 1), nb))
        def _():
            z_final(zt - (ntp - 1))
        for h in range(1, ntp):
            @pl.when(valid(zt - (ntp - 1) - h, nb))
            def _(h=h):
                z_hop(zt - (ntp - 1) - h, h)
        return carry
    lax.fori_loop(0, ticks, tick, 0)

    for k in range(max(nc - RING, 0), nc):
        rs1_copy(k).wait_send()
        rs2_copy(k).wait_send()
        for i, c in enumerate(fin_copies(k)):
            c.wait() if i == 0 else c.wait_send()
        for c in fwd_copies(k):
            c.wait_send()
        last_copy(k).wait_send()
    for b in range(max(nb - 2, 0), nb):
        for i in range(ntp - 1):
            @pl.when(z == i)
            def _(i=i, b=b):
                right_copy(b, i).wait_send()
        for i in range(1, ntp):
            @pl.when(z == i)
            def _(i=i, b=b):
                left_copy(b, i).wait_send()
        z_wait_fin(b, z >= 0)

    def drain(b, carry):
        for h in range(1, ntp - 1):
            @pl.when((z >= h) & (z < ntp - 1))
            def _(h=h):
                zag(b, h, 1, zfw_r, zag_rr).wait_send()

            @pl.when((z + h <= ntp - 1) & (z > 0))
            def _(h=h):
                zag(b, h, -1, zfw_l, zag_rl).wait_send()
        return carry
    lax.fori_loop(0, nb, drain, 0)


def gradients(ntp, zb, dx, lse, wgt, lab, tok, embed, chunk, tile, zrows):
    tokens, d = zb.shape
    vocab_loc = embed.shape[0]
    nc = vocab_loc // chunk
    half, quarter, eighth = chunk // 2, chunk // 4, chunk // 8
    nb = tokens // ntp // zrows
    vm = pl.BlockSpec(memory_space=pltpu.VMEM)
    hbm = pl.BlockSpec(memory_space=pl.ANY)
    dma = lambda *s: pltpu.SemaphoreType.DMA(s)
    vf = lambda *s: pltpu.VMEM(s, F32)
    sds = lambda *s: jax.ShapeDtypeStruct(s, F32)
    flops = 2 * tokens * d * vocab_loc
    rows = lambda a: a.reshape(tokens // tile, 1, tile)
    res = pl.pallas_call(
        functools.partial(grad_kernel, ntp, chunk, tile, zrows),
        out_shape=(sds(vocab_loc, d), sds(tokens, d), sds(nc, half, d), sds(nc, half, d),
                   sds(nb, ntp - 1, zrows, d), sds(nb, ntp - 1, zrows, d)),
        in_specs=[vm] * 6 + [hbm],
        out_specs=(hbm,) * 6,
        scratch_shapes=[
            pltpu.VMEM((2, chunk, d), BF16), pltpu.VMEM((chunk, tokens), BF16), pltpu.VMEM((chunk, tokens), BF16),
            vf(tokens, d), vf(2, chunk, d), vf(half, d), vf(half, d),
            vf(RING, half, d), vf(RING, quarter, d), vf(RING, eighth, d), vf(SLOTS, quarter, d), vf(SLOTS, eighth, d),
            vf(ntp - 1, zrows, d), vf(ntp - 1, zrows, d), vf(2, ntp - 1, zrows, d), vf(2, ntp - 1, zrows, d),
            vf(2, zrows, d),
            dma(2), dma(2), dma(2), dma(nc), dma(2), dma(RING), dma(SLOTS), dma(RING), dma(SLOTS), dma(4, RING),
            dma(nc), dma(2, nc), dma(3, RING), dma(3, nc),
            dma(1), dma(2), dma(2), dma(nb), dma(nb), dma(3, 2), dma(nb, ntp - 1), dma(nb, ntp - 1),
            dma(nb, ntp - 1), dma(nb, ntp - 1),
        ],
        compiler_params=pltpu.CompilerParams(vmem_limit_bytes=VMEM_LIMIT, has_side_effects=True),
        cost_estimate=pl.CostEstimate(flops=4 * flops, bytes_accessed=4 * vocab_loc * d * 4,
                                      transcendentals=tokens * vocab_loc),
        name='gradients',
    )(zb, dx, rows(lse), rows(wgt), rows(lab), rows(tok), embed)
    return res[0], res[1]


def layer_norm(h_f32, ln_gain, ln_bias):
    mean_val = jnp.mean(h_f32, axis=-1, keepdims=True)
    centered = h_f32 - mean_val
    var_val = jnp.mean(centered * centered, axis=-1, keepdims=True)
    return centered * lax.rsqrt(var_val + 1e-5) * ln_gain + ln_bias


def solution(mesh):
    ntp, ndp = mesh.shape['tp'], mesh.shape['dp']

    def device_fn(tokens, labels, lossmask, hidden, grad_x0, embed_loc, pos_table, ln_gain, ln_bias):
        vocab_loc, d = embed_loc.shape
        batch, ctx = tokens.shape
        ntok = batch * ctx
        chunk, tile, zrows = sizes(ntok, vocab_loc)
        shard_start = lax.axis_index('tp') * vocab_loc
        tok_local = tokens - shard_start
        tok_here = (tok_local >= 0) & (tok_local < vocab_loc)
        rows = jnp.take(embed_loc, jnp.where(tok_here, tok_local, 0), axis=0)
        rows = jnp.where(tok_here[..., None], rows.astype(F32), 0.0)
        rows = lax.psum(rows, 'tp')
        embed_out = (rows + pos_table.astype(F32)[None]).astype(BF16)
        grad_pos = lax.psum(jnp.sum(grad_x0.astype(F32), axis=0), 'dp')

        lab_local = (labels - shard_start).reshape(1, ntok)
        hidden2 = hidden.reshape(ntok, d)
        zb, stats = token_stats(hidden2, ln_gain.reshape(1, d), ln_bias.reshape(1, d), lab_local, embed_loc, chunk, tile)
        mask_f = lossmask.astype(F32).reshape(1, ntok)
        every = lax.all_gather(jnp.concatenate([stats, mask_f]), ('tp', 'dp'))
        every = every.reshape(ntp, ndp, 3, ntok)
        top = jnp.max(every[:, :, 0], axis=0)
        lse_all = top + jnp.log(jnp.sum(jnp.exp(every[:, :, 0] - top), axis=0))
        lab_all = jnp.sum(every[:, :, 1], axis=0)
        mask_all = every[0, :, 2]
        count = jnp.sum(mask_all)
        mean_loss = jnp.sum(mask_all * (lse_all - lab_all)) / count
        lse = lax.dynamic_index_in_dim(lse_all, lax.axis_index('dp'), 0, keepdims=True)
        wgt = mask_f / count

        grad_embed, grad_z = gradients(ntp, zb, grad_x0.reshape(ntok, d), lse, wgt, lab_local, tok_local.reshape(1, ntok),
                                       embed_loc, chunk, tile, zrows)
        norm_vjp = jax.vjp(lambda h: layer_norm(h, ln_gain, ln_bias), hidden2.astype(F32))[1]
        grad_hidden = norm_vjp(grad_z)[0].astype(BF16).reshape(batch, ctx, d)
        return mean_loss, embed_out, grad_hidden, grad_embed, grad_pos

    row_spec = P('dp', None)
    act_spec = P('dp', None, None)
    return jax.shard_map(device_fn, mesh=mesh, in_specs=(row_spec, row_spec, row_spec, act_spec, act_spec, P('tp', None), P(None, None), P(None), P(None)), out_specs=(P(), act_spec, act_spec, P('tp', None), P(None, None)), check_vma=False)
```

```python
import functools

import jax
import jax.numpy as jnp
from jax import lax
from jax.experimental import pallas as pl
from jax.experimental.pallas import tpu as pltpu
from jax.sharding import PartitionSpec as P

MESH = pl.DeviceIdType.MESH
F32 = jnp.float32
BF16 = jnp.bfloat16
NT = (((1,), (1,)), ((), ()))
TN = (((0,), (0,)), ((), ()))
RING = 4
SLOTS = 8
VMEM_LIMIT = 66_000_000


def sizes(tokens, vocab_loc):
    if vocab_loc % 448 == 0 and tokens % 1792 == 0:
        return 448, 256, 56
    return 64, 128, 8


def stats_kernel(chunk, tile, starts, order, skey, hidden, gain, bias, lab, embed, zb, stats, logits_out, rows_out, m_ref, s_ref, l_ref):
    step = pl.program_id(0)
    tokens, d = hidden.shape
    tiles = tokens // tile

    @pl.when(step == 0)
    def _():
        def norm(j, carry):
            rows = pl.ds(pl.multiple_of(j * tile, tile), tile)
            h = hidden[rows, :].astype(F32)
            centered = h - jnp.mean(h, axis=-1, keepdims=True)
            var = jnp.mean(centered * centered, axis=-1, keepdims=True)
            zb[rows, :] = (centered * lax.rsqrt(var + 1e-5) * gain[...] + bias[...]).astype(BF16)
            rows_out[rows, :] = jnp.zeros((tile, d), F32)
            return carry
        lax.fori_loop(0, tiles, norm, 0)
        m_ref[...] = jnp.full_like(m_ref, -jnp.inf)
        s_ref[...] = jnp.zeros_like(s_ref)
        l_ref[...] = jnp.zeros_like(l_ref)

    def token_row(i, carry):
        row = skey[i] - step * chunk
        first = lax.div(row, 16) * 16
        block = embed[pl.ds(pl.multiple_of(first, 16), 16), :].astype(F32)
        pick = lax.broadcasted_iota(jnp.int32, (16, 1), 0) == row - first
        rows_out[pl.ds(order[i], 1), :] = jnp.sum(jnp.where(pick, block, 0.0), axis=0, keepdims=True)
        return carry
    lax.fori_loop(starts[step], starts[step + 1], token_row, 0)

    e = embed[...]
    ids = lax.broadcasted_iota(jnp.int32, (chunk, tile), 0) + step * chunk
    for j in range(tiles):
        cols = slice(j * tile, (j + 1) * tile)
        logits = lax.dot_general(e, zb[cols, :], NT, preferred_element_type=F32)
        logits_out[:, cols] = logits
        m_old = m_ref[:, cols]
        m_new = jnp.maximum(m_old, jnp.max(logits, axis=0, keepdims=True))
        m_ref[:, cols] = m_new
        s_ref[:, cols] = s_ref[:, cols] * jnp.exp(m_old - m_new) + jnp.sum(jnp.exp(logits - m_new), axis=0, keepdims=True)
        l_ref[:, cols] += jnp.sum(jnp.where(ids == lab[:, cols], logits, 0.0), axis=0, keepdims=True)

    @pl.when(step == pl.num_programs(0) - 1)
    def _():
        for j in range(tiles):
            cols = slice(j * tile, (j + 1) * tile)
            stats[j, 0:1, :] = m_ref[:, cols] + jnp.log(s_ref[:, cols])
            stats[j, 1:2, :] = l_ref[:, cols]
            stats[j, 2:8, :] = jnp.zeros((6, tile), F32)


def token_stats(hidden, gain, bias, lab, tok, here, embed, chunk, tile):
    tokens, d = hidden.shape
    vocab_loc = embed.shape[0]
    steps = vocab_loc // chunk
    key = jnp.where(here, tok, vocab_loc).reshape(tokens)
    skey, order = lax.sort_key_val(key, lax.iota(jnp.int32, tokens))
    bounds = lax.iota(jnp.int32, steps + 1) * chunk
    starts = jnp.sum((key[None, :] < bounds[:, None]).astype(jnp.int32), axis=1)
    whole = lambda *shape: pl.BlockSpec(shape, lambda i, *_: (0,) * len(shape))
    return pl.pallas_call(
        functools.partial(stats_kernel, chunk, tile),
        grid_spec=pltpu.PrefetchScalarGridSpec(
            num_scalar_prefetch=3,
            grid=(steps,),
            in_specs=[whole(tokens, d), whole(1, d), whole(1, d), whole(1, tokens),
                      pl.BlockSpec((chunk, d), lambda i, *_: (i, 0))],
            out_specs=(whole(tokens, d), whole(tokens // tile, 8, tile), pl.BlockSpec((chunk, tokens), lambda i, *_: (i, 0)),
                       whole(tokens, d)),
            scratch_shapes=[pltpu.VMEM((1, tokens), F32)] * 3),
        out_shape=(jax.ShapeDtypeStruct((tokens, d), BF16), jax.ShapeDtypeStruct((tokens // tile, 8, tile), F32),
                   jax.ShapeDtypeStruct((vocab_loc, tokens), F32), jax.ShapeDtypeStruct((tokens, d), F32)),
        compiler_params=pltpu.CompilerParams(vmem_limit_bytes=VMEM_LIMIT),
        cost_estimate=pl.CostEstimate(flops=2 * tokens * d * vocab_loc, bytes_accessed=2 * embed.size + 4 * vocab_loc * tokens,
                                      transcendentals=tokens * vocab_loc),
        name='token_stats',
    )(starts, order, skey, hidden, gain, bias, lab, embed)


def grad_kernel(ntp, ndp, chunk, tile, zrows,
                zb, dx, stats, mask, lab, tok, embed, logits,
                out, loss, gz, own, d2d, rs_r, rs_l,
                lse, wgt, st_in, cnt_in, loss_in, lbuf, ebuf, gt, oh, acc, gbuf, ld_own, ld_d2d, s1, s2, fin, rs1, rs2, zin_r, zin_l, zout_r, zout_l, zfin,
                st_s, st_r, cnt_s, cnt_r, loss_s, loss_r, l_sem, e_sem, own_sem, d2d_s, d2d_r, ld_sem, rs1_s, rs1_r, rs2_s, rs2_r, fin_s, ag1_r, ag2_r, fwd_s, part_r,
                zld, zrs_sr, zrs_sl, zrs_rr, zrs_rl, zfin_s, zag_rr, zag_rl, zfw_r, zfw_l):
    tokens, d = zb.shape
    vocab_loc = embed.shape[0]
    nc = vocab_loc // chunk
    tiles = tokens // tile
    ntile = 256 if d % 256 == 0 and d > 256 else 128
    half, quarter, eighth = chunk // 2, chunk // 4, chunk // 8
    dp, z = lax.axis_index('dp'), lax.axis_index('tp')
    core = lax.rem(dp, 2)
    xpos = lax.rem(lax.div(dp, 2), 2)
    ypos = lax.div(dp, 4)
    partner = dp + 1 - 2 * core
    x_nbr = dp + 2 - 4 * xpos
    y_nbr = dp + 4 - 8 * ypos

    def place(k):
        odd = lax.rem(k, 2)
        n1 = x_nbr + (y_nbr - x_nbr) * odd
        n2 = y_nbr + (x_nbr - y_nbr) * odd
        a1 = xpos + (ypos - xpos) * odd
        a2 = ypos + (xpos - ypos) * odd
        return n1, n2, a1, a2

    def rdma(src, dst, ssem, rsem, dev):
        return pltpu.make_async_remote_copy(src_ref=src, dst_ref=dst, send_sem=ssem, recv_sem=rsem,
                                            device_id={'dp': dev}, device_id_type=MESH)

    def zdma(src, dst, ssem, rsem, dev):
        return pltpu.make_async_remote_copy(src_ref=src, dst_ref=dst, send_sem=ssem, recv_sem=rsem,
                                            device_id={'tp': dev}, device_id_type=MESH)

    def rows8(start, n):
        return pl.ds(pl.multiple_of(start, 8), n)

    def valid(k, limit=None):
        return (k >= 0) & (k < (nc if limit is None else limit))

    def e_copy(k):
        return pltpu.make_async_copy(embed.at[rows8(k * chunk, chunk)], ebuf.at[lax.rem(k, 2)], e_sem.at[lax.rem(k, 2)])

    def l_copy(k):
        return pltpu.make_async_copy(logits.at[rows8(k * chunk, chunk)], lbuf.at[lax.rem(k, 2)], l_sem.at[lax.rem(k, 2)])

    def own_copy(k):
        b = lax.rem(k, 2)
        return pltpu.make_async_copy(gbuf.at[b, rows8(core * half, half)], own.at[k], own_sem.at[b])

    def d2d_copy(k):
        b = lax.rem(k, 2)
        return rdma(gbuf.at[b, rows8((1 - core) * half, half)], d2d.at[k], d2d_s.at[b], d2d_r.at[k], partner)

    def rs1_copy(k):
        n1, _, a1, _ = place(k)
        b, r = lax.rem(k, RING), lax.rem(k, SLOTS)
        return rdma(s1.at[b, rows8((1 - a1) * quarter, quarter)], rs1.at[r], rs1_s.at[b], rs1_r.at[r], n1)

    def rs2_copy(k):
        _, n2, _, a2 = place(k)
        b, r = lax.rem(k, RING), lax.rem(k, SLOTS)
        return rdma(s2.at[b, rows8((1 - a2) * eighth, eighth)], rs2.at[r], rs2_s.at[b], rs2_r.at[r], n2)

    def fin_copies(k):
        n1, n2, a1, a2 = place(k)
        b = lax.rem(k, RING)
        dst = out.at[rows8(k * chunk + core * half + a1 * quarter + a2 * eighth, eighth)]
        src = fin.at[b]
        return (pltpu.make_async_copy(src, dst, fin_s.at[0, b]),
                rdma(src, dst, fin_s.at[1, b], ag1_r.at[k], n2),
                rdma(src, dst, fin_s.at[2, b], ag2_r.at[0, k], n1),
                rdma(src, dst, fin_s.at[3, b], part_r.at[0, k], partner))

    def fwd_copies(k):
        n1, _, a1, a2 = place(k)
        b = lax.rem(k, RING)
        ref = out.at[rows8(k * chunk + core * half + a1 * quarter + (1 - a2) * eighth, eighth)]
        return (rdma(ref, ref, fwd_s.at[0, b], ag2_r.at[1, k], n1),
                rdma(ref, ref, fwd_s.at[1, b], part_r.at[1, k], partner))

    def last_copy(k):
        _, _, a1, _ = place(k)
        ref = out.at[rows8(k * chunk + core * half + (1 - a1) * quarter, quarter)]
        return rdma(ref, ref, fwd_s.at[2, lax.rem(k, RING)], part_r.at[2, k], partner)

    def peer(i, n, me):
        return lax.rem(me + i, n)

    def st_copy(i, src_of):
        return zdma(st_in.at[z], st_in.at[src_of], st_s.at[i - 1], st_r.at[src_of], peer(i, ntp, z))

    def tile_copy(buf, ssem, rsem, i, src_of):
        return rdma(buf.at[dp], buf.at[src_of], ssem.at[i - 1], rsem.at[src_of], peer(i, ndp, dp))

    def share_start():
        st_in[z] = stats[...]
        for i in range(1, ntp):
            st_copy(i, z).start()
        cnt_in[dp] = jnp.broadcast_to(jnp.sum(jnp.sum(mask[...], axis=0), axis=-1, keepdims=True), (8, 128))
        for i in range(1, ndp):
            tile_copy(cnt_in, cnt_s, cnt_r, i, dp).start()

    def in_order_sum(buf):
        total = buf[0]
        for i in range(1, ndp):
            total = total + buf[i]
        return total[0:1, 0:1]

    def share_use():
        for i in range(1, ndp):
            tile_copy(cnt_in, cnt_s, cnt_r, i, peer(i, ndp, dp)).wait_recv()
        for i in range(1, ntp):
            st_copy(i, peer(i, ntp, z)).wait_recv()
        count = in_order_sum(cnt_in)
        part = jnp.zeros((1, tile), F32)
        for j in range(tiles):
            shard = [st_in[q, j] for q in range(ntp)]
            top = functools.reduce(jnp.maximum, [a[0:1] for a in shard])
            total = functools.reduce(jnp.add, [jnp.exp(a[0:1] - top) for a in shard])
            lse_j = top + jnp.log(total)
            lse[j] = lse_j
            wgt[j] = mask[j] / count
            part = part + mask[j] * (lse_j - functools.reduce(jnp.add, [a[1:2] for a in shard]))
        loss_in[dp] = jnp.broadcast_to(jnp.sum(part, axis=-1, keepdims=True), (8, 128))
        for i in range(1, ndp):
            tile_copy(loss_in, loss_s, loss_r, i, dp).start()

    def share_end():
        for i in range(1, ndp):
            tile_copy(loss_in, loss_s, loss_r, i, peer(i, ndp, dp)).wait_recv()
        loss[...] = jnp.broadcast_to(in_order_sum(loss_in) / in_order_sum(cnt_in), (8, 128))
        for i in range(1, ndp):
            tile_copy(cnt_in, cnt_s, cnt_r, i, dp).wait_send()
            tile_copy(loss_in, loss_s, loss_r, i, dp).wait_send()
        for i in range(1, ntp):
            st_copy(i, z).wait_send()

    def compute(k, carry):
        slot = lax.rem(k, 2)
        e_copy(k).wait()
        l_copy(k).wait()

        @pl.when(k + 1 < nc)
        def _():
            e_copy(k + 1).start()
            l_copy(k + 1).start()

        ids = lax.broadcasted_iota(jnp.int32, (chunk, tile), 0) + k * chunk

        def per_tile(j, c):
            cols = pl.ds(pl.multiple_of(j * tile, tile), tile)
            hit = jnp.where(ids == lab[j], 1.0, 0.0)
            g = ((jnp.exp(lbuf[slot, :, cols] - lse[j]) - hit) * wgt[j]).astype(BF16)
            gt[:, cols] = g
            oh[:, cols] = jnp.where(ids == tok[j], 1.0, 0.0).astype(BF16)
            acc[cols, :] += lax.dot_general(g, ebuf[slot], TN, preferred_element_type=F32)
            return c
        lax.fori_loop(0, tiles, per_tile, 0)

        @pl.when(k >= 1)
        def _():
            own_copy(k - 1).wait()
            d2d_copy(k - 1).wait_send()

        def per_cols(n, c):
            cols = pl.ds(pl.multiple_of(n * ntile, ntile), ntile)
            gbuf[slot, :, cols] = (jnp.dot(gt[...], zb[:, cols], preferred_element_type=F32)
                                   + jnp.dot(oh[...], dx[:, cols], preferred_element_type=F32))
            return c
        lax.fori_loop(0, d // ntile, per_cols, 0)
        own_copy(k).start()
        d2d_copy(k).start()

        @pl.when(k == nc - 1)
        def _():
            own_copy(k).wait()
            d2d_copy(k).wait_send()
        return carry

    def load_start(k):
        d2d_copy(k).wait_recv()
        pltpu.make_async_copy(own.at[k], ld_own, ld_sem.at[0]).start()
        pltpu.make_async_copy(d2d.at[k], ld_d2d, ld_sem.at[1]).start()

    def stage_a(k):
        pltpu.make_async_copy(own.at[k], ld_own, ld_sem.at[0]).wait()
        pltpu.make_async_copy(d2d.at[k], ld_d2d, ld_sem.at[1]).wait()

        @pl.when(k >= RING)
        def _():
            rs1_copy(k - RING).wait_send()
        b = lax.rem(k, RING)

        def add(i, c):
            r = rows8(i * eighth, eighth)
            s1[b, r, :] = ld_own[r, :] + ld_d2d[r, :]
            return c
        lax.fori_loop(0, half // eighth, add, 0)
        rs1_copy(k).start()

    def stage_b(k):
        _, _, a1, _ = place(k)
        rs1_copy(k).wait_recv()

        @pl.when(k >= RING)
        def _():
            rs2_copy(k - RING).wait_send()
        b, r = lax.rem(k, RING), lax.rem(k, SLOTS)

        def add(i, c):
            s2[b, rows8(i * eighth, eighth), :] = (s1[b, rows8(a1 * quarter + i * eighth, eighth), :]
                                                   + rs1[r, rows8(i * eighth, eighth), :])
            return c
        lax.fori_loop(0, quarter // eighth, add, 0)
        rs2_copy(k).start()

    def stage_c(k):
        _, _, _, a2 = place(k)
        rs2_copy(k).wait_recv()

        @pl.when(k >= RING)
        def _():
            for i, c in enumerate(fin_copies(k - RING)):
                c.wait() if i == 0 else c.wait_send()
        b, r = lax.rem(k, RING), lax.rem(k, SLOTS)
        fin[b] = s2[b, rows8(a2 * eighth, eighth), :] + rs2[r]
        for c in fin_copies(k):
            c.start()

    def stage_d(k):
        fin_copies(k)[1].wait_recv()

        @pl.when(k >= RING)
        def _():
            for c in fwd_copies(k - RING):
                c.wait_send()
        for c in fwd_copies(k):
            c.start()

    def stage_e(k):
        fin_copies(k)[2].wait_recv()
        fwd_copies(k)[0].wait_recv()

        @pl.when(k >= RING)
        def _():
            last_copy(k - RING).wait_send()
        last_copy(k).start()

    def stage_f(k):
        fin_copies(k)[3].wait_recv()
        fwd_copies(k)[1].wait_recv()
        last_copy(k).wait_recv()

    nb = tokens // ntp // zrows
    qrows = tokens // ntp

    def zacc(q, b):
        return pl.multiple_of(q * qrows + b * zrows, 8)

    def right_copy(b, i, src=None):
        n = ntp - 1 - i
        s = zout_r.at[lax.rem(b, 2), pl.ds(i, n)] if src is None else src
        return zdma(s, rs_r.at[b, pl.ds(i, n)], zrs_sr.at[lax.rem(b, 2)], zrs_rr.at[b], i + 1)

    def left_copy(b, i):
        return zdma(zout_l.at[lax.rem(b, 2), pl.ds(0, i)], rs_l.at[b, pl.ds(0, i)], zrs_sl.at[lax.rem(b, 2)],
                    zrs_rl.at[b], i - 1)

    def z_right(b):
        for i in range(ntp - 1):
            @pl.when(z == i)
            def _(i=i):
                n = ntp - 1 - i
                if i > 0:
                    right_copy(b, i - 1).wait_recv()
                    load = pltpu.make_async_copy(rs_r.at[b, pl.ds(i, n)], zin_r.at[pl.ds(i, n)], zld.at[0])
                    load.start()
                    load.wait()

                @pl.when(b >= 2)
                def _():
                    right_copy(b - 2, i).wait_send()
                for q in range(i + 1, ntp):
                    mine = acc[pl.ds(zacc(q, b), zrows), :]
                    zout_r[lax.rem(b, 2), q - 1] = mine if i == 0 else zin_r[q - 1] + mine
                right_copy(b, i).start()

    def z_left(b):
        for i in range(1, ntp):
            @pl.when(z == i)
            def _(i=i):
                if i < ntp - 1:
                    left_copy(b, i + 1).wait_recv()
                    load = pltpu.make_async_copy(rs_l.at[b, pl.ds(0, i)], zin_l.at[pl.ds(0, i)], zld.at[0])
                    load.start()
                    load.wait()

                @pl.when(b >= 2)
                def _():
                    left_copy(b - 2, i).wait_send()
                for q in range(i):
                    mine = acc[pl.ds(zacc(q, b), zrows), :]
                    zout_l[lax.rem(b, 2), q] = mine if i == ntp - 1 else zin_l[q] + mine
                left_copy(b, i).start()

    def zfin_copies(b):
        s = lax.rem(b, 2)
        dst = gz.at[rows8(z * qrows + b * zrows, zrows)]
        return (pltpu.make_async_copy(zfin.at[s], dst, zfin_s.at[0, s]),
                zdma(zfin.at[s], dst, zfin_s.at[1, s], zag_rr.at[b, 0], z + 1),
                zdma(zfin.at[s], dst, zfin_s.at[2, s], zag_rl.at[b, 0], z - 1))

    def z_final(b):
        for i in range(ntp):
            @pl.when(z == i)
            def _(i=i):
                if i > 0:
                    right_copy(b, i - 1).wait_recv() if i == ntp - 1 else None
                    load = pltpu.make_async_copy(rs_r.at[b, i - 1], zin_r.at[i - 1], zld.at[0])
                    load.start()
                    load.wait()
                if i < ntp - 1:
                    left_copy(b, i + 1).wait_recv() if i == 0 else None
                    load = pltpu.make_async_copy(rs_l.at[b, i], zin_l.at[i], zld.at[0])
                    load.start()
                    load.wait()
                z_wait_fin(b - 2, b >= 2)
                total = acc[pl.ds(zacc(i, b), zrows), :]
                if i > 0:
                    total = zin_r[i - 1] + total
                if i < ntp - 1:
                    total = total + zin_l[i]
                zfin[lax.rem(b, 2)] = total
        copies = zfin_copies(b)
        copies[0].start()

        @pl.when(z < ntp - 1)
        def _():
            copies[1].start()

        @pl.when(z > 0)
        def _():
            copies[2].start()

    def z_wait_fin(b, cond):
        @pl.when(cond)
        def _():
            copies = zfin_copies(b)
            copies[0].wait()

            @pl.when(z < ntp - 1)
            def _():
                copies[1].wait_send()

            @pl.when(z > 0)
            def _():
                copies[2].wait_send()

    def zag(b, h, sign, ssem, rsem):
        ref = gz.at[rows8((z - sign * h) * qrows + b * zrows, zrows)]
        return zdma(ref, ref, ssem.at[b, h - 1], rsem.at[b, h], z + sign)

    def z_hop(b, h):
        ref_r = gz.at[rows8((z - h) * qrows + b * zrows, zrows)]
        ref_l = gz.at[rows8((z + h) * qrows + b * zrows, zrows)]

        @pl.when(z >= h)
        def _():
            zdma(ref_r, ref_r, zfw_r.at[b, 0], zag_rr.at[b, h - 1], z).wait_recv()
            if h < ntp - 1:
                @pl.when(z < ntp - 1)
                def _():
                    zag(b, h, 1, zfw_r, zag_rr).start()

        @pl.when(z + h <= ntp - 1)
        def _():
            zdma(ref_l, ref_l, zfw_l.at[b, 0], zag_rl.at[b, h - 1], z).wait_recv()
            if h < ntp - 1:
                @pl.when(z > 0)
                def _():
                    zag(b, h, -1, zfw_l, zag_rl).start()

    lead = min(5, nc)

    def cs(t):
        late = t - lead
        c = lead + lax.div(late * 3, 2)
        return jnp.minimum(jnp.where(t <= lead, t, c), nc)

    z_start = lead + -(-(nc - lead) * 2 // 3)
    ticks = max(nc + 9, z_start + nb + 2 * ntp)
    share_start()
    e_copy(0).start()
    l_copy(0).start()

    def clear(j, carry):
        acc[pl.ds(pl.multiple_of(j * tile, tile), tile), :] = jnp.zeros((tile, d), F32)
        return carry
    lax.fori_loop(0, tiles, clear, 0)
    share_use()

    def tick(t, carry):
        ka = t - 2

        @pl.when(valid(ka))
        def _():
            load_start(ka)
        lax.fori_loop(cs(t), cs(t + 1), compute, 0)
        for stage, lag in ((stage_e, 7), (stage_d, 6), (stage_c, 5), (stage_b, 4), (stage_a, 2), (stage_f, 8)):
            @pl.when(valid(t - lag))
            def _(stage=stage, lag=lag):
                stage(t - lag)
        zt = t - z_start

        @pl.when(valid(zt - z, nb))
        def _():
            z_right(zt - z)

        @pl.when(valid(zt - (ntp - 1 - z), nb))
        def _():
            z_left(zt - (ntp - 1 - z))

        @pl.when(valid(zt - (ntp - 1), nb))
        def _():
            z_final(zt - (ntp - 1))
        for h in range(1, ntp):
            @pl.when(valid(zt - (ntp - 1) - h, nb))
            def _(h=h):
                z_hop(zt - (ntp - 1) - h, h)
        return carry
    lax.fori_loop(0, ticks, tick, 0)

    share_end()

    for k in range(max(nc - RING, 0), nc):
        rs1_copy(k).wait_send()
        rs2_copy(k).wait_send()
        for i, c in enumerate(fin_copies(k)):
            c.wait() if i == 0 else c.wait_send()
        for c in fwd_copies(k):
            c.wait_send()
        last_copy(k).wait_send()
    for b in range(max(nb - 2, 0), nb):
        for i in range(ntp - 1):
            @pl.when(z == i)
            def _(i=i, b=b):
                right_copy(b, i).wait_send()
        for i in range(1, ntp):
            @pl.when(z == i)
            def _(i=i, b=b):
                left_copy(b, i).wait_send()
        z_wait_fin(b, z >= 0)

    def drain(b, carry):
        for h in range(1, ntp - 1):
            @pl.when((z >= h) & (z < ntp - 1))
            def _(h=h):
                zag(b, h, 1, zfw_r, zag_rr).wait_send()

            @pl.when((z + h <= ntp - 1) & (z > 0))
            def _(h=h):
                zag(b, h, -1, zfw_l, zag_rl).wait_send()
        return carry
    lax.fori_loop(0, nb, drain, 0)


def gradients(ntp, ndp, zb, dx, stats, mask, lab, tok, embed, logits, chunk, tile, zrows):
    tokens, d = zb.shape
    vocab_loc = embed.shape[0]
    nc = vocab_loc // chunk
    half, quarter, eighth = chunk // 2, chunk // 4, chunk // 8
    tiles = tokens // tile
    nb = tokens // ntp // zrows
    vm = pl.BlockSpec(memory_space=pltpu.VMEM)
    hbm = pl.BlockSpec(memory_space=pl.ANY)
    dma = lambda *s: pltpu.SemaphoreType.DMA(s)
    vf = lambda *s: pltpu.VMEM(s, F32)
    sds = lambda *s: jax.ShapeDtypeStruct(s, F32)
    flops = 2 * tokens * d * vocab_loc
    rows = lambda a: a.reshape(tiles, 1, tile)
    res = pl.pallas_call(
        functools.partial(grad_kernel, ntp, ndp, chunk, tile, zrows),
        out_shape=(sds(vocab_loc, d), sds(8, 128), sds(tokens, d), sds(nc, half, d), sds(nc, half, d),
                   sds(nb, ntp - 1, zrows, d), sds(nb, ntp - 1, zrows, d)),
        in_specs=[vm] * 6 + [hbm] * 2,
        out_specs=(hbm, vm) + (hbm,) * 5,
        scratch_shapes=[
            vf(tiles, 1, tile), vf(tiles, 1, tile), vf(ntp, tiles, 8, tile), vf(ndp, 8, 128), vf(ndp, 8, 128),
            vf(2, chunk, tokens),
            pltpu.VMEM((2, chunk, d), BF16), pltpu.VMEM((chunk, tokens), BF16), pltpu.VMEM((chunk, tokens), BF16),
            vf(tokens, d), vf(2, chunk, d), vf(half, d), vf(half, d),
            vf(RING, half, d), vf(RING, quarter, d), vf(RING, eighth, d), vf(SLOTS, quarter, d), vf(SLOTS, eighth, d),
            vf(ntp - 1, zrows, d), vf(ntp - 1, zrows, d), vf(2, ntp - 1, zrows, d), vf(2, ntp - 1, zrows, d),
            vf(2, zrows, d),
            dma(ntp - 1), dma(ntp), dma(ndp - 1), dma(ndp), dma(ndp - 1), dma(ndp), dma(2),
            dma(2), dma(2), dma(2), dma(nc), dma(2), dma(RING), dma(SLOTS), dma(RING), dma(SLOTS), dma(4, RING),
            dma(nc), dma(2, nc), dma(3, RING), dma(3, nc),
            dma(1), dma(2), dma(2), dma(nb), dma(nb), dma(3, 2), dma(nb, ntp - 1), dma(nb, ntp - 1),
            dma(nb, ntp - 1), dma(nb, ntp - 1),
        ],
        compiler_params=pltpu.CompilerParams(vmem_limit_bytes=VMEM_LIMIT, has_side_effects=True),
        cost_estimate=pl.CostEstimate(flops=3 * flops, bytes_accessed=4 * vocab_loc * (4 * d + tokens),
                                      transcendentals=tokens * vocab_loc),
        name='gradients',
    )(zb, dx, stats, rows(mask), rows(lab), rows(tok), embed, logits)
    return res[:3]


def layer_norm(h_f32, ln_gain, ln_bias):
    mean_val = jnp.mean(h_f32, axis=-1, keepdims=True)
    centered = h_f32 - mean_val
    var_val = jnp.mean(centered * centered, axis=-1, keepdims=True)
    return centered * lax.rsqrt(var_val + 1e-5) * ln_gain + ln_bias


def solution(mesh):
    ntp, ndp = mesh.shape['tp'], mesh.shape['dp']

    def device_fn(tokens, labels, lossmask, hidden, grad_x0, embed_loc, pos_table, ln_gain, ln_bias):
        vocab_loc, d = embed_loc.shape
        batch, ctx = tokens.shape
        ntok = batch * ctx
        chunk, tile, zrows = sizes(ntok, vocab_loc)
        shard_start = lax.axis_index('tp') * vocab_loc
        tok_local = (tokens - shard_start).reshape(1, ntok)
        lab_local = (labels - shard_start).reshape(1, ntok)
        tok_here = (tok_local >= 0) & (tok_local < vocab_loc)
        grad_pos = lax.psum(jnp.sum(grad_x0.astype(F32), axis=0), 'dp')

        hidden2 = hidden.reshape(ntok, d)
        zb, stats, logits, rows = token_stats(hidden2, ln_gain.reshape(1, d), ln_bias.reshape(1, d), lab_local, tok_local,
                                              tok_here, embed_loc, chunk, tile)
        rows = lax.psum(rows, 'tp').reshape(batch, ctx, d)
        embed_out = (rows + pos_table.astype(F32)[None]).astype(BF16)
        grad_embed, loss, grad_z = gradients(ntp, ndp, zb, grad_x0.reshape(ntok, d), stats, lossmask.astype(F32), lab_local,
                                             tok_local, embed_loc, logits, chunk, tile, zrows)
        mean_loss = loss[0, 0]
        norm_vjp = jax.vjp(lambda h: layer_norm(h, ln_gain, ln_bias), hidden2.astype(F32))[1]
        grad_hidden = norm_vjp(grad_z)[0].astype(BF16).reshape(batch, ctx, d)
        return mean_loss, embed_out, grad_hidden, grad_embed, grad_pos

    row_spec = P('dp', None)
    act_spec = P('dp', None, None)
    return jax.shard_map(device_fn, mesh=mesh, in_specs=(row_spec, row_spec, row_spec, act_spec, act_spec, P('tp', None), P(None, None), P(None), P(None)), out_specs=(P(), act_spec, act_spec, P('tp', None), P(None, None)), check_vma=False)
```

```python
import functools

import jax
import jax.numpy as jnp
from jax import lax
from jax.experimental import pallas as pl
from jax.experimental.pallas import tpu as pltpu
from jax.sharding import PartitionSpec as P

MESH = pl.DeviceIdType.MESH
F32 = jnp.float32
BF16 = jnp.bfloat16
NT = (((1,), (1,)), ((), ()))
TN = (((0,), (0,)), ((), ()))
RING = 4
SLOTS = 8
STEPS = 2
VMEM_LIMIT = 66_000_000


def sizes(tokens, vocab_loc):
    if vocab_loc % 448 == 0 and tokens % 1792 == 0:
        return (928 if vocab_loc % 928 == 0 else 448), 448, 256, 32
    return 64, 64, 128, 8


def stats_kernel(chunk, tile, starts, order, skey, hidden, gain, bias, lab, embed, zb, stats, logits_out, rows_out, m_ref, s_ref, l_ref):
    step = pl.program_id(0)
    tokens, d = hidden.shape
    tiles = tokens // tile

    @pl.when(step == 0)
    def _():
        def norm(j, carry):
            rows = pl.ds(pl.multiple_of(j * tile, tile), tile)
            h = hidden[rows, :].astype(F32)
            centered = h - jnp.mean(h, axis=-1, keepdims=True)
            var = jnp.mean(centered * centered, axis=-1, keepdims=True)
            zb[rows, :] = (centered * lax.rsqrt(var + 1e-5) * gain[...] + bias[...]).astype(BF16)
            rows_out[rows, :] = jnp.zeros((tile, d), F32)
            return carry
        lax.fori_loop(0, tiles, norm, 0)
        m_ref[...] = jnp.full_like(m_ref, -jnp.inf)
        s_ref[...] = jnp.zeros_like(s_ref)
        l_ref[...] = jnp.zeros_like(l_ref)

    first_tok, end_tok = starts[step], starts[step + 1]

    def token_rows(n, carry):
        for u in range(4):
            i = jnp.minimum(first_tok + n * 4 + u, end_tok - 1)
            row = skey[i] - step * chunk
            group = lax.div(row, 16) * 16
            block = embed[pl.ds(pl.multiple_of(group, 16), 16), :].astype(F32)
            pick = lax.broadcasted_iota(jnp.int32, (16, 1), 0) == row - group
            rows_out[pl.ds(order[i], 1), :] = jnp.sum(jnp.where(pick, block, 0.0), axis=0, keepdims=True)
        return carry
    lax.fori_loop(0, lax.div(end_tok - first_tok + 3, 4), token_rows, 0)

    ids = lax.broadcasted_iota(jnp.int32, (chunk, tile), 0) + step * chunk

    def product(j):
        cols = slice(j * tile, (j + 1) * tile)
        logits_out[:, cols] = lax.dot_general(embed[...], zb[cols, :], NT, preferred_element_type=F32)

    product(0)
    for j in range(tiles):
        cols = slice(j * tile, (j + 1) * tile)
        if j + 1 < tiles:
            product(j + 1)
        logits = logits_out[:, cols]
        m_old = m_ref[:, cols]
        m_new = jnp.maximum(m_old, jnp.max(logits, axis=0, keepdims=True))
        m_ref[:, cols] = m_new
        s_ref[:, cols] = s_ref[:, cols] * jnp.exp(m_old - m_new) + jnp.sum(jnp.exp(logits - m_new), axis=0, keepdims=True)
        l_ref[:, cols] += jnp.sum(jnp.where(ids == lab[:, cols], logits, 0.0), axis=0, keepdims=True)

    @pl.when(step == pl.num_programs(0) - 1)
    def _():
        for j in range(tiles):
            cols = slice(j * tile, (j + 1) * tile)
            stats[j, 0:1, :] = m_ref[:, cols] + jnp.log(s_ref[:, cols])
            stats[j, 1:2, :] = l_ref[:, cols]
            stats[j, 2:8, :] = jnp.zeros((6, tile), F32)


def token_stats(hidden, gain, bias, lab, tok, here, embed, chunk, tile):
    tokens, d = hidden.shape
    vocab_loc = embed.shape[0]
    steps = vocab_loc // chunk
    key = jnp.where(here, tok, vocab_loc).reshape(tokens)
    skey, order = lax.sort_key_val(key, lax.iota(jnp.int32, tokens))
    bounds = lax.iota(jnp.int32, steps + 1) * chunk
    starts = jnp.sum((key[None, :] < bounds[:, None]).astype(jnp.int32), axis=1)
    whole = pl.BlockSpec(memory_space=pltpu.VMEM)
    return pl.pallas_call(
        functools.partial(stats_kernel, chunk, tile),
        grid_spec=pltpu.PrefetchScalarGridSpec(
            num_scalar_prefetch=3,
            grid=(steps,),
            in_specs=[whole, whole, whole, whole, pl.BlockSpec((chunk, d), lambda i, *_: (i, 0))],
            out_specs=(whole, whole, pl.BlockSpec((chunk, tokens), lambda i, *_: (i, 0)), whole),
            scratch_shapes=[pltpu.VMEM((1, tokens), F32)] * 3),
        out_shape=(jax.ShapeDtypeStruct((tokens, d), BF16), jax.ShapeDtypeStruct((tokens // tile, 8, tile), F32),
                   jax.ShapeDtypeStruct((vocab_loc, tokens), F32), jax.ShapeDtypeStruct((tokens, d), F32)),
        compiler_params=pltpu.CompilerParams(vmem_limit_bytes=VMEM_LIMIT),
        cost_estimate=pl.CostEstimate(flops=2 * tokens * d * vocab_loc, bytes_accessed=2 * embed.size + 4 * vocab_loc * tokens,
                                      transcendentals=tokens * vocab_loc),
        name='token_stats',
    )(starts, order, skey, hidden, gain, bias, lab, embed)


def grad_kernel(ntp, ndp, chunk, tile, zrows,
                zb, dx, stats, mask, lab, tok, gain, hidden, embed, logits,
                out, loss, gz, own, d2d, rs_r, rs_l, gsave,
                lse, wgt, st_in, cnt_in, loss_in, lbuf, ebuf, gz_t, hbuf, gt, oh, acc, gbuf, ld_own, ld_d2d, s1, s2, fin, rs1, rs2, zin_r, zin_l, zout_r, zout_l, zfin,
                st_s, st_r, cnt_s, cnt_r, loss_s, loss_r, l_sem, e_sem, gs_sem, gl_sem, h_sem, own_sem, d2d_s, d2d_r, ld_sem, rs1_s, rs1_r, rs2_s, rs2_r, fin_s, ag1_r, ag2_r, fwd_s, part_r,
                zld, zrs_sr, zrs_sl, zrs_rr, zrs_rl, zfin_s, zag_rr, zag_rl, zfw_r, zfw_l):
    tokens, d = zb.shape
    vocab_loc = embed.shape[0]
    nc = vocab_loc // chunk
    tiles = tokens // tile
    ntile = 256 if d % 256 == 0 and d > 256 else 128
    ntiles = d // ntile
    half, quarter, eighth = chunk // 2, chunk // 4, chunk // 8
    dp, z = lax.axis_index('dp'), lax.axis_index('tp')
    core = lax.rem(dp, 2)
    xpos = lax.rem(lax.div(dp, 2), 2)
    ypos = lax.div(dp, 4)
    partner = dp + 1 - 2 * core
    x_nbr = dp + 2 - 4 * xpos
    y_nbr = dp + 4 - 8 * ypos

    def place(k):
        odd = lax.rem(k, 2)
        n1 = x_nbr + (y_nbr - x_nbr) * odd
        n2 = y_nbr + (x_nbr - y_nbr) * odd
        a1 = xpos + (ypos - xpos) * odd
        a2 = ypos + (xpos - ypos) * odd
        return n1, n2, a1, a2

    def rdma(src, dst, ssem, rsem, dev):
        return pltpu.make_async_remote_copy(src_ref=src, dst_ref=dst, send_sem=ssem, recv_sem=rsem,
                                            device_id={'dp': dev}, device_id_type=MESH)

    def zdma(src, dst, ssem, rsem, dev):
        return pltpu.make_async_remote_copy(src_ref=src, dst_ref=dst, send_sem=ssem, recv_sem=rsem,
                                            device_id={'tp': dev}, device_id_type=MESH)

    def rows8(start, n):
        return pl.ds(pl.multiple_of(start, 8), n)

    def valid(k, limit=None):
        return (k >= 0) & (k < (nc if limit is None else limit))

    def e_copy(k):
        return pltpu.make_async_copy(embed.at[rows8(k * chunk, chunk)], ebuf.at[lax.rem(k, 2)], e_sem.at[lax.rem(k, 2)])

    def l_copy(k):
        return pltpu.make_async_copy(logits.at[rows8(k * chunk, chunk)], lbuf.at[lax.rem(k, 2)], l_sem.at[lax.rem(k, 2)])

    def gs_copy(k):
        b = lax.rem(k, 2)
        return pltpu.make_async_copy(gz_t.at[b], gsave.at[k], gs_sem.at[b])

    def gl_copy(k):
        return pltpu.make_async_copy(gsave.at[k], gt, gl_sem.at[0])

    def own_copy(k):
        return pltpu.make_async_copy(gbuf.at[rows8(core * half, half)], own.at[k], own_sem.at[0])

    def d2d_copy(k):
        return rdma(gbuf.at[rows8((1 - core) * half, half)], d2d.at[k], d2d_s.at[0], d2d_r.at[k], partner)

    def rs1_copy(k):
        n1, _, a1, _ = place(k)
        b, r = lax.rem(k, RING), lax.rem(k, SLOTS)
        return rdma(s1.at[b, rows8((1 - a1) * quarter, quarter)], rs1.at[r], rs1_s.at[b], rs1_r.at[r], n1)

    def rs2_copy(k):
        _, n2, _, a2 = place(k)
        b, r = lax.rem(k, RING), lax.rem(k, SLOTS)
        return rdma(s2.at[b, rows8((1 - a2) * eighth, eighth)], rs2.at[r], rs2_s.at[b], rs2_r.at[r], n2)

    def fin_copies(k):
        n1, n2, a1, a2 = place(k)
        b = lax.rem(k, RING)
        dst = out.at[rows8(k * chunk + core * half + a1 * quarter + a2 * eighth, eighth)]
        src = fin.at[b]
        return (pltpu.make_async_copy(src, dst, fin_s.at[0, b]),
                rdma(src, dst, fin_s.at[1, b], ag1_r.at[k], n2),
                rdma(src, dst, fin_s.at[2, b], ag2_r.at[0, k], n1),
                rdma(src, dst, fin_s.at[3, b], part_r.at[0, k], partner))

    def fwd_copies(k):
        n1, _, a1, a2 = place(k)
        b = lax.rem(k, RING)
        ref = out.at[rows8(k * chunk + core * half + a1 * quarter + (1 - a2) * eighth, eighth)]
        return (rdma(ref, ref, fwd_s.at[0, b], ag2_r.at[1, k], n1),
                rdma(ref, ref, fwd_s.at[1, b], part_r.at[1, k], partner))

    def last_copy(k):
        _, _, a1, _ = place(k)
        ref = out.at[rows8(k * chunk + core * half + (1 - a1) * quarter, quarter)]
        return rdma(ref, ref, fwd_s.at[2, lax.rem(k, RING)], part_r.at[2, k], partner)

    def peer(i, n, me):
        return lax.rem(me + i, n)

    def st_copy(i, src_of):
        return zdma(st_in.at[z], st_in.at[src_of], st_s.at[i - 1], st_r.at[src_of], peer(i, ntp, z))

    def tile_copy(buf, ssem, rsem, i, src_of):
        return rdma(buf.at[dp], buf.at[src_of], ssem.at[i - 1], rsem.at[src_of], peer(i, ndp, dp))

    def share_start():
        st_in[z] = stats[...]
        for i in range(1, ntp):
            st_copy(i, z).start()
        cnt_in[dp] = jnp.broadcast_to(jnp.sum(jnp.sum(mask[...], axis=0), axis=-1, keepdims=True), (8, 128))
        for i in range(1, ndp):
            tile_copy(cnt_in, cnt_s, cnt_r, i, dp).start()

    def in_order_sum(buf):
        total = buf[0]
        for i in range(1, ndp):
            total = total + buf[i]
        return total[0:1, 0:1]

    def share_use():
        for i in range(1, ndp):
            tile_copy(cnt_in, cnt_s, cnt_r, i, peer(i, ndp, dp)).wait_recv()
        for i in range(1, ntp):
            st_copy(i, peer(i, ntp, z)).wait_recv()
        count = in_order_sum(cnt_in)
        part = jnp.zeros((1, tile), F32)
        for j in range(tiles):
            shard = [st_in[q, j] for q in range(ntp)]
            top = functools.reduce(jnp.maximum, [a[0:1] for a in shard])
            total = functools.reduce(jnp.add, [jnp.exp(a[0:1] - top) for a in shard])
            lse_j = top + jnp.log(total)
            lse[j] = lse_j
            wgt[j] = mask[j] / count
            part = part + mask[j] * (lse_j - functools.reduce(jnp.add, [a[1:2] for a in shard]))
        loss_in[dp] = jnp.broadcast_to(jnp.sum(part, axis=-1, keepdims=True), (8, 128))
        for i in range(1, ndp):
            tile_copy(loss_in, loss_s, loss_r, i, dp).start()

    def share_end():
        for i in range(1, ndp):
            tile_copy(loss_in, loss_s, loss_r, i, peer(i, ndp, dp)).wait_recv()
        loss[...] = jnp.broadcast_to(in_order_sum(loss_in) / in_order_sum(cnt_in), (8, 128))
        for i in range(1, ndp):
            tile_copy(cnt_in, cnt_s, cnt_r, i, dp).wait_send()
            tile_copy(loss_in, loss_s, loss_r, i, dp).wait_send()
        for i in range(1, ntp):
            st_copy(i, z).wait_send()

    def z_unit(u, carry):
        k, j = lax.div(u, tiles), lax.rem(u, tiles)
        slot = lax.rem(k, 2)

        @pl.when(j == 0)
        def _():
            e_copy(k).wait()
            l_copy(k).wait()

            @pl.when(k + 1 < nc)
            def _():
                e_copy(k + 1).start()
                l_copy(k + 1).start()

            @pl.when(k >= 1)
            def _():
                gs_copy(k - 1).wait()
        cols = pl.ds(pl.multiple_of(j * tile, tile), tile)
        ids = lax.broadcasted_iota(jnp.int32, (chunk, tile), 0) + k * chunk
        hit = jnp.where(ids == lab[j], 1.0, 0.0)
        g = ((jnp.exp(lbuf[slot, :, cols] - lse[j]) - hit) * wgt[j]).astype(BF16)
        gz_t[slot, :, cols] = g
        acc[cols, :] += lax.dot_general(g, ebuf[slot], TN, preferred_element_type=F32)

        @pl.when(j == tiles - 1)
        def _():
            gs_copy(k).start()

            @pl.when(k == nc - 1)
            def _():
                gs_copy(k).wait()
        return carry

    def g_unit(u, carry):
        k, n = lax.div(u, ntiles), lax.rem(u, ntiles)

        @pl.when(n == 0)
        def _():
            def one_hot(j, c):
                cols = pl.ds(pl.multiple_of(j * tile, tile), tile)
                ids = lax.broadcasted_iota(jnp.int32, (chunk, tile), 0) + k * chunk
                oh[:, cols] = jnp.where(ids == tok[j], 1.0, 0.0).astype(BF16)
                return c
            lax.fori_loop(0, tiles, one_hot, 0)

            @pl.when(k >= 1)
            def _():
                own_copy(k - 1).wait()
                d2d_copy(k - 1).wait_send()
            gl_copy(k).wait()
        cols = pl.ds(pl.multiple_of(n * ntile, ntile), ntile)
        gbuf[:, cols] = (jnp.dot(gt[...], zb[:, cols], preferred_element_type=F32)
                         + jnp.dot(oh[...], dx[:, cols], preferred_element_type=F32))

        @pl.when(n == ntiles - 1)
        def _():
            own_copy(k).start()
            d2d_copy(k).start()

            @pl.when(k == nc - 1)
            def _():
                own_copy(k).wait()
                d2d_copy(k).wait_send()
        return carry

    def load_start(k):
        d2d_copy(k).wait_recv()
        pltpu.make_async_copy(own.at[k], ld_own, ld_sem.at[0]).start()
        pltpu.make_async_copy(d2d.at[k], ld_d2d, ld_sem.at[1]).start()

    def stage_a(k):
        pltpu.make_async_copy(own.at[k], ld_own, ld_sem.at[0]).wait()
        pltpu.make_async_copy(d2d.at[k], ld_d2d, ld_sem.at[1]).wait()

        @pl.when(k >= RING)
        def _():
            rs1_copy(k - RING).wait_send()
        b = lax.rem(k, RING)

        def add(i, c):
            r = rows8(i * eighth, eighth)
            s1[b, r, :] = ld_own[r, :] + ld_d2d[r, :]
            return c
        lax.fori_loop(0, half // eighth, add, 0)
        rs1_copy(k).start()

    def stage_b(k):
        _, _, a1, _ = place(k)
        rs1_copy(k).wait_recv()

        @pl.when(k >= RING)
        def _():
            rs2_copy(k - RING).wait_send()
        b, r = lax.rem(k, RING), lax.rem(k, SLOTS)

        def add(i, c):
            s2[b, rows8(i * eighth, eighth), :] = (s1[b, rows8(a1 * quarter + i * eighth, eighth), :]
                                                   + rs1[r, rows8(i * eighth, eighth), :])
            return c
        lax.fori_loop(0, quarter // eighth, add, 0)
        rs2_copy(k).start()

    def stage_c(k):
        _, _, _, a2 = place(k)
        rs2_copy(k).wait_recv()

        @pl.when(k >= RING)
        def _():
            for i, c in enumerate(fin_copies(k - RING)):
                c.wait() if i == 0 else c.wait_send()
        b, r = lax.rem(k, RING), lax.rem(k, SLOTS)
        fin[b] = s2[b, rows8(a2 * eighth, eighth), :] + rs2[r]
        for c in fin_copies(k):
            c.start()

    def stage_d(k):
        fin_copies(k)[1].wait_recv()

        @pl.when(k >= RING)
        def _():
            for c in fwd_copies(k - RING):
                c.wait_send()
        for c in fwd_copies(k):
            c.start()

    def stage_w(k):
        fin_copies(k)[2].wait_recv()

    def stage_e(k):
        fwd_copies(k)[0].wait_recv()

        @pl.when(k >= RING)
        def _():
            last_copy(k - RING).wait_send()
        last_copy(k).start()

    def stage_f(k):
        fin_copies(k)[3].wait_recv()
        fwd_copies(k)[1].wait_recv()
        last_copy(k).wait_recv()

    nb = tokens // ntp // zrows
    qrows = tokens // ntp

    def zacc(q, b):
        return pl.multiple_of(q * qrows + b * zrows, 8)

    def right_copy(b, i, src=None):
        n = ntp - 1 - i
        s = zout_r.at[lax.rem(b, RING), pl.ds(i, n)] if src is None else src
        return zdma(s, rs_r.at[b, pl.ds(i, n)], zrs_sr.at[lax.rem(b, RING)], zrs_rr.at[b], i + 1)

    def left_copy(b, i):
        return zdma(zout_l.at[lax.rem(b, RING), pl.ds(0, i)], rs_l.at[b, pl.ds(0, i)], zrs_sl.at[lax.rem(b, RING)],
                    zrs_rl.at[b], i - 1)

    def z_right(b):
        for i in range(ntp - 1):
            @pl.when(z == i)
            def _(i=i):
                n = ntp - 1 - i
                if i > 0:
                    right_copy(b, i - 1).wait_recv()
                    load = pltpu.make_async_copy(rs_r.at[b, pl.ds(i, n)], zin_r.at[pl.ds(i, n)], zld.at[0])
                    load.start()
                    load.wait()

                @pl.when(b >= RING)
                def _():
                    right_copy(b - RING, i).wait_send()
                for q in range(i + 1, ntp):
                    mine = acc[pl.ds(zacc(q, b), zrows), :]
                    zout_r[lax.rem(b, RING), q - 1] = mine if i == 0 else zin_r[q - 1] + mine
                right_copy(b, i).start()

    def z_left(b):
        for i in range(1, ntp):
            @pl.when(z == i)
            def _(i=i):
                if i < ntp - 1:
                    left_copy(b, i + 1).wait_recv()
                    load = pltpu.make_async_copy(rs_l.at[b, pl.ds(0, i)], zin_l.at[pl.ds(0, i)], zld.at[0])
                    load.start()
                    load.wait()

                @pl.when(b >= RING)
                def _():
                    left_copy(b - RING, i).wait_send()
                for q in range(i):
                    mine = acc[pl.ds(zacc(q, b), zrows), :]
                    zout_l[lax.rem(b, RING), q] = mine if i == ntp - 1 else zin_l[q] + mine
                left_copy(b, i).start()

    def zfin_copies(b):
        s = lax.rem(b, RING)
        dst = gz.at[rows8(z * qrows + b * zrows, zrows)]
        return (pltpu.make_async_copy(zfin.at[s], dst, zfin_s.at[0, s]),
                zdma(zfin.at[s], dst, zfin_s.at[1, s], zag_rr.at[b, 0], z + 1),
                zdma(zfin.at[s], dst, zfin_s.at[2, s], zag_rl.at[b, 0], z - 1))

    def z_final(b):
        load_h = pltpu.make_async_copy(hidden.at[rows8(z * qrows + b * zrows, zrows)], hbuf, h_sem.at[0])
        load_h.start()
        for i in range(ntp):
            @pl.when(z == i)
            def _(i=i):
                if i > 0:
                    right_copy(b, i - 1).wait_recv() if i == ntp - 1 else None
                    load = pltpu.make_async_copy(rs_r.at[b, i - 1], zin_r.at[i - 1], zld.at[0])
                    load.start()
                    load.wait()
                if i < ntp - 1:
                    left_copy(b, i + 1).wait_recv() if i == 0 else None
                    load = pltpu.make_async_copy(rs_l.at[b, i], zin_l.at[i], zld.at[0])
                    load.start()
                    load.wait()
                z_wait_fin(b - RING, b >= RING)
                total = acc[pl.ds(zacc(i, b), zrows), :]
                if i > 0:
                    total = zin_r[i - 1] + total
                if i < ntp - 1:
                    total = total + zin_l[i]
                zfin[lax.rem(b, RING)] = total
        load_h.wait()
        h = hbuf[...].astype(F32)
        centered = h - jnp.mean(h, axis=-1, keepdims=True)
        rstd = lax.rsqrt(jnp.mean(centered * centered, axis=-1, keepdims=True) + 1e-5)
        unit = centered * rstd
        dy = zfin[lax.rem(b, RING)] * gain[...]
        zfin[lax.rem(b, RING)] = rstd * (dy - jnp.mean(dy, axis=-1, keepdims=True)
                                         - unit * jnp.mean(dy * unit, axis=-1, keepdims=True))
        copies = zfin_copies(b)
        copies[0].start()

        @pl.when(z < ntp - 1)
        def _():
            copies[1].start()

        @pl.when(z > 0)
        def _():
            copies[2].start()

    def z_wait_fin(b, cond):
        @pl.when(cond)
        def _():
            copies = zfin_copies(b)
            copies[0].wait()

            @pl.when(z < ntp - 1)
            def _():
                copies[1].wait_send()

            @pl.when(z > 0)
            def _():
                copies[2].wait_send()

    def zag(b, h, sign, ssem, rsem):
        ref = gz.at[rows8((z - sign * h) * qrows + b * zrows, zrows)]
        return zdma(ref, ref, ssem.at[b, h - 1], rsem.at[b, h], z + sign)

    def z_hop(b, h):
        ref_r = gz.at[rows8((z - h) * qrows + b * zrows, zrows)]
        ref_l = gz.at[rows8((z + h) * qrows + b * zrows, zrows)]

        @pl.when(z >= h)
        def _():
            zdma(ref_r, ref_r, zfw_r.at[b, 0], zag_rr.at[b, h - 1], z).wait_recv()
            if h < ntp - 1:
                @pl.when(z < ntp - 1)
                def _():
                    zag(b, h, 1, zfw_r, zag_rr).start()

        @pl.when(z + h <= ntp - 1)
        def _():
            zdma(ref_l, ref_l, zfw_l.at[b, 0], zag_rl.at[b, h - 1], z).wait_recv()
            if h < ntp - 1:
                @pl.when(z > 0)
                def _():
                    zag(b, h, -1, zfw_l, zag_rl).start()

    lead = min(7, nc)
    g_first = STEPS + 1
    nz, ng = nc * tiles, nc * ntiles
    fast = (tiles * 12) // 7

    def uz(i):
        late = i - lead * STEPS
        return jnp.minimum(lax.div(jnp.minimum(i, lead * STEPS) * tiles + jnp.maximum(late, 0) * fast, STEPS), nz)

    def ug(i):
        return jnp.minimum(lax.div(jnp.maximum(i - g_first, 0) * ntiles, STEPS), ng)

    base = g_first + STEPS
    lags = (('w', base + 16), ('f', base + 26), ('e', base + 22), ('d', base + 12), ('c', base + 8), ('b', base + 5),
            ('a', base + 1), ('p', base))
    stages = {'w': stage_w, 'f': stage_f, 'e': stage_e, 'd': stage_d, 'c': stage_c, 'b': stage_b, 'a': stage_a,
              'p': load_start}
    z_start = lead * STEPS + -(-(nz - lead * tiles) * STEPS // fast)
    hop = 3
    steps = max((nc - 1) * STEPS + base + 27, z_start + nb + hop * 2 * (ntp - 1))
    share_start()
    e_copy(0).start()
    l_copy(0).start()

    def clear(j, carry):
        acc[pl.ds(pl.multiple_of(j * tile, tile), tile), :] = jnp.zeros((tile, d), F32)
        return carry
    lax.fori_loop(0, tiles, clear, 0)
    share_use()

    def one_step(i, carry):
        gk = i - g_first

        @pl.when((gk >= 0) & (gk < nc * STEPS) & (lax.rem(gk, STEPS) == 0))
        def _():
            gl_copy(lax.div(gk, STEPS)).start()
        lax.fori_loop(uz(i), uz(i + 1), z_unit, 0)
        lax.fori_loop(ug(i), ug(i + 1), g_unit, 0)
        for name, lag in lags:
            @pl.when((i >= lag) & (i - lag < nc * STEPS) & (lax.rem(i - lag + STEPS * 64, STEPS) == 0))
            def _(name=name, lag=lag):
                stages[name](lax.div(i - lag, STEPS))
        zt = i - z_start

        @pl.when(valid(zt - hop * z, nb))
        def _():
            z_right(zt - hop * z)

        @pl.when(valid(zt - hop * (ntp - 1 - z), nb))
        def _():
            z_left(zt - hop * (ntp - 1 - z))

        @pl.when(valid(zt - hop * (ntp - 1), nb))
        def _():
            z_final(zt - hop * (ntp - 1))
        for h in range(1, ntp):
            @pl.when(valid(zt - hop * (ntp - 1 + h), nb))
            def _(h=h):
                z_hop(zt - hop * (ntp - 1 + h), h)
        return carry
    lax.fori_loop(0, steps, one_step, 0)

    share_end()

    for k in range(max(nc - RING, 0), nc):
        rs1_copy(k).wait_send()
        rs2_copy(k).wait_send()
        for i, c in enumerate(fin_copies(k)):
            c.wait() if i == 0 else c.wait_send()
        for c in fwd_copies(k):
            c.wait_send()
        last_copy(k).wait_send()
    for b in range(max(nb - RING, 0), nb):
        for i in range(ntp - 1):
            @pl.when(z == i)
            def _(i=i, b=b):
                right_copy(b, i).wait_send()
        for i in range(1, ntp):
            @pl.when(z == i)
            def _(i=i, b=b):
                left_copy(b, i).wait_send()
        z_wait_fin(b, z >= 0)

    def drain(b, carry):
        for h in range(1, ntp - 1):
            @pl.when((z >= h) & (z < ntp - 1))
            def _(h=h):
                zag(b, h, 1, zfw_r, zag_rr).wait_send()

            @pl.when((z + h <= ntp - 1) & (z > 0))
            def _(h=h):
                zag(b, h, -1, zfw_l, zag_rl).wait_send()
        return carry
    lax.fori_loop(0, nb, drain, 0)


def gradients(ntp, ndp, zb, dx, stats, mask, lab, tok, gain, hidden, embed, logits, chunk, tile, zrows):
    tokens, d = zb.shape
    vocab_loc = embed.shape[0]
    nc = vocab_loc // chunk
    half, quarter, eighth = chunk // 2, chunk // 4, chunk // 8
    tiles = tokens // tile
    nb = tokens // ntp // zrows
    vm = pl.BlockSpec(memory_space=pltpu.VMEM)
    hbm = pl.BlockSpec(memory_space=pl.ANY)
    dma = lambda *s: pltpu.SemaphoreType.DMA(s)
    vf = lambda *s: pltpu.VMEM(s, F32)
    sds = lambda *s: jax.ShapeDtypeStruct(s, F32)
    flops = 2 * tokens * d * vocab_loc
    rows = lambda a: a.reshape(tiles, 1, tile)
    res = pl.pallas_call(
        functools.partial(grad_kernel, ntp, ndp, chunk, tile, zrows),
        out_shape=(sds(vocab_loc, d), sds(8, 128), sds(tokens, d), sds(nc, half, d), sds(nc, half, d),
                   sds(nb, ntp - 1, zrows, d), sds(nb, ntp - 1, zrows, d), jax.ShapeDtypeStruct((nc, chunk, tokens), BF16)),
        in_specs=[vm] * 7 + [hbm] * 3,
        out_specs=(hbm, vm) + (hbm,) * 6,
        scratch_shapes=[
            vf(tiles, 1, tile), vf(tiles, 1, tile), vf(ntp, tiles, 8, tile), vf(ndp, 8, 128), vf(ndp, 8, 128),
            vf(2, chunk, tokens),
            pltpu.VMEM((2, chunk, d), BF16), pltpu.VMEM((2, chunk, tokens), BF16), pltpu.VMEM((zrows, d), BF16),
            pltpu.VMEM((chunk, tokens), BF16), pltpu.VMEM((chunk, tokens), BF16),
            vf(tokens, d), vf(chunk, d), vf(half, d), vf(half, d),
            vf(RING, half, d), vf(RING, quarter, d), vf(RING, eighth, d), vf(SLOTS, quarter, d), vf(SLOTS, eighth, d),
            vf(ntp - 1, zrows, d), vf(ntp - 1, zrows, d), vf(RING, ntp - 1, zrows, d), vf(RING, ntp - 1, zrows, d),
            vf(RING, zrows, d),
            dma(ntp - 1), dma(ntp), dma(ndp - 1), dma(ndp), dma(ndp - 1), dma(ndp), dma(2),
            dma(2), dma(2), dma(1), dma(1), dma(1), dma(1), dma(nc), dma(2), dma(RING), dma(SLOTS), dma(RING), dma(SLOTS), dma(4, RING),
            dma(nc), dma(2, nc), dma(3, RING), dma(3, nc),
            dma(1), dma(RING), dma(RING), dma(nb), dma(nb), dma(3, RING), dma(nb, ntp - 1), dma(nb, ntp - 1),
            dma(nb, ntp - 1), dma(nb, ntp - 1),
        ],
        compiler_params=pltpu.CompilerParams(vmem_limit_bytes=VMEM_LIMIT, has_side_effects=True),
        cost_estimate=pl.CostEstimate(flops=3 * flops, bytes_accessed=4 * vocab_loc * (4 * d + tokens),
                                      transcendentals=tokens * vocab_loc),
        name='gradients',
    )(zb, dx, stats, rows(mask), rows(lab), rows(tok), gain, hidden, embed, logits)
    return res[:3]


def solution(mesh):
    ntp, ndp = mesh.shape['tp'], mesh.shape['dp']

    def device_fn(tokens, labels, lossmask, hidden, grad_x0, embed_loc, pos_table, ln_gain, ln_bias):
        vocab_loc, d = embed_loc.shape
        batch, ctx = tokens.shape
        ntok = batch * ctx
        chunk1, chunk, tile, zrows = sizes(ntok, vocab_loc)
        shard_start = lax.axis_index('tp') * vocab_loc
        tok_local = (tokens - shard_start).reshape(1, ntok)
        lab_local = (labels - shard_start).reshape(1, ntok)
        tok_here = (tok_local >= 0) & (tok_local < vocab_loc)
        grad_pos = lax.psum(jnp.sum(grad_x0.astype(F32), axis=0), 'dp')

        hidden2 = hidden.reshape(ntok, d)
        zb, stats, logits, rows = token_stats(hidden2, ln_gain.reshape(1, d), ln_bias.reshape(1, d), lab_local, tok_local,
                                              tok_here, embed_loc, chunk1, tile)
        rows = lax.psum(rows, 'tp').reshape(batch, ctx, d)
        embed_out = (rows + pos_table.astype(F32)[None]).astype(BF16)
        grad_embed, loss, grad_h = gradients(ntp, ndp, zb, grad_x0.reshape(ntok, d), stats, lossmask.astype(F32), lab_local,
                                             tok_local, ln_gain.reshape(1, d), hidden2, embed_loc, logits, chunk, tile, zrows)
        mean_loss = loss[0, 0]
        grad_hidden = grad_h.astype(BF16).reshape(batch, ctx, d)
        return mean_loss, embed_out, grad_hidden, grad_embed, grad_pos

    row_spec = P('dp', None)
    act_spec = P('dp', None, None)
    return jax.shard_map(device_fn, mesh=mesh, in_specs=(row_spec, row_spec, row_spec, act_spec, act_spec, P('tp', None), P(None, None), P(None), P(None)), out_specs=(P(), act_spec, act_spec, P('tp', None), P(None, None)), check_vma=False)
```

```python
import functools

import jax
import jax.numpy as jnp
from jax import lax
from jax.experimental import pallas as pl
from jax.experimental.pallas import tpu as pltpu
from jax.sharding import PartitionSpec as P

MESH = pl.DeviceIdType.MESH
F32 = jnp.float32
BF16 = jnp.bfloat16
NT = (((1,), (1,)), ((), ()))
TN = (((0,), (0,)), ((), ()))
RING = 4
SLOTS = 8
STEPS = 2
VMEM_LIMIT = 66_000_000


def sizes(tokens, vocab_loc):
    if vocab_loc % 448 == 0 and tokens % 1792 == 0:
        return (928 if vocab_loc % 928 == 0 else 448), 448, 256, 32
    return 64, 64, 128, 8


def stats_kernel(chunk, tile, starts, order, skey, hidden, affine, lab, embed, zb, stats, logits_out, rows_out, m_ref, s_ref, l_ref):
    step = pl.program_id(0)
    tokens, d = hidden.shape
    tiles = tokens // tile

    @pl.when(step == 0)
    def _():
        def norm(j, carry):
            rows = pl.ds(pl.multiple_of(j * tile, tile), tile)
            h = hidden[rows, :].astype(F32)
            centered = h - jnp.mean(h, axis=-1, keepdims=True)
            var = jnp.mean(centered * centered, axis=-1, keepdims=True)
            zb[rows, :] = (centered * lax.rsqrt(var + 1e-5) * affine[0:1, :] + affine[1:2, :]).astype(BF16)
            rows_out[rows, :] = jnp.zeros((tile, d), F32)
            return carry
        lax.fori_loop(0, tiles, norm, 0)
        m_ref[...] = jnp.full_like(m_ref, -jnp.inf)
        s_ref[...] = jnp.zeros_like(s_ref)
        l_ref[...] = jnp.zeros_like(l_ref)

    first_tok, end_tok = starts[step], starts[step + 1]

    def token_row(i):
        real = i < end_tok
        i = jnp.where(real, i, 0)
        row = jnp.where(real, skey[i] - step * chunk, 0)
        group = lax.div(row, 16) * 16
        block = embed[pl.ds(pl.multiple_of(group, 16), 16), :].astype(F32)
        pick = lax.broadcasted_iota(jnp.int32, (16, 1), 0) == row - group
        rows_out[pl.ds(jnp.where(real, order[i], tokens), 1), :] = jnp.sum(jnp.where(pick, block, 0.0), axis=0, keepdims=True)

    def more_rows(n, carry):
        for u in range(4):
            token_row(first_tok + n * 4 + u)
        return carry
    lax.fori_loop(0, lax.div(end_tok - first_tok + 3, 4), more_rows, 0)

    ids = lax.broadcasted_iota(jnp.int32, (chunk, tile), 0) + step * chunk

    def product(j):
        cols = slice(j * tile, (j + 1) * tile)
        logits_out[:, cols] = lax.dot_general(embed[...], zb[cols, :], NT, preferred_element_type=F32)

    product(0)
    for j in range(tiles):
        cols = slice(j * tile, (j + 1) * tile)
        if j + 1 < tiles:
            product(j + 1)
        logits = logits_out[:, cols]
        m_old = m_ref[:, cols]
        m_new = jnp.maximum(m_old, jnp.max(logits, axis=0, keepdims=True))
        m_ref[:, cols] = m_new
        s_ref[:, cols] = s_ref[:, cols] * jnp.exp(m_old - m_new) + jnp.sum(jnp.exp(logits - m_new), axis=0, keepdims=True)
        l_ref[:, cols] += jnp.sum(jnp.where(ids == lab[:, cols], logits, 0.0), axis=0, keepdims=True)

    @pl.when(step == pl.num_programs(0) - 1)
    def _():
        for j in range(tiles):
            cols = slice(j * tile, (j + 1) * tile)
            stats[j, 0:1, :] = m_ref[:, cols] + jnp.log(s_ref[:, cols])
            stats[j, 1:2, :] = l_ref[:, cols]
            stats[j, 2:8, :] = jnp.zeros((6, tile), F32)


def token_stats(hidden, affine, lab, tok, here, embed, chunk, tile):
    tokens, d = hidden.shape
    vocab_loc = embed.shape[0]
    steps = vocab_loc // chunk
    key = jnp.where(here, tok, vocab_loc).reshape(tokens)
    skey, order = lax.sort_key_val(key, lax.iota(jnp.int32, tokens))
    bounds = lax.iota(jnp.int32, steps + 1) * chunk
    starts = jnp.sum((key[None, :] < bounds[:, None]).astype(jnp.int32), axis=1)
    whole = pl.BlockSpec(memory_space=pltpu.VMEM)
    return pl.pallas_call(
        functools.partial(stats_kernel, chunk, tile),
        grid_spec=pltpu.PrefetchScalarGridSpec(
            num_scalar_prefetch=3,
            grid=(steps,),
            in_specs=[whole, whole, whole, pl.BlockSpec((chunk, d), lambda i, *_: (i, 0))],
            out_specs=(whole, whole, pl.BlockSpec((chunk, tokens), lambda i, *_: (i, 0)), whole),
            scratch_shapes=[pltpu.VMEM((1, tokens), F32)] * 3),
        out_shape=(jax.ShapeDtypeStruct((tokens, d), BF16), jax.ShapeDtypeStruct((tokens // tile, 8, tile), F32),
                   jax.ShapeDtypeStruct((vocab_loc, tokens), F32), jax.ShapeDtypeStruct((tokens + 8, d), F32)),
        compiler_params=pltpu.CompilerParams(vmem_limit_bytes=VMEM_LIMIT),
        cost_estimate=pl.CostEstimate(flops=2 * tokens * d * vocab_loc, bytes_accessed=2 * embed.size + 4 * vocab_loc * tokens,
                                      transcendentals=tokens * vocab_loc),
        name='token_stats',
    )(starts, order, skey, hidden, affine, lab, embed)


def grad_kernel(ntp, ndp, chunk, tile, zrows,
                dx, stats, mask, lab, tok, affine, zb_hbm, hidden, embed, logits,
                out, loss, gz, own, d2d, rs_r, rs_l, gsave,
                zb, lse, wgt, st_in, cnt_in, loss_in, lbuf, ebuf, gz_t, hbuf, gt, oh, acc, gbuf, ld_own, ld_d2d, s1, s2, fin, rs1, rs2, zin_r, zin_l, zout_r, zout_l, zfin,
                st_s, st_r, cnt_s, cnt_r, loss_s, loss_r, zb_sem, l_sem, e_sem, gs_sem, gl_sem, h_sem, own_sem, d2d_s, d2d_r, ld_sem, rs1_s, rs1_r, rs2_s, rs2_r, fin_s, ag1_r, ag2_r, fwd_s, part_r,
                zld, zrs_sr, zrs_sl, zrs_rr, zrs_rl, zfin_s, zag_rr, zag_rl, zfw_r, zfw_l):
    tokens, d = dx.shape
    vocab_loc = embed.shape[0]
    nc = vocab_loc // chunk
    ncc = nc + 1
    tiles = tokens // tile
    ntile = 256 if d % 256 == 0 and d > 256 else 128
    ntiles = d // ntile
    half, quarter, eighth = chunk // 2, chunk // 4, chunk // 8
    dp, z = lax.axis_index('dp'), lax.axis_index('tp')
    core = lax.rem(dp, 2)
    xpos = lax.rem(lax.div(dp, 2), 2)
    ypos = lax.div(dp, 4)
    partner = dp + 1 - 2 * core
    x_nbr = dp + 2 - 4 * xpos
    y_nbr = dp + 4 - 8 * ypos

    def place(k):
        odd = lax.rem(k, 2)
        n1 = x_nbr + (y_nbr - x_nbr) * odd
        n2 = y_nbr + (x_nbr - y_nbr) * odd
        a1 = xpos + (ypos - xpos) * odd
        a2 = ypos + (xpos - ypos) * odd
        return n1, n2, a1, a2

    def rdma(src, dst, ssem, rsem, dev):
        return pltpu.make_async_remote_copy(src_ref=src, dst_ref=dst, send_sem=ssem, recv_sem=rsem,
                                            device_id={'dp': dev}, device_id_type=MESH)

    def zdma(src, dst, ssem, rsem, dev):
        return pltpu.make_async_remote_copy(src_ref=src, dst_ref=dst, send_sem=ssem, recv_sem=rsem,
                                            device_id={'tp': dev}, device_id_type=MESH)

    def row0(c):
        return lax.rem(c + nc, ncc) * chunk

    def rows8(start, n):
        return pl.ds(pl.multiple_of(start, 8), n)

    def valid(k, limit):
        return (k >= 0) & (k < limit)

    def e_copy(k):
        return pltpu.make_async_copy(embed.at[rows8(k * chunk, chunk)], ebuf.at[lax.rem(k, 2)], e_sem.at[lax.rem(k, 2)])

    def l_copy(k):
        return pltpu.make_async_copy(logits.at[rows8(k * chunk, chunk)], lbuf.at[lax.rem(k, 2)], l_sem.at[lax.rem(k, 2)])

    def gs_copy(k):
        b = lax.rem(k, 2)
        return pltpu.make_async_copy(gz_t.at[b], gsave.at[k], gs_sem.at[b])

    def gl_copy(k):
        return pltpu.make_async_copy(gsave.at[k], gt, gl_sem.at[0])

    def own_copy(k):
        return pltpu.make_async_copy(gbuf.at[rows8(core * half, half)], own.at[k], own_sem.at[0])

    def d2d_copy(k):
        return rdma(gbuf.at[rows8((1 - core) * half, half)], d2d.at[k], d2d_s.at[0], d2d_r.at[k], partner)

    def rs1_copy(k):
        n1, _, a1, _ = place(k)
        b, r = lax.rem(k, RING), lax.rem(k, SLOTS)
        return rdma(s1.at[b, rows8((1 - a1) * quarter, quarter)], rs1.at[r], rs1_s.at[b], rs1_r.at[r], n1)

    def rs2_copy(k):
        _, n2, _, a2 = place(k)
        b, r = lax.rem(k, RING), lax.rem(k, SLOTS)
        return rdma(s2.at[b, rows8((1 - a2) * eighth, eighth)], rs2.at[r], rs2_s.at[b], rs2_r.at[r], n2)

    def fin_copies(k):
        n1, n2, a1, a2 = place(k)
        b = lax.rem(k, RING)
        dst = out.at[rows8(row0(k) + core * half + a1 * quarter + a2 * eighth, eighth)]
        src = fin.at[b]
        return (pltpu.make_async_copy(src, dst, fin_s.at[0, b]),
                rdma(src, dst, fin_s.at[1, b], ag1_r.at[k], n2),
                rdma(src, dst, fin_s.at[2, b], ag2_r.at[0, k], n1),
                rdma(src, dst, fin_s.at[3, b], part_r.at[0, k], partner))

    def fwd_copies(k):
        n1, _, a1, a2 = place(k)
        b = lax.rem(k, RING)
        ref = out.at[rows8(row0(k) + core * half + a1 * quarter + (1 - a2) * eighth, eighth)]
        return (rdma(ref, ref, fwd_s.at[0, b], ag2_r.at[1, k], n1),
                rdma(ref, ref, fwd_s.at[1, b], part_r.at[1, k], partner))

    def last_copy(k):
        _, _, a1, _ = place(k)
        ref = out.at[rows8(row0(k) + core * half + (1 - a1) * quarter, quarter)]
        return rdma(ref, ref, fwd_s.at[2, lax.rem(k, RING)], part_r.at[2, k], partner)

    def peer(i, n, me):
        return lax.rem(me + i, n)

    def st_copy(i, src_of):
        return zdma(st_in.at[z], st_in.at[src_of], st_s.at[i - 1], st_r.at[src_of], peer(i, ntp, z))

    def tile_copy(buf, ssem, rsem, i, src_of):
        return rdma(buf.at[dp], buf.at[src_of], ssem.at[i - 1], rsem.at[src_of], peer(i, ndp, dp))

    def share_start():
        st_in[z] = stats[...]
        for i in range(1, ntp):
            st_copy(i, z).start()
        cnt_in[dp] = jnp.broadcast_to(jnp.sum(jnp.sum(mask[...], axis=0), axis=-1, keepdims=True), (8, 128))
        for i in range(1, ndp):
            tile_copy(cnt_in, cnt_s, cnt_r, i, dp).start()

    def in_order_sum(buf):
        total = buf[0]
        for i in range(1, ndp):
            total = total + buf[i]
        return total[0:1, 0:1]

    def share_use():
        for i in range(1, ndp):
            tile_copy(cnt_in, cnt_s, cnt_r, i, peer(i, ndp, dp)).wait_recv()
        for i in range(1, ntp):
            st_copy(i, peer(i, ntp, z)).wait_recv()
        count = in_order_sum(cnt_in)
        part = jnp.zeros((1, tile), F32)
        for j in range(tiles):
            shard = [st_in[q, j] for q in range(ntp)]
            top = functools.reduce(jnp.maximum, [a[0:1] for a in shard])
            total = functools.reduce(jnp.add, [jnp.exp(a[0:1] - top) for a in shard])
            lse_j = top + jnp.log(total)
            lse[j] = lse_j
            wgt[j] = mask[j] / count
            part = part + mask[j] * (lse_j - functools.reduce(jnp.add, [a[1:2] for a in shard]))
        loss_in[dp] = jnp.broadcast_to(jnp.sum(part, axis=-1, keepdims=True), (8, 128))
        for i in range(1, ndp):
            tile_copy(loss_in, loss_s, loss_r, i, dp).start()

    def share_end():
        for i in range(1, ndp):
            tile_copy(loss_in, loss_s, loss_r, i, peer(i, ndp, dp)).wait_recv()
        loss[...] = jnp.broadcast_to(in_order_sum(loss_in) / in_order_sum(cnt_in), (8, 128))
        for i in range(1, ndp):
            tile_copy(cnt_in, cnt_s, cnt_r, i, dp).wait_send()
            tile_copy(loss_in, loss_s, loss_r, i, dp).wait_send()
        for i in range(1, ntp):
            st_copy(i, z).wait_send()

    zb_copy = pltpu.make_async_copy(zb_hbm, zb, zb_sem.at[0])

    def z_unit(u, carry):
        k, j = lax.div(u, tiles), lax.rem(u, tiles)
        slot = lax.rem(k, 2)

        @pl.when(j == 0)
        def _():
            e_copy(k).wait()
            l_copy(k).wait()

            @pl.when(k + 1 < nc)
            def _():
                e_copy(k + 1).start()
                l_copy(k + 1).start()

            @pl.when(k >= 2)
            def _():
                gs_copy(k - 1).wait()
        cols = pl.ds(pl.multiple_of(j * tile, tile), tile)
        ids = lax.broadcasted_iota(jnp.int32, (chunk, tile), 0) + k * chunk
        hit = jnp.where(ids == lab[j], 1.0, 0.0)
        g = ((jnp.exp(lbuf[slot, :, cols] - lse[j]) - hit) * wgt[j]).astype(BF16)
        gz_t[slot, :, cols] = g
        acc[cols, :] += lax.dot_general(g, ebuf[slot], TN, preferred_element_type=F32)

        @pl.when(j == tiles - 1)
        def _():
            gs_copy(k).start()

            @pl.when((k == 0) | (k == nc - 1))
            def _():
                gs_copy(k).wait()
        return carry

    def g_unit(u, carry):
        k, n = lax.div(u, ntiles), lax.rem(u, ntiles)

        @pl.when(n == 0)
        def _():
            gl_copy(k).start()

            def one_hot(j, c):
                cols = pl.ds(pl.multiple_of(j * tile, tile), tile)
                ids = lax.broadcasted_iota(jnp.int32, (chunk, tile), 0) + k * chunk
                oh[:, cols] = jnp.where(ids == tok[j], 1.0, 0.0).astype(BF16)
                return c
            lax.fori_loop(0, tiles, one_hot, 0)

            own_copy(k).wait()
            d2d_copy(k).wait_send()
            gl_copy(k).wait()

            @pl.when(k == 0)
            def _():
                zb_copy.wait()
        cols = pl.ds(pl.multiple_of(n * ntile, ntile), ntile)
        gbuf[:, cols] = (jnp.dot(gt[...], zb[:, cols], preferred_element_type=F32)
                         + jnp.dot(oh[...], dx[:, cols], preferred_element_type=F32))

        @pl.when(n == ntiles - 1)
        def _():
            own_copy(k + 1).start()
            d2d_copy(k + 1).start()

            @pl.when(k == nc - 1)
            def _():
                own_copy(k + 1).wait()
                d2d_copy(k + 1).wait_send()
        return carry

    def load_start(k):
        d2d_copy(k).wait_recv()
        pltpu.make_async_copy(own.at[k], ld_own, ld_sem.at[0]).start()
        pltpu.make_async_copy(d2d.at[k], ld_d2d, ld_sem.at[1]).start()

    def stage_a(k):
        pltpu.make_async_copy(own.at[k], ld_own, ld_sem.at[0]).wait()
        pltpu.make_async_copy(d2d.at[k], ld_d2d, ld_sem.at[1]).wait()

        @pl.when(k >= RING)
        def _():
            rs1_copy(k - RING).wait_send()
        b = lax.rem(k, RING)

        def add(i, c):
            r = rows8(i * eighth, eighth)
            s1[b, r, :] = ld_own[r, :] + ld_d2d[r, :]
            return c
        lax.fori_loop(0, half // eighth, add, 0)
        rs1_copy(k).start()

    def stage_b(k):
        _, _, a1, _ = place(k)
        rs1_copy(k).wait_recv()

        @pl.when(k >= RING)
        def _():
            rs2_copy(k - RING).wait_send()
        b, r = lax.rem(k, RING), lax.rem(k, SLOTS)

        def add(i, c):
            s2[b, rows8(i * eighth, eighth), :] = (s1[b, rows8(a1 * quarter + i * eighth, eighth), :]
                                                   + rs1[r, rows8(i * eighth, eighth), :])
            return c
        lax.fori_loop(0, quarter // eighth, add, 0)
        rs2_copy(k).start()

    def stage_c(k):
        _, _, _, a2 = place(k)
        rs2_copy(k).wait_recv()

        @pl.when(k >= RING)
        def _():
            for i, c in enumerate(fin_copies(k - RING)):
                c.wait() if i == 0 else c.wait_send()
        b, r = lax.rem(k, RING), lax.rem(k, SLOTS)
        fin[b] = s2[b, rows8(a2 * eighth, eighth), :] + rs2[r]
        for c in fin_copies(k):
            c.start()

    def stage_d(k):
        fin_copies(k)[1].wait_recv()

        @pl.when(k >= RING)
        def _():
            for c in fwd_copies(k - RING):
                c.wait_send()
        for c in fwd_copies(k):
            c.start()

    def stage_w(k):
        fin_copies(k)[2].wait_recv()

    def stage_e(k):
        fwd_copies(k)[0].wait_recv()

        @pl.when(k >= RING)
        def _():
            last_copy(k - RING).wait_send()
        last_copy(k).start()

    def stage_f(k):
        fin_copies(k)[3].wait_recv()
        fwd_copies(k)[1].wait_recv()
        last_copy(k).wait_recv()

    nb = tokens // ntp // zrows
    qrows = tokens // ntp

    def zacc(q, b):
        return pl.multiple_of(q * qrows + b * zrows, 8)

    def right_copy(b, i, src=None):
        n = ntp - 1 - i
        s = zout_r.at[lax.rem(b, RING), pl.ds(i, n)] if src is None else src
        return zdma(s, rs_r.at[b, pl.ds(i, n)], zrs_sr.at[lax.rem(b, RING)], zrs_rr.at[b], i + 1)

    def left_copy(b, i):
        return zdma(zout_l.at[lax.rem(b, RING), pl.ds(0, i)], rs_l.at[b, pl.ds(0, i)], zrs_sl.at[lax.rem(b, RING)],
                    zrs_rl.at[b], i - 1)

    def z_right(b):
        for i in range(ntp - 1):
            @pl.when(z == i)
            def _(i=i):
                n = ntp - 1 - i
                if i > 0:
                    right_copy(b, i - 1).wait_recv()
                    load = pltpu.make_async_copy(rs_r.at[b, pl.ds(i, n)], zin_r.at[pl.ds(i, n)], zld.at[0])
                    load.start()
                    load.wait()

                @pl.when(b >= RING)
                def _():
                    right_copy(b - RING, i).wait_send()
                for q in range(i + 1, ntp):
                    mine = acc[pl.ds(zacc(q, b), zrows), :]
                    zout_r[lax.rem(b, RING), q - 1] = mine if i == 0 else zin_r[q - 1] + mine
                right_copy(b, i).start()

    def z_left(b):
        for i in range(1, ntp):
            @pl.when(z == i)
            def _(i=i):
                if i < ntp - 1:
                    left_copy(b, i + 1).wait_recv()
                    load = pltpu.make_async_copy(rs_l.at[b, pl.ds(0, i)], zin_l.at[pl.ds(0, i)], zld.at[0])
                    load.start()
                    load.wait()

                @pl.when(b >= RING)
                def _():
                    left_copy(b - RING, i).wait_send()
                for q in range(i):
                    mine = acc[pl.ds(zacc(q, b), zrows), :]
                    zout_l[lax.rem(b, RING), q] = mine if i == ntp - 1 else zin_l[q] + mine
                left_copy(b, i).start()

    def zfin_copies(b):
        s = lax.rem(b, RING)
        dst = gz.at[rows8(z * qrows + b * zrows, zrows)]
        return (pltpu.make_async_copy(zfin.at[s], dst, zfin_s.at[0, s]),
                zdma(zfin.at[s], dst, zfin_s.at[1, s], zag_rr.at[b, 0], z + 1),
                zdma(zfin.at[s], dst, zfin_s.at[2, s], zag_rl.at[b, 0], z - 1))

    def z_final(b):
        load_h = pltpu.make_async_copy(hidden.at[rows8(z * qrows + b * zrows, zrows)], hbuf, h_sem.at[0])
        load_h.start()
        for i in range(ntp):
            @pl.when(z == i)
            def _(i=i):
                if i > 0:
                    right_copy(b, i - 1).wait_recv() if i == ntp - 1 else None
                    load = pltpu.make_async_copy(rs_r.at[b, i - 1], zin_r.at[i - 1], zld.at[0])
                    load.start()
                    load.wait()
                if i < ntp - 1:
                    left_copy(b, i + 1).wait_recv() if i == 0 else None
                    load = pltpu.make_async_copy(rs_l.at[b, i], zin_l.at[i], zld.at[0])
                    load.start()
                    load.wait()
                z_wait_fin(b - RING, b >= RING)
                total = acc[pl.ds(zacc(i, b), zrows), :]
                if i > 0:
                    total = zin_r[i - 1] + total
                if i < ntp - 1:
                    total = total + zin_l[i]
                zfin[lax.rem(b, RING)] = total
        load_h.wait()
        h = hbuf[...].astype(F32)
        centered = h - jnp.mean(h, axis=-1, keepdims=True)
        rstd = lax.rsqrt(jnp.mean(centered * centered, axis=-1, keepdims=True) + 1e-5)
        unit = centered * rstd
        dy = zfin[lax.rem(b, RING)] * affine[0:1, :]
        zfin[lax.rem(b, RING)] = rstd * (dy - jnp.mean(dy, axis=-1, keepdims=True)
                                         - unit * jnp.mean(dy * unit, axis=-1, keepdims=True))
        copies = zfin_copies(b)
        copies[0].start()

        @pl.when(z < ntp - 1)
        def _():
            copies[1].start()

        @pl.when(z > 0)
        def _():
            copies[2].start()

    def z_wait_fin(b, cond):
        @pl.when(cond)
        def _():
            copies = zfin_copies(b)
            copies[0].wait()

            @pl.when(z < ntp - 1)
            def _():
                copies[1].wait_send()

            @pl.when(z > 0)
            def _():
                copies[2].wait_send()

    def zag(b, h, sign, ssem, rsem):
        ref = gz.at[rows8((z - sign * h) * qrows + b * zrows, zrows)]
        return zdma(ref, ref, ssem.at[b, h - 1], rsem.at[b, h], z + sign)

    def z_hop(b, h):
        ref_r = gz.at[rows8((z - h) * qrows + b * zrows, zrows)]
        ref_l = gz.at[rows8((z + h) * qrows + b * zrows, zrows)]

        @pl.when(z >= h)
        def _():
            zdma(ref_r, ref_r, zfw_r.at[b, 0], zag_rr.at[b, h - 1], z).wait_recv()
            if h < ntp - 1:
                @pl.when(z < ntp - 1)
                def _():
                    zag(b, h, 1, zfw_r, zag_rr).start()

        @pl.when(z + h <= ntp - 1)
        def _():
            zdma(ref_l, ref_l, zfw_l.at[b, 0], zag_rl.at[b, h - 1], z).wait_recv()
            if h < ntp - 1:
                @pl.when(z > 0)
                def _():
                    zag(b, h, -1, zfw_l, zag_rl).start()

    lead, g_first = 10, STEPS
    nz, ng = nc * tiles, nc * ntiles
    fast = (tiles * 12) // 7

    def uz(i):
        late = jnp.maximum(i - 1 - lead, 0)
        count = tiles + 1 + lax.div(jnp.minimum(i - 1, lead) * tiles + late * fast, STEPS)
        return jnp.where(i <= 0, 0, jnp.minimum(count, nz))

    def ug(i):
        return jnp.where(i <= 0, 0, jnp.minimum(ntiles + lax.div(jnp.maximum(i - g_first, 0) * ntiles, STEPS), ng))

    lags = (('p', 0), ('a', 1), ('b', 4), ('c', 6), ('d', 10), ('w', 16), ('e', 16), ('f', 24))
    stages = {'w': stage_w, 'f': stage_f, 'e': stage_e, 'd': stage_d, 'c': stage_c, 'b': stage_b, 'a': stage_a,
              'p': load_start}
    z_start = lead + -(-max(nz - (tiles + 1 + lead * tiles // STEPS), 0) * STEPS // fast)
    hop = 4
    steps = max((ncc - 1) * STEPS + 25, z_start + nb + hop * 2 * (ntp - 1))
    share_start()
    zb_copy.start()
    e_copy(0).start()
    l_copy(0).start()

    def pos_rows(j, carry):
        total = dx[rows8(j * eighth, eighth), :].astype(F32)
        for b in range(1, tokens // chunk):
            total = total + dx[pl.ds(pl.multiple_of(b * chunk + j * eighth, 8), eighth), :].astype(F32)
        gbuf[rows8(j * eighth, eighth), :] = total
        return carry
    lax.fori_loop(0, 8, pos_rows, 0)
    own_copy(0).start()
    d2d_copy(0).start()

    def clear(j, carry):
        acc[pl.ds(pl.multiple_of(j * tile, tile), tile), :] = jnp.zeros((tile, d), F32)
        return carry
    lax.fori_loop(0, tiles, clear, 0)
    share_use()

    def one_step(i, carry):
        lax.fori_loop(uz(i), uz(i + 1), z_unit, 0)
        lax.fori_loop(ug(i), ug(i + 1), g_unit, 0)
        for name, lag in lags:
            @pl.when((i >= lag) & (i - lag < ncc * STEPS) & (lax.rem(i - lag + STEPS * 64, STEPS) == 0))
            def _(name=name, lag=lag):
                stages[name](lax.div(i - lag, STEPS))
        zt = i - z_start

        @pl.when(valid(zt - hop * z, nb))
        def _():
            z_right(zt - hop * z)

        @pl.when(valid(zt - hop * (ntp - 1 - z), nb))
        def _():
            z_left(zt - hop * (ntp - 1 - z))

        @pl.when(valid(zt - hop * (ntp - 1), nb))
        def _():
            z_final(zt - hop * (ntp - 1))
        for h in range(1, ntp):
            @pl.when(valid(zt - hop * (ntp - 1 + h), nb))
            def _(h=h):
                z_hop(zt - hop * (ntp - 1 + h), h)
        return carry
    lax.fori_loop(0, steps, one_step, 0)

    share_end()

    for k in range(max(ncc - RING, 0), ncc):
        rs1_copy(k).wait_send()
        rs2_copy(k).wait_send()
        for i, c in enumerate(fin_copies(k)):
            c.wait() if i == 0 else c.wait_send()
        for c in fwd_copies(k):
            c.wait_send()
        last_copy(k).wait_send()
    for b in range(max(nb - RING, 0), nb):
        for i in range(ntp - 1):
            @pl.when(z == i)
            def _(i=i, b=b):
                right_copy(b, i).wait_send()
        for i in range(1, ntp):
            @pl.when(z == i)
            def _(i=i, b=b):
                left_copy(b, i).wait_send()
        z_wait_fin(b, z >= 0)

    def drain(b, carry):
        for h in range(1, ntp - 1):
            @pl.when((z >= h) & (z < ntp - 1))
            def _(h=h):
                zag(b, h, 1, zfw_r, zag_rr).wait_send()

            @pl.when((z + h <= ntp - 1) & (z > 0))
            def _(h=h):
                zag(b, h, -1, zfw_l, zag_rl).wait_send()
        return carry
    lax.fori_loop(0, nb, drain, 0)


def gradients(ntp, ndp, zb, dx, stats, mask, lab, tok, affine, hidden, embed, logits, chunk, tile, zrows):
    tokens, d = zb.shape
    vocab_loc = embed.shape[0]
    nc = vocab_loc // chunk
    ncc = nc + 1
    half, quarter, eighth = chunk // 2, chunk // 4, chunk // 8
    tiles = tokens // tile
    nb = tokens // ntp // zrows
    vm = pl.BlockSpec(memory_space=pltpu.VMEM)
    hbm = pl.BlockSpec(memory_space=pl.ANY)
    dma = lambda *s: pltpu.SemaphoreType.DMA(s)
    vf = lambda *s: pltpu.VMEM(s, F32)
    sds = lambda *s: jax.ShapeDtypeStruct(s, F32)
    flops = 2 * tokens * d * vocab_loc
    rows = lambda a: a.reshape(tiles, 1, tile)
    res = pl.pallas_call(
        functools.partial(grad_kernel, ntp, ndp, chunk, tile, zrows),
        out_shape=(sds(vocab_loc + chunk, d), sds(8, 128), sds(tokens, d), sds(ncc, half, d), sds(ncc, half, d),
                   sds(nb, ntp - 1, zrows, d), sds(nb, ntp - 1, zrows, d), jax.ShapeDtypeStruct((nc, chunk, tokens), BF16)),
        in_specs=[vm] * 6 + [hbm] * 4,
        out_specs=(hbm, vm) + (hbm,) * 6,
        scratch_shapes=[
            pltpu.VMEM((tokens, d), BF16), vf(tiles, 1, tile), vf(tiles, 1, tile), vf(ntp, tiles, 8, tile), vf(ndp, 8, 128), vf(ndp, 8, 128),
            vf(2, chunk, tokens),
            pltpu.VMEM((2, chunk, d), BF16), pltpu.VMEM((2, chunk, tokens), BF16), pltpu.VMEM((zrows, d), BF16),
            pltpu.VMEM((chunk, tokens), BF16), pltpu.VMEM((chunk, tokens), BF16),
            vf(tokens, d), vf(chunk, d), vf(half, d), vf(half, d),
            vf(RING, half, d), vf(RING, quarter, d), vf(RING, eighth, d), vf(SLOTS, quarter, d), vf(SLOTS, eighth, d),
            vf(ntp - 1, zrows, d), vf(ntp - 1, zrows, d), vf(RING, ntp - 1, zrows, d), vf(RING, ntp - 1, zrows, d),
            vf(RING, zrows, d),
            dma(ntp - 1), dma(ntp), dma(ndp - 1), dma(ndp), dma(ndp - 1), dma(ndp), dma(1), dma(2),
            dma(2), dma(2), dma(1), dma(1), dma(1), dma(1), dma(ncc), dma(2), dma(RING), dma(SLOTS), dma(RING), dma(SLOTS), dma(4, RING),
            dma(ncc), dma(2, ncc), dma(3, RING), dma(3, ncc),
            dma(1), dma(RING), dma(RING), dma(nb), dma(nb), dma(3, RING), dma(nb, ntp - 1), dma(nb, ntp - 1),
            dma(nb, ntp - 1), dma(nb, ntp - 1),
        ],
        compiler_params=pltpu.CompilerParams(vmem_limit_bytes=VMEM_LIMIT, has_side_effects=True),
        cost_estimate=pl.CostEstimate(flops=3 * flops, bytes_accessed=4 * vocab_loc * (4 * d + tokens),
                                      transcendentals=tokens * vocab_loc),
        name='gradients',
    )(dx, stats, rows(mask), rows(lab), rows(tok), affine, zb, hidden, embed, logits)
    return res[:3]


def finish_kernel(grad_in, pos_in, rows, gh_in, pos_table, grad_out, pos_out, embed_out, gh_out):
    grad_out[...] = grad_in[...]
    pos_out[...] = pos_in[...]
    embed_out[...] = (rows[...] + pos_table[...].astype(F32)).astype(BF16)
    gh_out[...] = gh_in[...].astype(BF16)


def finish(grads, rows, grad_h, pos_table, vocab_loc):
    tokens, d = grad_h.shape
    ctx = pos_table.shape[0]
    n = tokens // 64
    big, mid, small = vocab_loc // n, 64, ctx // n
    at = lambda r, f=lambda i: i: pl.BlockSpec((r, d), lambda i: (f(i), 0))
    return pl.pallas_call(
        finish_kernel,
        grid=(n,),
        in_specs=[at(big), at(small, lambda i: vocab_loc // small + i), at(mid), at(mid), at(mid, lambda i: lax.rem(i, ctx // mid))],
        out_specs=(at(big), at(small), at(mid), at(mid)),
        out_shape=(jax.ShapeDtypeStruct((vocab_loc, d), F32), jax.ShapeDtypeStruct((ctx, d), F32),
                   jax.ShapeDtypeStruct((tokens, d), BF16), jax.ShapeDtypeStruct((tokens, d), BF16)),
        compiler_params=pltpu.CompilerParams(vmem_limit_bytes=VMEM_LIMIT),
        cost_estimate=pl.CostEstimate(flops=tokens * d, bytes_accessed=8 * vocab_loc * d, transcendentals=0),
        name='finish',
    )(grads, grads, rows, grad_h, pos_table)


def solution(mesh):
    ntp, ndp = mesh.shape['tp'], mesh.shape['dp']

    def device_fn(tokens, labels, lossmask, hidden, grad_x0, embed_loc, pos_table, ln_gain, ln_bias):
        vocab_loc, d = embed_loc.shape
        batch, ctx = tokens.shape
        ntok = batch * ctx
        chunk1, chunk, tile, zrows = sizes(ntok, vocab_loc)
        shard_start = lax.axis_index('tp') * vocab_loc
        tok_local = (tokens - shard_start).reshape(1, ntok)
        lab_local = (labels - shard_start).reshape(1, ntok)
        tok_here = (tok_local >= 0) & (tok_local < vocab_loc)
        hidden2 = hidden.reshape(ntok, d)
        affine = jnp.stack([ln_gain, ln_bias])
        zb, stats, logits, rows = token_stats(hidden2, affine, lab_local, tok_local, tok_here, embed_loc, chunk1, tile)
        rows = lax.psum(rows, 'tp')
        grads, loss, grad_h = gradients(ntp, ndp, zb, grad_x0.reshape(ntok, d), stats, lossmask.astype(F32), lab_local,
                                        tok_local, affine, hidden2, embed_loc, logits, chunk, tile, zrows)
        grad_embed, grad_pos, embed_out, grad_hidden = finish(grads, rows, grad_h, pos_table, vocab_loc)
        mean_loss = loss[0, 0]
        embed_out = embed_out.reshape(batch, ctx, d)
        grad_hidden = grad_hidden.reshape(batch, ctx, d)
        return mean_loss, embed_out, grad_hidden, grad_embed, grad_pos

    row_spec = P('dp', None)
    act_spec = P('dp', None, None)
    return jax.shard_map(device_fn, mesh=mesh, in_specs=(row_spec, row_spec, row_spec, act_spec, act_spec, P('tp', None), P(None, None), P(None), P(None)), out_specs=(P(), act_spec, act_spec, P('tp', None), P(None, None)), check_vma=False)
```

```python
import functools

import jax
import jax.numpy as jnp
from jax import lax
from jax.experimental import pallas as pl
from jax.experimental.pallas import tpu as pltpu
from jax.sharding import PartitionSpec as P

MESH = pl.DeviceIdType.MESH
F32 = jnp.float32
BF16 = jnp.bfloat16
NT = (((1,), (1,)), ((), ()))
RING = 4
SLOTS = 8
STEPS = 2
VMEM_LIMIT = 66_000_000


def sizes(tokens, vocab_loc):
    if vocab_loc % 448 == 0 and tokens % 1792 == 0:
        return (928 if vocab_loc % 928 == 0 else 448), 448, 256, 32
    return 64, 64, 128, 8


def stats_kernel(chunk, tile, ctx, starts, order, skey, hidden, affine, lab, dx, embed,
                 zb, stats, logits_out, rows_out, scatter, pos, m_ref, s_ref, l_ref, dx_f32, dx_in, dx_sem):
    step = pl.program_id(0)
    tokens, d = hidden.shape
    tiles = tokens // tile

    @pl.when(step == 0)
    def _():
        def dx_copy(j):
            rows = pl.ds(pl.multiple_of(j * tile, tile), tile)
            return pltpu.make_async_copy(dx.at[rows], dx_in.at[lax.rem(j, 2)], dx_sem.at[lax.rem(j, 2)])
        dx_copy(0).start()

        def norm(j, carry):
            rows = pl.ds(pl.multiple_of(j * tile, tile), tile)
            dx_copy(j).wait()

            @pl.when(j + 1 < tiles)
            def _():
                dx_copy(j + 1).start()
            dx_f32[rows, :] = dx_in[lax.rem(j, 2)].astype(F32)
            h = hidden[rows, :].astype(F32)
            centered = h - jnp.mean(h, axis=-1, keepdims=True)
            var = jnp.mean(centered * centered, axis=-1, keepdims=True)
            zb[rows, :] = (centered * lax.rsqrt(var + 1e-5) * affine[0:1, :] + affine[1:2, :]).astype(BF16)
            rows_out[rows, :] = jnp.zeros((tile, d), F32)
            return carry
        lax.fori_loop(0, tiles, norm, 0)

        def pos_rows(j, carry):
            n = ctx // 8
            pos[pl.ds(pl.multiple_of(j * n, 8), n), :] = functools.reduce(jnp.add, [
                dx_f32[pl.ds(pl.multiple_of(b * ctx + j * n, 8), n), :] for b in range(tokens // ctx)])
            return carry
        lax.fori_loop(0, 8, pos_rows, 0)
        m_ref[...] = jnp.full_like(m_ref, -jnp.inf)
        s_ref[...] = jnp.zeros_like(s_ref)
        l_ref[...] = jnp.zeros_like(l_ref)

    ids = lax.broadcasted_iota(jnp.int32, (chunk, tile), 0) + step * chunk

    def product(j):
        cols = slice(j * tile, (j + 1) * tile)
        logits_out[:, cols] = lax.dot_general(embed[...], zb[cols, :], NT, preferred_element_type=F32)

    product(0)
    band = -(-chunk // tiles // 8) * 8
    for j in range(tiles):
        cols = slice(j * tile, (j + 1) * tile)
        if j + 1 < tiles:
            product(j + 1)
        if j * band < chunk:
            scatter[j * band:min((j + 1) * band, chunk), :] = jnp.zeros((min(band, chunk - j * band), d), F32)
        logits = logits_out[:, cols]
        m_old = m_ref[:, cols]
        m_new = jnp.maximum(m_old, jnp.max(logits, axis=0, keepdims=True))
        m_ref[:, cols] = m_new
        s_ref[:, cols] = s_ref[:, cols] * jnp.exp(m_old - m_new) + jnp.sum(jnp.exp(logits - m_new), axis=0, keepdims=True)
        l_ref[:, cols] += jnp.sum(jnp.where(ids == lab[:, cols], logits, 0.0), axis=0, keepdims=True)

    first_tok, end_tok = starts[step], starts[step + 1]

    def token_row(i):
        real = i < end_tok
        i = jnp.where(real, i, 0)
        row = jnp.where(real, skey[i] - step * chunk, 0)
        group = lax.div(row, 16) * 16
        block = embed[pl.ds(pl.multiple_of(group, 16), 16), :].astype(F32)
        pick = lax.broadcasted_iota(jnp.int32, (16, 1), 0) == row - group
        rows_out[pl.ds(jnp.where(real, order[i], tokens), 1), :] = jnp.sum(jnp.where(pick, block, 0.0), axis=0, keepdims=True)
        scatter[pl.ds(row, 1), :] += jnp.where(real, dx_f32[pl.ds(order[i], 1), :], 0.0)

    def token_rows(n, carry):
        for u in range(4):
            token_row(first_tok + n * 4 + u)
        return carry
    lax.fori_loop(0, lax.div(end_tok - first_tok + 3, 4), token_rows, 0)

    @pl.when(step == pl.num_programs(0) - 1)
    def _():
        for j in range(tiles):
            cols = slice(j * tile, (j + 1) * tile)
            stats[j, 0:1, :] = m_ref[:, cols] + jnp.log(s_ref[:, cols])
            stats[j, 1:2, :] = l_ref[:, cols]
            stats[j, 2:8, :] = jnp.zeros((6, tile), F32)


def token_stats(hidden, affine, lab, tok, here, dx, embed, chunk, tile, ctx):
    tokens, d = hidden.shape
    vocab_loc = embed.shape[0]
    steps = vocab_loc // chunk
    key = jnp.where(here, tok, vocab_loc).reshape(tokens)
    skey, order = lax.sort_key_val(key, lax.iota(jnp.int32, tokens))
    bounds = lax.iota(jnp.int32, steps + 1) * chunk
    starts = jnp.sum((key[None, :] < bounds[:, None]).astype(jnp.int32), axis=1)
    whole = pl.BlockSpec(memory_space=pltpu.VMEM)
    return pl.pallas_call(
        functools.partial(stats_kernel, chunk, tile, ctx),
        grid_spec=pltpu.PrefetchScalarGridSpec(
            num_scalar_prefetch=3,
            grid=(steps,),
            in_specs=[whole, whole, whole, pl.BlockSpec(memory_space=pl.ANY), pl.BlockSpec((chunk, d), lambda i, *_: (i, 0))],
            out_specs=(whole, whole, pl.BlockSpec((chunk, tokens), lambda i, *_: (i, 0)), whole,
                       pl.BlockSpec((chunk, d), lambda i, *_: (i, 0)), whole),
            scratch_shapes=[pltpu.VMEM((1, tokens), F32)] * 3 + [pltpu.VMEM((tokens, d), F32), pltpu.VMEM((2, tile, d), BF16),
                                                               pltpu.SemaphoreType.DMA((2,))]),
        out_shape=(jax.ShapeDtypeStruct((tokens, d), BF16), jax.ShapeDtypeStruct((tokens // tile, 8, tile), F32),
                   jax.ShapeDtypeStruct((vocab_loc, tokens), F32), jax.ShapeDtypeStruct((tokens + 8, d), F32),
                   jax.ShapeDtypeStruct((vocab_loc, d), F32), jax.ShapeDtypeStruct((ctx, d), F32)),
        compiler_params=pltpu.CompilerParams(vmem_limit_bytes=VMEM_LIMIT),
        cost_estimate=pl.CostEstimate(flops=2 * tokens * d * vocab_loc, bytes_accessed=6 * embed.size + 4 * vocab_loc * tokens,
                                      transcendentals=tokens * vocab_loc),
        name='token_stats',
    )(starts, order, skey, hidden, affine, lab, dx, embed)


def grad_kernel(ntp, ndp, chunk, tile, zrows,
                stats, mask, lab, affine, zb_hbm, hidden, embed, logits, scatter, pos,
                out, loss, gz, own, d2d, rs_r, rs_l, gsave,
                zb, lse, wgt, st_in, cnt_in, loss_in, lbuf, ebuf, gz_t, gtile, hbuf, gt, sbuf, acc, gbuf, ld_own, ld_d2d, s1, s2, fin, rs1, rs2, zin_r, zin_l, zout_r, zout_l, zfin,
                st_s, st_r, cnt_s, cnt_r, loss_s, loss_r, zb_sem, l_sem, e_sem, gs_sem, gl_sem, h_sem, s_sem, own_sem, d2d_s, d2d_r, ld_sem, rs1_s, rs1_r, rs2_s, rs2_r, fin_s, ag1_r, ag2_r, fwd_s, part_r,
                zld, zrs_sr, zrs_sl, zrs_rr, zrs_rl, zfin_s, zag_rr, zag_rl, zfw_r, zfw_l):
    tokens, d = zb_hbm.shape
    vocab_loc = embed.shape[0]
    nc = vocab_loc // chunk
    ncc = nc + 1
    tiles = tokens // tile
    ntile = 256 if d % 256 == 0 and d > 256 else 128
    ntiles = d // ntile
    half, quarter, eighth = chunk // 2, chunk // 4, chunk // 8
    dp, z = lax.axis_index('dp'), lax.axis_index('tp')
    core = lax.rem(dp, 2)
    xpos = lax.rem(lax.div(dp, 2), 2)
    ypos = lax.div(dp, 4)
    partner = dp + 1 - 2 * core
    x_nbr = dp + 2 - 4 * xpos
    y_nbr = dp + 4 - 8 * ypos

    def place(k):
        odd = lax.rem(k, 2)
        n1 = x_nbr + (y_nbr - x_nbr) * odd
        n2 = y_nbr + (x_nbr - y_nbr) * odd
        a1 = xpos + (ypos - xpos) * odd
        a2 = ypos + (xpos - ypos) * odd
        return n1, n2, a1, a2

    def rdma(src, dst, ssem, rsem, dev):
        return pltpu.make_async_remote_copy(src_ref=src, dst_ref=dst, send_sem=ssem, recv_sem=rsem,
                                            device_id={'dp': dev}, device_id_type=MESH)

    def zdma(src, dst, ssem, rsem, dev):
        return pltpu.make_async_remote_copy(src_ref=src, dst_ref=dst, send_sem=ssem, recv_sem=rsem,
                                            device_id={'tp': dev}, device_id_type=MESH)

    def row0(c):
        return lax.rem(c + nc, ncc) * chunk

    def rows8(start, n):
        return pl.ds(pl.multiple_of(start, 8), n)

    def valid(k, limit):
        return (k >= 0) & (k < limit)

    def e_copy(k):
        return pltpu.make_async_copy(embed.at[rows8(k * chunk, chunk)], ebuf.at[lax.rem(k, 2)], e_sem.at[lax.rem(k, 2)])

    def l_copy(k):
        return pltpu.make_async_copy(logits.at[rows8(k * chunk, chunk)], lbuf.at[lax.rem(k, 2)], l_sem.at[lax.rem(k, 2)])

    def gs_copy(k):
        b = lax.rem(k, 2)
        return pltpu.make_async_copy(gz_t.at[b], gsave.at[k], gs_sem.at[b])

    def gl_copy(k):
        return pltpu.make_async_copy(gsave.at[k], gt, gl_sem.at[0])

    def own_copy(k):
        return pltpu.make_async_copy(gbuf.at[rows8(core * half, half)], own.at[k], own_sem.at[0])

    def d2d_copy(k):
        return rdma(gbuf.at[rows8((1 - core) * half, half)], d2d.at[k], d2d_s.at[0], d2d_r.at[k], partner)

    def rs1_copy(k):
        n1, _, a1, _ = place(k)
        b, r = lax.rem(k, RING), lax.rem(k, SLOTS)
        return rdma(s1.at[b, rows8((1 - a1) * quarter, quarter)], rs1.at[r], rs1_s.at[b], rs1_r.at[r], n1)

    def rs2_copy(k):
        _, n2, _, a2 = place(k)
        b, r = lax.rem(k, RING), lax.rem(k, SLOTS)
        return rdma(s2.at[b, rows8((1 - a2) * eighth, eighth)], rs2.at[r], rs2_s.at[b], rs2_r.at[r], n2)

    def fin_copies(k):
        n1, n2, a1, a2 = place(k)
        b = lax.rem(k, RING)
        dst = out.at[rows8(row0(k) + core * half + a1 * quarter + a2 * eighth, eighth)]
        src = fin.at[b]
        return (pltpu.make_async_copy(src, dst, fin_s.at[0, b]),
                rdma(src, dst, fin_s.at[1, b], ag1_r.at[k], n2),
                rdma(src, dst, fin_s.at[2, b], ag2_r.at[0, k], n1),
                rdma(src, dst, fin_s.at[3, b], part_r.at[0, k], partner))

    def fwd_copies(k):
        n1, _, a1, a2 = place(k)
        b = lax.rem(k, RING)
        ref = out.at[rows8(row0(k) + core * half + a1 * quarter + (1 - a2) * eighth, eighth)]
        return (rdma(ref, ref, fwd_s.at[0, b], ag2_r.at[1, k], n1),
                rdma(ref, ref, fwd_s.at[1, b], part_r.at[1, k], partner))

    def last_copy(k):
        _, _, a1, _ = place(k)
        ref = out.at[rows8(row0(k) + core * half + (1 - a1) * quarter, quarter)]
        return rdma(ref, ref, fwd_s.at[2, lax.rem(k, RING)], part_r.at[2, k], partner)

    def peer(i, n, me):
        return lax.rem(me + i, n)

    def st_copy(i, src_of):
        return zdma(st_in.at[z], st_in.at[src_of], st_s.at[i - 1], st_r.at[src_of], peer(i, ntp, z))

    def tile_copy(buf, ssem, rsem, i, src_of):
        return rdma(buf.at[dp], buf.at[src_of], ssem.at[i - 1], rsem.at[src_of], peer(i, ndp, dp))

    def share_start():
        st_in[z] = stats[...]
        for i in range(1, ntp):
            st_copy(i, z).start()
        cnt_in[dp] = jnp.broadcast_to(jnp.sum(jnp.sum(mask[...], axis=0), axis=-1, keepdims=True), (8, 128))
        for i in range(1, ndp):
            tile_copy(cnt_in, cnt_s, cnt_r, i, dp).start()

    def in_order_sum(buf):
        total = buf[0]
        for i in range(1, ndp):
            total = total + buf[i]
        return total[0:1, 0:1]

    def share_use():
        for i in range(1, ndp):
            tile_copy(cnt_in, cnt_s, cnt_r, i, peer(i, ndp, dp)).wait_recv()
        for i in range(1, ntp):
            st_copy(i, peer(i, ntp, z)).wait_recv()
        count = in_order_sum(cnt_in)
        part = jnp.zeros((1, tile), F32)
        for j in range(tiles):
            shard = [st_in[q, j] for q in range(ntp)]
            top = functools.reduce(jnp.maximum, [a[0:1] for a in shard])
            total = functools.reduce(jnp.add, [jnp.exp(a[0:1] - top) for a in shard])
            lse_j = top + jnp.log(total)
            lse[j] = lse_j
            wgt[j] = mask[j] / count
            part = part + mask[j] * (lse_j - functools.reduce(jnp.add, [a[1:2] for a in shard]))
        loss_in[dp] = jnp.broadcast_to(jnp.sum(part, axis=-1, keepdims=True), (8, 128))
        for i in range(1, ndp):
            tile_copy(loss_in, loss_s, loss_r, i, dp).start()

    def share_end():
        for i in range(1, ndp):
            tile_copy(loss_in, loss_s, loss_r, i, peer(i, ndp, dp)).wait_recv()
        loss[...] = jnp.broadcast_to(in_order_sum(loss_in) / in_order_sum(cnt_in), (8, 128))
        for i in range(1, ndp):
            tile_copy(cnt_in, cnt_s, cnt_r, i, dp).wait_send()
            tile_copy(loss_in, loss_s, loss_r, i, dp).wait_send()
        for i in range(1, ntp):
            st_copy(i, z).wait_send()

    zb_copy = pltpu.make_async_copy(zb_hbm, zb, zb_sem.at[0])

    def s_copy(k):
        return pltpu.make_async_copy(scatter.at[rows8(k * chunk, chunk)], sbuf, s_sem.at[0])

    def z_product(u):
        k, j = lax.div(u, tiles), lax.rem(u, tiles)
        cols = pl.ds(pl.multiple_of(j * tile, tile), tile)
        acc[cols, :] += jnp.dot(gtile[lax.rem(u, 2)], ebuf[lax.rem(k, 2)], preferred_element_type=F32)

    def z_unit(u, carry):
        k, j = lax.div(u, tiles), lax.rem(u, tiles)
        slot = lax.rem(k, 2)

        @pl.when(j == 0)
        def _():
            e_copy(k).wait()
            l_copy(k).wait()

            @pl.when(k >= 2)
            def _():
                gs_copy(k - 1).wait()
        z_product(jnp.maximum(u - 1, 0) + jnp.where(u == 0, 1, 0))
        cols = pl.ds(pl.multiple_of(j * tile, tile), tile)
        ids = lax.broadcasted_iota(jnp.int32, (chunk, tile), 0) + k * chunk
        hit = jnp.where(ids == lab[j], 1.0, 0.0)
        g = ((jnp.exp(lbuf[slot, :, cols] - lse[j]) - hit) * wgt[j]).astype(BF16)
        gz_t[slot, :, cols] = g
        gtile[lax.rem(u, 2)] = g.T

        @pl.when((j == 0) & (k + 1 < nc))
        def _():
            e_copy(k + 1).start()
            l_copy(k + 1).start()

        @pl.when(j == tiles - 1)
        def _():
            gs_copy(k).start()

            @pl.when((k == 0) | (k == nc - 1))
            def _():
                gs_copy(k).wait()

        @pl.when(u == nc * tiles - 1)
        def _():
            z_product(u)
        return carry

    def g_unit(u, carry):
        k, n = lax.div(u, ntiles), lax.rem(u, ntiles)

        @pl.when(n == 0)
        def _():
            gl_copy(k).start()
            own_copy(k).wait()
            d2d_copy(k).wait_send()
            s_copy(k).wait()

            @pl.when(k == 0)
            def _():
                zb_copy.wait()
            gl_copy(k).wait()
        cols = pl.ds(pl.multiple_of(n * ntile, ntile), ntile)
        gbuf[:, cols] = sbuf[:, cols] + jnp.dot(gt[...], zb[:, cols], preferred_element_type=F32)

        @pl.when(n == ntiles - 1)
        def _():
            own_copy(k + 1).start()
            d2d_copy(k + 1).start()

            @pl.when(k + 1 < nc)
            def _():
                s_copy(k + 1).start()

            @pl.when(k == nc - 1)
            def _():
                own_copy(k + 1).wait()
                d2d_copy(k + 1).wait_send()
        return carry

    def load_start(k):
        d2d_copy(k).wait_recv()
        pltpu.make_async_copy(own.at[k], ld_own, ld_sem.at[0]).start()
        pltpu.make_async_copy(d2d.at[k], ld_d2d, ld_sem.at[1]).start()

    def stage_a(k):
        pltpu.make_async_copy(own.at[k], ld_own, ld_sem.at[0]).wait()
        pltpu.make_async_copy(d2d.at[k], ld_d2d, ld_sem.at[1]).wait()

        @pl.when(k >= RING)
        def _():
            rs1_copy(k - RING).wait_send()
        b = lax.rem(k, RING)

        def add(i, c):
            r = rows8(i * eighth, eighth)
            s1[b, r, :] = ld_own[r, :] + ld_d2d[r, :]
            return c
        lax.fori_loop(0, half // eighth, add, 0)
        rs1_copy(k).start()

    def stage_b(k):
        _, _, a1, _ = place(k)
        rs1_copy(k).wait_recv()

        @pl.when(k >= RING)
        def _():
            rs2_copy(k - RING).wait_send()
        b, r = lax.rem(k, RING), lax.rem(k, SLOTS)

        def add(i, c):
            s2[b, rows8(i * eighth, eighth), :] = (s1[b, rows8(a1 * quarter + i * eighth, eighth), :]
                                                   + rs1[r, rows8(i * eighth, eighth), :])
            return c
        lax.fori_loop(0, quarter // eighth, add, 0)
        rs2_copy(k).start()

    def stage_c(k):
        _, _, _, a2 = place(k)
        rs2_copy(k).wait_recv()

        @pl.when(k >= RING)
        def _():
            for i, c in enumerate(fin_copies(k - RING)):
                c.wait() if i == 0 else c.wait_send()
        b, r = lax.rem(k, RING), lax.rem(k, SLOTS)
        fin[b] = s2[b, rows8(a2 * eighth, eighth), :] + rs2[r]
        for c in fin_copies(k):
            c.start()

    def stage_d(k):
        fin_copies(k)[1].wait_recv()

        @pl.when(k >= RING)
        def _():
            for c in fwd_copies(k - RING):
                c.wait_send()
        for c in fwd_copies(k):
            c.start()

    def stage_w(k):
        fin_copies(k)[2].wait_recv()

    def stage_e(k):
        fwd_copies(k)[0].wait_recv()

        @pl.when(k >= RING)
        def _():
            last_copy(k - RING).wait_send()
        last_copy(k).start()

    def stage_f(k):
        fin_copies(k)[3].wait_recv()
        fwd_copies(k)[1].wait_recv()
        last_copy(k).wait_recv()

    nb = tokens // ntp // zrows
    qrows = tokens // ntp

    def zacc(q, b):
        return pl.multiple_of(q * qrows + b * zrows, 8)

    def right_copy(b, i, src=None):
        n = ntp - 1 - i
        s = zout_r.at[lax.rem(b, RING), pl.ds(i, n)] if src is None else src
        return zdma(s, rs_r.at[b, pl.ds(i, n)], zrs_sr.at[lax.rem(b, RING)], zrs_rr.at[b], i + 1)

    def left_copy(b, i):
        return zdma(zout_l.at[lax.rem(b, RING), pl.ds(0, i)], rs_l.at[b, pl.ds(0, i)], zrs_sl.at[lax.rem(b, RING)],
                    zrs_rl.at[b], i - 1)

    def z_right(b):
        for i in range(ntp - 1):
            @pl.when(z == i)
            def _(i=i):
                n = ntp - 1 - i
                if i > 0:
                    right_copy(b, i - 1).wait_recv()
                    load = pltpu.make_async_copy(rs_r.at[b, pl.ds(i, n)], zin_r.at[pl.ds(i, n)], zld.at[0])
                    load.start()
                    load.wait()

                @pl.when(b >= RING)
                def _():
                    right_copy(b - RING, i).wait_send()
                for q in range(i + 1, ntp):
                    mine = acc[pl.ds(zacc(q, b), zrows), :]
                    zout_r[lax.rem(b, RING), q - 1] = mine if i == 0 else zin_r[q - 1] + mine
                right_copy(b, i).start()

    def z_left(b):
        for i in range(1, ntp):
            @pl.when(z == i)
            def _(i=i):
                if i < ntp - 1:
                    left_copy(b, i + 1).wait_recv()
                    load = pltpu.make_async_copy(rs_l.at[b, pl.ds(0, i)], zin_l.at[pl.ds(0, i)], zld.at[0])
                    load.start()
                    load.wait()

                @pl.when(b >= RING)
                def _():
                    left_copy(b - RING, i).wait_send()
                for q in range(i):
                    mine = acc[pl.ds(zacc(q, b), zrows), :]
                    zout_l[lax.rem(b, RING), q] = mine if i == ntp - 1 else zin_l[q] + mine
                left_copy(b, i).start()

    def zfin_copies(b):
        s = lax.rem(b, RING)
        dst = gz.at[rows8(z * qrows + b * zrows, zrows)]
        return (pltpu.make_async_copy(zfin.at[s], dst, zfin_s.at[0, s]),
                zdma(zfin.at[s], dst, zfin_s.at[1, s], zag_rr.at[b, 0], z + 1),
                zdma(zfin.at[s], dst, zfin_s.at[2, s], zag_rl.at[b, 0], z - 1))

    def z_final(b):
        load_h = pltpu.make_async_copy(hidden.at[rows8(z * qrows + b * zrows, zrows)], hbuf, h_sem.at[0])
        load_h.start()
        for i in range(ntp):
            @pl.when(z == i)
            def _(i=i):
                if i > 0:
                    right_copy(b, i - 1).wait_recv() if i == ntp - 1 else None
                    load = pltpu.make_async_copy(rs_r.at[b, i - 1], zin_r.at[i - 1], zld.at[0])
                    load.start()
                    load.wait()
                if i < ntp - 1:
                    left_copy(b, i + 1).wait_recv() if i == 0 else None
                    load = pltpu.make_async_copy(rs_l.at[b, i], zin_l.at[i], zld.at[0])
                    load.start()
                    load.wait()
                z_wait_fin(b - RING, b >= RING)
                total = acc[pl.ds(zacc(i, b), zrows), :]
                if i > 0:
                    total = zin_r[i - 1] + total
                if i < ntp - 1:
                    total = total + zin_l[i]
                zfin[lax.rem(b, RING)] = total
        load_h.wait()
        h = hbuf[...].astype(F32)
        centered = h - jnp.mean(h, axis=-1, keepdims=True)
        rstd = lax.rsqrt(jnp.mean(centered * centered, axis=-1, keepdims=True) + 1e-5)
        unit = centered * rstd
        dy = zfin[lax.rem(b, RING)] * affine[0:1, :]
        zfin[lax.rem(b, RING)] = rstd * (dy - jnp.mean(dy, axis=-1, keepdims=True)
                                         - unit * jnp.mean(dy * unit, axis=-1, keepdims=True))
        copies = zfin_copies(b)
        copies[0].start()

        @pl.when(z < ntp - 1)
        def _():
            copies[1].start()

        @pl.when(z > 0)
        def _():
            copies[2].start()

    def z_wait_fin(b, cond):
        @pl.when(cond)
        def _():
            copies = zfin_copies(b)
            copies[0].wait()

            @pl.when(z < ntp - 1)
            def _():
                copies[1].wait_send()

            @pl.when(z > 0)
            def _():
                copies[2].wait_send()

    def zag(b, h, sign, ssem, rsem):
        ref = gz.at[rows8((z - sign * h) * qrows + b * zrows, zrows)]
        return zdma(ref, ref, ssem.at[b, h - 1], rsem.at[b, h], z + sign)

    def z_hop(b, h):
        ref_r = gz.at[rows8((z - h) * qrows + b * zrows, zrows)]
        ref_l = gz.at[rows8((z + h) * qrows + b * zrows, zrows)]

        @pl.when(z >= h)
        def _():
            zdma(ref_r, ref_r, zfw_r.at[b, 0], zag_rr.at[b, h - 1], z).wait_recv()
            if h < ntp - 1:
                @pl.when(z < ntp - 1)
                def _():
                    zag(b, h, 1, zfw_r, zag_rr).start()

        @pl.when(z + h <= ntp - 1)
        def _():
            zdma(ref_l, ref_l, zfw_l.at[b, 0], zag_rl.at[b, h - 1], z).wait_recv()
            if h < ntp - 1:
                @pl.when(z > 0)
                def _():
                    zag(b, h, -1, zfw_l, zag_rl).start()

    lead, g_first = 8, STEPS
    nz, ng = nc * tiles, nc * ntiles
    slow, fast = -(-tiles * 8 // 7), tiles * 11 // 7

    def uz(i):
        late = jnp.maximum(i - 1 - lead, 0)
        count = tiles + lax.div(jnp.minimum(i - 1, lead) * slow + late * fast, STEPS)
        return jnp.where(i <= 0, 0, jnp.minimum(count, nz))

    def ug(i):
        return jnp.where(i <= 0, 0, jnp.minimum(ntiles + lax.div(jnp.maximum(i - g_first, 0) * ntiles, STEPS), ng))

    lags = (('w', 17), ('f', 25), ('e', 21), ('d', 11), ('c', 8), ('b', 4), ('a', 1), ('p', 0))
    stages = {'w': stage_w, 'f': stage_f, 'e': stage_e, 'd': stage_d, 'c': stage_c, 'b': stage_b, 'a': stage_a,
              'p': load_start}
    z_start = lead + -(-max(nz - (tiles + lead * slow // STEPS), 0) * STEPS // fast)
    hop = 3
    steps = max((ncc - 1) * STEPS + 26, z_start + nb + hop * 2 * (ntp - 1))
    share_start()
    zb_copy.start()
    e_copy(0).start()
    l_copy(0).start()

    pos_copy = pltpu.make_async_copy(pos, gbuf, s_sem.at[0])
    pos_copy.start()
    gtile[...] = jnp.zeros_like(gtile)
    pos_copy.wait()
    s_copy(0).start()
    own_copy(0).start()
    d2d_copy(0).start()

    def clear(j, carry):
        acc[pl.ds(pl.multiple_of(j * tile, tile), tile), :] = jnp.zeros((tile, d), F32)
        return carry
    lax.fori_loop(0, tiles, clear, 0)
    share_use()

    def one_step(i, carry):
        lax.fori_loop(uz(i), uz(i + 1), z_unit, 0)
        lax.fori_loop(ug(i), ug(i + 1), g_unit, 0)
        for name, lag in lags:
            @pl.when((i >= lag) & (i - lag < ncc * STEPS) & (lax.rem(i - lag + STEPS * 64, STEPS) == 0))
            def _(name=name, lag=lag):
                stages[name](lax.div(i - lag, STEPS))
        zt = i - z_start

        @pl.when(valid(zt - hop * z, nb))
        def _():
            z_right(zt - hop * z)

        @pl.when(valid(zt - hop * (ntp - 1 - z), nb))
        def _():
            z_left(zt - hop * (ntp - 1 - z))

        @pl.when(valid(zt - hop * (ntp - 1), nb))
        def _():
            z_final(zt - hop * (ntp - 1))
        for h in range(1, ntp):
            @pl.when(valid(zt - hop * (ntp - 1 + h), nb))
            def _(h=h):
                z_hop(zt - hop * (ntp - 1 + h), h)
        return carry
    lax.fori_loop(0, steps, one_step, 0)

    share_end()

    for k in range(max(ncc - RING, 0), ncc):
        rs1_copy(k).wait_send()
        rs2_copy(k).wait_send()
        for i, c in enumerate(fin_copies(k)):
            c.wait() if i == 0 else c.wait_send()
        for c in fwd_copies(k):
            c.wait_send()
        last_copy(k).wait_send()
    for b in range(max(nb - RING, 0), nb):
        for i in range(ntp - 1):
            @pl.when(z == i)
            def _(i=i, b=b):
                right_copy(b, i).wait_send()
        for i in range(1, ntp):
            @pl.when(z == i)
            def _(i=i, b=b):
                left_copy(b, i).wait_send()
        z_wait_fin(b, z >= 0)

    def drain(b, carry):
        for h in range(1, ntp - 1):
            @pl.when((z >= h) & (z < ntp - 1))
            def _(h=h):
                zag(b, h, 1, zfw_r, zag_rr).wait_send()

            @pl.when((z + h <= ntp - 1) & (z > 0))
            def _(h=h):
                zag(b, h, -1, zfw_l, zag_rl).wait_send()
        return carry
    lax.fori_loop(0, nb, drain, 0)


def gradients(ntp, ndp, zb, stats, mask, lab, affine, hidden, embed, logits, scatter, pos, chunk, tile, zrows):
    tokens, d = zb.shape
    vocab_loc = embed.shape[0]
    nc = vocab_loc // chunk
    ncc = nc + 1
    half, quarter, eighth = chunk // 2, chunk // 4, chunk // 8
    tiles = tokens // tile
    nb = tokens // ntp // zrows
    vm = pl.BlockSpec(memory_space=pltpu.VMEM)
    hbm = pl.BlockSpec(memory_space=pl.ANY)
    dma = lambda *s: pltpu.SemaphoreType.DMA(s)
    vf = lambda *s: pltpu.VMEM(s, F32)
    sds = lambda *s: jax.ShapeDtypeStruct(s, F32)
    flops = 2 * tokens * d * vocab_loc
    rows = lambda a: a.reshape(tiles, 1, tile)
    res = pl.pallas_call(
        functools.partial(grad_kernel, ntp, ndp, chunk, tile, zrows),
        out_shape=(sds(vocab_loc + chunk, d), sds(8, 128), sds(tokens, d), sds(ncc, half, d), sds(ncc, half, d),
                   sds(nb, ntp - 1, zrows, d), sds(nb, ntp - 1, zrows, d), jax.ShapeDtypeStruct((nc, chunk, tokens), BF16)),
        in_specs=[vm] * 4 + [hbm] * 6,
        out_specs=(hbm, vm) + (hbm,) * 6,
        scratch_shapes=[
            pltpu.VMEM((tokens, d), BF16), vf(tiles, 1, tile), vf(tiles, 1, tile), vf(ntp, tiles, 8, tile), vf(ndp, 8, 128), vf(ndp, 8, 128),
            vf(2, chunk, tokens),
            pltpu.VMEM((2, chunk, d), BF16), pltpu.VMEM((2, chunk, tokens), BF16), pltpu.VMEM((2, tile, chunk), BF16),
            pltpu.VMEM((zrows, d), BF16), pltpu.VMEM((chunk, tokens), BF16), vf(chunk, d),
            vf(tokens, d), vf(chunk, d), vf(half, d), vf(half, d),
            vf(RING, half, d), vf(RING, quarter, d), vf(RING, eighth, d), vf(SLOTS, quarter, d), vf(SLOTS, eighth, d),
            vf(ntp - 1, zrows, d), vf(ntp - 1, zrows, d), vf(RING, ntp - 1, zrows, d), vf(RING, ntp - 1, zrows, d),
            vf(RING, zrows, d),
            dma(ntp - 1), dma(ntp), dma(ndp - 1), dma(ndp), dma(ndp - 1), dma(ndp), dma(1), dma(2),
            dma(2), dma(2), dma(1), dma(1), dma(1), dma(1), dma(1), dma(ncc), dma(2), dma(RING), dma(SLOTS), dma(RING), dma(SLOTS), dma(4, RING),
            dma(ncc), dma(2, ncc), dma(3, RING), dma(3, ncc),
            dma(1), dma(RING), dma(RING), dma(nb), dma(nb), dma(3, RING), dma(nb, ntp - 1), dma(nb, ntp - 1),
            dma(nb, ntp - 1), dma(nb, ntp - 1),
        ],
        compiler_params=pltpu.CompilerParams(vmem_limit_bytes=VMEM_LIMIT, has_side_effects=True),
        cost_estimate=pl.CostEstimate(flops=2 * flops, bytes_accessed=4 * vocab_loc * (4 * d + tokens),
                                      transcendentals=tokens * vocab_loc),
        name='gradients',
    )(stats, rows(mask), rows(lab), affine, zb, hidden, embed, logits, scatter, pos)
    return res[:3]


def finish_kernel(grad_in, pos_in, rows, gh_in, pos_table, grad_out, pos_out, embed_out, gh_out):
    grad_out[...] = grad_in[...]
    pos_out[...] = pos_in[...]
    embed_out[...] = (rows[...] + pos_table[...].astype(F32)).astype(BF16)
    gh_out[...] = gh_in[...].astype(BF16)


def finish(grads, rows, grad_h, pos_table, vocab_loc):
    tokens, d = grad_h.shape
    ctx = pos_table.shape[0]
    n = tokens // 64
    big, mid, small = vocab_loc // n, 64, ctx // n
    at = lambda r, f=lambda i: i: pl.BlockSpec((r, d), lambda i: (f(i), 0))
    return pl.pallas_call(
        finish_kernel,
        grid=(n,),
        in_specs=[at(big), at(small, lambda i: vocab_loc // small + i), at(mid), at(mid), at(mid, lambda i: lax.rem(i, ctx // mid))],
        out_specs=(at(big), at(small), at(mid), at(mid)),
        out_shape=(jax.ShapeDtypeStruct((vocab_loc, d), F32), jax.ShapeDtypeStruct((ctx, d), F32),
                   jax.ShapeDtypeStruct((tokens, d), BF16), jax.ShapeDtypeStruct((tokens, d), BF16)),
        compiler_params=pltpu.CompilerParams(vmem_limit_bytes=VMEM_LIMIT),
        cost_estimate=pl.CostEstimate(flops=tokens * d, bytes_accessed=8 * vocab_loc * d, transcendentals=0),
        name='finish',
    )(grads, grads, rows, grad_h, pos_table)


def solution(mesh):
    ntp, ndp = mesh.shape['tp'], mesh.shape['dp']

    def device_fn(tokens, labels, lossmask, hidden, grad_x0, embed_loc, pos_table, ln_gain, ln_bias):
        vocab_loc, d = embed_loc.shape
        batch, ctx = tokens.shape
        ntok = batch * ctx
        chunk1, chunk, tile, zrows = sizes(ntok, vocab_loc)
        shard_start = lax.axis_index('tp') * vocab_loc
        tok_local = (tokens - shard_start).reshape(1, ntok)
        lab_local = (labels - shard_start).reshape(1, ntok)
        tok_here = (tok_local >= 0) & (tok_local < vocab_loc)
        hidden2 = hidden.reshape(ntok, d)
        affine = jnp.stack([ln_gain, ln_bias])
        zb, stats, logits, rows, scatter, pos = token_stats(hidden2, affine, lab_local, tok_local, tok_here,
                                                            grad_x0.reshape(ntok, d), embed_loc, chunk1, tile, ctx)
        rows = lax.psum(rows, 'tp')
        grads, loss, grad_h = gradients(ntp, ndp, zb, stats, lossmask.astype(F32), lab_local, affine, hidden2, embed_loc,
                                        logits, scatter, pos, chunk, tile, zrows)
        grad_embed, grad_pos, embed_out, grad_hidden = finish(grads, rows, grad_h, pos_table, vocab_loc)
        mean_loss = loss[0, 0]
        embed_out = embed_out.reshape(batch, ctx, d)
        grad_hidden = grad_hidden.reshape(batch, ctx, d)
        return mean_loss, embed_out, grad_hidden, grad_embed, grad_pos

    row_spec = P('dp', None)
    act_spec = P('dp', None, None)
    return jax.shard_map(device_fn, mesh=mesh, in_specs=(row_spec, row_spec, row_spec, act_spec, act_spec, P('tp', None), P(None, None), P(None), P(None)), out_specs=(P(), act_spec, act_spec, P('tp', None), P(None, None)), check_vma=False)
```

```python
import functools

import jax
import jax.numpy as jnp
from jax import lax
from jax.experimental import pallas as pl
from jax.experimental.pallas import tpu as pltpu
from jax.sharding import PartitionSpec as P

MESH = pl.DeviceIdType.MESH
F32 = jnp.float32
BF16 = jnp.bfloat16
NT = (((1,), (1,)), ((), ()))
RING = 4
SLOTS = 8
STEPS = 2
VMEM_LIMIT = 66_000_000


def sizes(tokens, vocab_loc):
    if vocab_loc % 448 == 0 and tokens % 1792 == 0:
        return (928 if vocab_loc % 928 == 0 else 448), 448, 256, 32
    return 64, 64, 128, 8


def stats_kernel(chunk, tile, ctx, starts, order, skey, hidden, affine, lab, dx, embed,
                 zb_out, stats, logits_out, rows_out, scatter, pos_out, zb, pos, m_ref, s_ref, l_ref, dx_f32, dx_in, dx_sem, out_sem):
    step = pl.program_id(0)
    tokens, d = hidden.shape
    tiles = tokens // tile
    early = (pltpu.make_async_copy(zb, zb_out, out_sem.at[0]), pltpu.make_async_copy(pos, pos_out, out_sem.at[1]))

    @pl.when(step == 0)
    def _():
        def dx_copy(j):
            rows = pl.ds(pl.multiple_of(j * tile, tile), tile)
            return pltpu.make_async_copy(dx.at[rows], dx_in.at[lax.rem(j, 2)], dx_sem.at[lax.rem(j, 2)])
        dx_copy(0).start()

        def norm(j, carry):
            rows = pl.ds(pl.multiple_of(j * tile, tile), tile)
            dx_copy(j).wait()

            @pl.when(j + 1 < tiles)
            def _():
                dx_copy(j + 1).start()
            dx_f32[rows, :] = dx_in[lax.rem(j, 2)].astype(F32)
            h = hidden[rows, :].astype(F32)
            centered = h - jnp.mean(h, axis=-1, keepdims=True)
            var = jnp.mean(centered * centered, axis=-1, keepdims=True)
            zb[rows, :] = (centered * lax.rsqrt(var + 1e-5) * affine[0:1, :] + affine[1:2, :]).astype(BF16)
            rows_out[rows, :] = jnp.zeros((tile, d), F32)
            return carry
        lax.fori_loop(0, tiles, norm, 0)

        def pos_rows(j, carry):
            n = ctx // 8
            pos[pl.ds(pl.multiple_of(j * n, 8), n), :] = functools.reduce(jnp.add, [
                dx_f32[pl.ds(pl.multiple_of(b * ctx + j * n, 8), n), :] for b in range(tokens // ctx)])
            return carry
        lax.fori_loop(0, 8, pos_rows, 0)
        for c in early:
            c.start()
        m_ref[...] = jnp.full_like(m_ref, -jnp.inf)
        s_ref[...] = jnp.zeros_like(s_ref)
        l_ref[...] = jnp.zeros_like(l_ref)

    ids = lax.broadcasted_iota(jnp.int32, (chunk, tile), 0) + step * chunk

    def product(j):
        cols = slice(j * tile, (j + 1) * tile)
        logits_out[:, cols] = lax.dot_general(embed[...], zb[cols, :], NT, preferred_element_type=F32)

    product(0)
    band = -(-chunk // tiles // 8) * 8
    for j in range(tiles):
        cols = slice(j * tile, (j + 1) * tile)
        if j + 1 < tiles:
            product(j + 1)
        if j * band < chunk:
            scatter[j * band:min((j + 1) * band, chunk), :] = jnp.zeros((min(band, chunk - j * band), d), F32)
        logits = logits_out[:, cols]
        m_old = m_ref[:, cols]
        m_new = jnp.maximum(m_old, jnp.max(logits, axis=0, keepdims=True))
        m_ref[:, cols] = m_new
        s_ref[:, cols] = s_ref[:, cols] * jnp.exp(m_old - m_new) + jnp.sum(jnp.exp(logits - m_new), axis=0, keepdims=True)
        l_ref[:, cols] += jnp.sum(jnp.where(ids == lab[:, cols], logits, 0.0), axis=0, keepdims=True)

    first_tok, end_tok = starts[step], starts[step + 1]

    def token_row(i):
        real = i < end_tok
        i = jnp.where(real, i, 0)
        row = jnp.where(real, skey[i] - step * chunk, 0)
        group = lax.div(row, 16) * 16
        block = embed[pl.ds(pl.multiple_of(group, 16), 16), :].astype(F32)
        pick = lax.broadcasted_iota(jnp.int32, (16, 1), 0) == row - group
        rows_out[pl.ds(jnp.where(real, order[i], tokens), 1), :] = jnp.sum(jnp.where(pick, block, 0.0), axis=0, keepdims=True)
        scatter[pl.ds(row, 1), :] += jnp.where(real, dx_f32[pl.ds(order[i], 1), :], 0.0)

    def token_rows(n, carry):
        for u in range(4):
            token_row(first_tok + n * 4 + u)
        return carry
    lax.fori_loop(0, lax.div(end_tok - first_tok + 3, 4), token_rows, 0)

    @pl.when(step == pl.num_programs(0) - 1)
    def _():
        for c in early:
            c.wait()
        for j in range(tiles):
            cols = slice(j * tile, (j + 1) * tile)
            stats[j, 0:1, :] = m_ref[:, cols] + jnp.log(s_ref[:, cols])
            stats[j, 1:2, :] = l_ref[:, cols]
            stats[j, 2:8, :] = jnp.zeros((6, tile), F32)


def token_stats(hidden, affine, lab, tok, here, dx, embed, chunk, tile, ctx):
    tokens, d = hidden.shape
    vocab_loc = embed.shape[0]
    steps = vocab_loc // chunk
    key = jnp.where(here, tok, vocab_loc).reshape(tokens)
    skey, order = lax.sort_key_val(key, lax.iota(jnp.int32, tokens))
    bounds = lax.iota(jnp.int32, steps + 1) * chunk
    starts = jnp.sum((key[None, :] < bounds[:, None]).astype(jnp.int32), axis=1)
    whole = pl.BlockSpec(memory_space=pltpu.VMEM)
    return pl.pallas_call(
        functools.partial(stats_kernel, chunk, tile, ctx),
        grid_spec=pltpu.PrefetchScalarGridSpec(
            num_scalar_prefetch=3,
            grid=(steps,),
            in_specs=[whole, whole, whole, pl.BlockSpec(memory_space=pl.ANY), pl.BlockSpec((chunk, d), lambda i, *_: (i, 0))],
            out_specs=(pl.BlockSpec(memory_space=pl.ANY), whole, pl.BlockSpec((chunk, tokens), lambda i, *_: (i, 0)), whole,
                       pl.BlockSpec((chunk, d), lambda i, *_: (i, 0)), pl.BlockSpec(memory_space=pl.ANY)),
            scratch_shapes=[pltpu.VMEM((tokens, d), BF16), pltpu.VMEM((ctx, d), F32)] + [pltpu.VMEM((1, tokens), F32)] * 3 + [pltpu.VMEM((tokens, d), F32), pltpu.VMEM((2, tile, d), BF16),
                                                               pltpu.SemaphoreType.DMA((2,)), pltpu.SemaphoreType.DMA((2,))]),
        out_shape=(jax.ShapeDtypeStruct((tokens, d), BF16), jax.ShapeDtypeStruct((tokens // tile, 8, tile), F32),
                   jax.ShapeDtypeStruct((vocab_loc, tokens), F32), jax.ShapeDtypeStruct((tokens + 8, d), F32),
                   jax.ShapeDtypeStruct((vocab_loc, d), F32), jax.ShapeDtypeStruct((ctx, d), F32)),
        compiler_params=pltpu.CompilerParams(vmem_limit_bytes=VMEM_LIMIT),
        cost_estimate=pl.CostEstimate(flops=2 * tokens * d * vocab_loc, bytes_accessed=6 * embed.size + 4 * vocab_loc * tokens,
                                      transcendentals=tokens * vocab_loc),
        name='token_stats',
    )(starts, order, skey, hidden, affine, lab, dx, embed)


def grad_kernel(ntp, ndp, chunk, tile, zrows,
                stats, mask, lab, affine, zb_hbm, hidden, embed, logits, scatter, pos,
                out, loss, gz, own, d2d, rs_r, rs_l, gsave,
                zb, lse, wgt, st_in, cnt_in, loss_in, lbuf, ebuf, gz_t, gtile, hbuf, gt, sbuf, acc, gbuf, ld_own, ld_d2d, s1, s2, fin, rs1, rs2, zin_r, zin_l, zout_r, zout_l, zfin,
                st_s, st_r, cnt_s, cnt_r, loss_s, loss_r, zb_sem, l_sem, e_sem, gs_sem, gl_sem, h_sem, s_sem, own_sem, d2d_s, d2d_r, ld_sem, rs1_s, rs1_r, rs2_s, rs2_r, fin_s, ag1_r, ag2_r, fwd_s, part_r,
                zld, zrs_sr, zrs_sl, zrs_rr, zrs_rl, zfin_s, zag_rr, zag_rl, zfw_r, zfw_l):
    tokens, d = zb_hbm.shape
    vocab_loc = embed.shape[0]
    nc = vocab_loc // chunk
    ncc = nc + 1
    tiles = tokens // tile
    ntile = 256 if d % 256 == 0 and d > 256 else 128
    ntiles = d // ntile
    half, quarter, eighth = chunk // 2, chunk // 4, chunk // 8
    dp, z = lax.axis_index('dp'), lax.axis_index('tp')
    core = lax.rem(dp, 2)
    xpos = lax.rem(lax.div(dp, 2), 2)
    ypos = lax.div(dp, 4)
    partner = dp + 1 - 2 * core
    x_nbr = dp + 2 - 4 * xpos
    y_nbr = dp + 4 - 8 * ypos

    def place(k):
        odd = lax.rem(k, 2)
        n1 = x_nbr + (y_nbr - x_nbr) * odd
        n2 = y_nbr + (x_nbr - y_nbr) * odd
        a1 = xpos + (ypos - xpos) * odd
        a2 = ypos + (xpos - ypos) * odd
        return n1, n2, a1, a2

    def rdma(src, dst, ssem, rsem, dev):
        return pltpu.make_async_remote_copy(src_ref=src, dst_ref=dst, send_sem=ssem, recv_sem=rsem,
                                            device_id={'dp': dev}, device_id_type=MESH)

    def zdma(src, dst, ssem, rsem, dev):
        return pltpu.make_async_remote_copy(src_ref=src, dst_ref=dst, send_sem=ssem, recv_sem=rsem,
                                            device_id={'tp': dev}, device_id_type=MESH)

    def row0(c):
        return lax.rem(c + nc, ncc) * chunk

    def rows8(start, n):
        return pl.ds(pl.multiple_of(start, 8), n)

    def valid(k, limit):
        return (k >= 0) & (k < limit)

    def e_copy(k):
        return pltpu.make_async_copy(embed.at[rows8(k * chunk, chunk)], ebuf.at[lax.rem(k, 2)], e_sem.at[lax.rem(k, 2)])

    def l_copy(k):
        return pltpu.make_async_copy(logits.at[rows8(k * chunk, chunk)], lbuf.at[lax.rem(k, 2)], l_sem.at[lax.rem(k, 2)])

    def gs_copy(k):
        b = lax.rem(k, 2)
        return pltpu.make_async_copy(gz_t.at[b], gsave.at[k], gs_sem.at[b])

    def gl_copy(k):
        return pltpu.make_async_copy(gsave.at[k], gt, gl_sem.at[0])

    def own_copy(k):
        return pltpu.make_async_copy(gbuf.at[rows8(core * half, half)], own.at[k], own_sem.at[0])

    def d2d_copy(k):
        return rdma(gbuf.at[rows8((1 - core) * half, half)], d2d.at[k], d2d_s.at[0], d2d_r.at[k], partner)

    def rs1_copy(k):
        n1, _, a1, _ = place(k)
        b, r = lax.rem(k, RING), lax.rem(k, SLOTS)
        return rdma(s1.at[b, rows8((1 - a1) * quarter, quarter)], rs1.at[r], rs1_s.at[b], rs1_r.at[r], n1)

    def rs2_copy(k):
        _, n2, _, a2 = place(k)
        b, r = lax.rem(k, RING), lax.rem(k, SLOTS)
        return rdma(s2.at[b, rows8((1 - a2) * eighth, eighth)], rs2.at[r], rs2_s.at[b], rs2_r.at[r], n2)

    def fin_copies(k):
        n1, n2, a1, a2 = place(k)
        b = lax.rem(k, RING)
        dst = out.at[rows8(row0(k) + core * half + a1 * quarter + a2 * eighth, eighth)]
        src = fin.at[b]
        return (pltpu.make_async_copy(src, dst, fin_s.at[0, b]),
                rdma(src, dst, fin_s.at[1, b], ag1_r.at[k], n2),
                rdma(src, dst, fin_s.at[2, b], ag2_r.at[0, k], n1),
                rdma(src, dst, fin_s.at[3, b], part_r.at[0, k], partner))

    def fwd_copies(k):
        n1, _, a1, a2 = place(k)
        b = lax.rem(k, RING)
        ref = out.at[rows8(row0(k) + core * half + a1 * quarter + (1 - a2) * eighth, eighth)]
        return (rdma(ref, ref, fwd_s.at[0, b], ag2_r.at[1, k], n1),
                rdma(ref, ref, fwd_s.at[1, b], part_r.at[1, k], partner))

    def last_copy(k):
        _, _, a1, _ = place(k)
        ref = out.at[rows8(row0(k) + core * half + (1 - a1) * quarter, quarter)]
        return rdma(ref, ref, fwd_s.at[2, lax.rem(k, RING)], part_r.at[2, k], partner)

    def peer(i, n, me):
        return lax.rem(me + i, n)

    def st_copy(i, src_of):
        return zdma(st_in.at[z], st_in.at[src_of], st_s.at[i - 1], st_r.at[src_of], peer(i, ntp, z))

    def tile_copy(buf, ssem, rsem, i, src_of):
        return rdma(buf.at[dp], buf.at[src_of], ssem.at[i - 1], rsem.at[src_of], peer(i, ndp, dp))

    def share_start():
        st_in[z] = stats[...]
        for i in range(1, ntp):
            st_copy(i, z).start()
        cnt_in[dp] = jnp.broadcast_to(jnp.sum(jnp.sum(mask[...], axis=0), axis=-1, keepdims=True), (8, 128))
        for i in range(1, ndp):
            tile_copy(cnt_in, cnt_s, cnt_r, i, dp).start()

    def in_order_sum(buf):
        total = buf[0]
        for i in range(1, ndp):
            total = total + buf[i]
        return total[0:1, 0:1]

    def share_use():
        for i in range(1, ndp):
            tile_copy(cnt_in, cnt_s, cnt_r, i, peer(i, ndp, dp)).wait_recv()
        for i in range(1, ntp):
            st_copy(i, peer(i, ntp, z)).wait_recv()
        count = in_order_sum(cnt_in)
        part = jnp.zeros((1, tile), F32)
        for j in range(tiles):
            shard = [st_in[q, j] for q in range(ntp)]
            top = functools.reduce(jnp.maximum, [a[0:1] for a in shard])
            total = functools.reduce(jnp.add, [jnp.exp(a[0:1] - top) for a in shard])
            lse_j = top + jnp.log(total)
            lse[j] = lse_j
            wgt[j] = mask[j] / count
            part = part + mask[j] * (lse_j - functools.reduce(jnp.add, [a[1:2] for a in shard]))
        loss_in[dp] = jnp.broadcast_to(jnp.sum(part, axis=-1, keepdims=True), (8, 128))
        for i in range(1, ndp):
            tile_copy(loss_in, loss_s, loss_r, i, dp).start()

    def share_end():
        for i in range(1, ndp):
            tile_copy(loss_in, loss_s, loss_r, i, peer(i, ndp, dp)).wait_recv()
        loss[...] = jnp.broadcast_to(in_order_sum(loss_in) / in_order_sum(cnt_in), (8, 128))
        for i in range(1, ndp):
            tile_copy(cnt_in, cnt_s, cnt_r, i, dp).wait_send()
            tile_copy(loss_in, loss_s, loss_r, i, dp).wait_send()
        for i in range(1, ntp):
            st_copy(i, z).wait_send()

    zb_copy = pltpu.make_async_copy(zb_hbm, zb, zb_sem.at[0])

    def s_copy(k):
        return pltpu.make_async_copy(scatter.at[rows8(k * chunk, chunk)], sbuf, s_sem.at[0])

    def z_product(u):
        k, j = lax.div(u, tiles), lax.rem(u, tiles)
        cols = pl.ds(pl.multiple_of(j * tile, tile), tile)
        acc[cols, :] += jnp.dot(gtile[lax.rem(u, 2)], ebuf[lax.rem(k, 2)], preferred_element_type=F32)

    def z_unit(u, carry):
        k, j = lax.div(u, tiles), lax.rem(u, tiles)
        slot = lax.rem(k, 2)

        @pl.when(j == 0)
        def _():
            e_copy(k).wait()
            l_copy(k).wait()

            @pl.when(k >= 2)
            def _():
                gs_copy(k - 1).wait()
        z_product(jnp.maximum(u - 1, 0) + jnp.where(u == 0, 1, 0))
        cols = pl.ds(pl.multiple_of(j * tile, tile), tile)
        ids = lax.broadcasted_iota(jnp.int32, (chunk, tile), 0) + k * chunk
        hit = jnp.where(ids == lab[j], 1.0, 0.0)
        g = ((jnp.exp(lbuf[slot, :, cols] - lse[j]) - hit) * wgt[j]).astype(BF16)
        gz_t[slot, :, cols] = g
        gtile[lax.rem(u, 2)] = g.T

        @pl.when((j == 0) & (k + 1 < nc))
        def _():
            e_copy(k + 1).start()
            l_copy(k + 1).start()

        @pl.when(j == tiles - 1)
        def _():
            gs_copy(k).start()

            @pl.when((k == 0) | (k == nc - 1))
            def _():
                gs_copy(k).wait()

        @pl.when(u == nc * tiles - 1)
        def _():
            z_product(u)
        return carry

    def g_unit(u, carry):
        k, n = lax.div(u, ntiles), lax.rem(u, ntiles)

        @pl.when(n == 0)
        def _():
            gl_copy(k).start()

            @pl.when(k >= 1)
            def _():
                own_copy(k).wait()
            d2d_copy(k).wait_send()
            s_copy(k).wait()

            @pl.when(k == 0)
            def _():
                zb_copy.wait()
            gl_copy(k).wait()
        cols = pl.ds(pl.multiple_of(n * ntile, ntile), ntile)
        gbuf[:, cols] = sbuf[:, cols] + jnp.dot(gt[...], zb[:, cols], preferred_element_type=F32)

        @pl.when(n == ntiles - 1)
        def _():
            own_copy(k + 1).start()
            d2d_copy(k + 1).start()

            @pl.when(k + 1 < nc)
            def _():
                s_copy(k + 1).start()

            @pl.when(k == nc - 1)
            def _():
                own_copy(k + 1).wait()
                d2d_copy(k + 1).wait_send()
        return carry

    def load_start(k):
        d2d_copy(k).wait_recv()
        pltpu.make_async_copy(own.at[k], ld_own, ld_sem.at[0]).start()
        pltpu.make_async_copy(d2d.at[k], ld_d2d, ld_sem.at[1]).start()

    def stage_a(k):
        pltpu.make_async_copy(own.at[k], ld_own, ld_sem.at[0]).wait()
        pltpu.make_async_copy(d2d.at[k], ld_d2d, ld_sem.at[1]).wait()

        @pl.when(k >= RING)
        def _():
            rs1_copy(k - RING).wait_send()
        b = lax.rem(k, RING)

        def add(i, c):
            r = rows8(i * eighth, eighth)
            s1[b, r, :] = ld_own[r, :] + ld_d2d[r, :]
            return c
        lax.fori_loop(0, half // eighth, add, 0)
        rs1_copy(k).start()

    def stage_b(k):
        _, _, a1, _ = place(k)
        rs1_copy(k).wait_recv()

        @pl.when(k >= RING)
        def _():
            rs2_copy(k - RING).wait_send()
        b, r = lax.rem(k, RING), lax.rem(k, SLOTS)

        def add(i, c):
            s2[b, rows8(i * eighth, eighth), :] = (s1[b, rows8(a1 * quarter + i * eighth, eighth), :]
                                                   + rs1[r, rows8(i * eighth, eighth), :])
            return c
        lax.fori_loop(0, quarter // eighth, add, 0)
        rs2_copy(k).start()

    def stage_c(k):
        _, _, _, a2 = place(k)
        rs2_copy(k).wait_recv()

        @pl.when(k >= RING)
        def _():
            for i, c in enumerate(fin_copies(k - RING)):
                c.wait() if i == 0 else c.wait_send()
        b, r = lax.rem(k, RING), lax.rem(k, SLOTS)
        fin[b] = s2[b, rows8(a2 * eighth, eighth), :] + rs2[r]
        for c in fin_copies(k):
            c.start()

    def stage_d(k):
        fin_copies(k)[1].wait_recv()

        @pl.when(k >= RING)
        def _():
            for c in fwd_copies(k - RING):
                c.wait_send()
        for c in fwd_copies(k):
            c.start()

    def stage_w(k):
        fin_copies(k)[2].wait_recv()

    def stage_e(k):
        fwd_copies(k)[0].wait_recv()

        @pl.when(k >= RING)
        def _():
            last_copy(k - RING).wait_send()
        last_copy(k).start()

    def stage_f(k):
        fin_copies(k)[3].wait_recv()
        fwd_copies(k)[1].wait_recv()
        last_copy(k).wait_recv()

    nb = tokens // ntp // zrows
    qrows = tokens // ntp

    def zacc(q, b):
        return pl.multiple_of(q * qrows + b * zrows, 8)

    def right_copy(b, i, src=None):
        n = ntp - 1 - i
        s = zout_r.at[lax.rem(b, RING), pl.ds(i, n)] if src is None else src
        return zdma(s, rs_r.at[b, pl.ds(i, n)], zrs_sr.at[lax.rem(b, RING)], zrs_rr.at[b], i + 1)

    def left_copy(b, i):
        return zdma(zout_l.at[lax.rem(b, RING), pl.ds(0, i)], rs_l.at[b, pl.ds(0, i)], zrs_sl.at[lax.rem(b, RING)],
                    zrs_rl.at[b], i - 1)

    def z_right(b):
        for i in range(ntp - 1):
            @pl.when(z == i)
            def _(i=i):
                n = ntp - 1 - i
                if i > 0:
                    right_copy(b, i - 1).wait_recv()
                    load = pltpu.make_async_copy(rs_r.at[b, pl.ds(i, n)], zin_r.at[pl.ds(i, n)], zld.at[0])
                    load.start()
                    load.wait()

                @pl.when(b >= RING)
                def _():
                    right_copy(b - RING, i).wait_send()
                for q in range(i + 1, ntp):
                    mine = acc[pl.ds(zacc(q, b), zrows), :]
                    zout_r[lax.rem(b, RING), q - 1] = mine if i == 0 else zin_r[q - 1] + mine
                right_copy(b, i).start()

    def z_left(b):
        for i in range(1, ntp):
            @pl.when(z == i)
            def _(i=i):
                if i < ntp - 1:
                    left_copy(b, i + 1).wait_recv()
                    load = pltpu.make_async_copy(rs_l.at[b, pl.ds(0, i)], zin_l.at[pl.ds(0, i)], zld.at[0])
                    load.start()
                    load.wait()

                @pl.when(b >= RING)
                def _():
                    left_copy(b - RING, i).wait_send()
                for q in range(i):
                    mine = acc[pl.ds(zacc(q, b), zrows), :]
                    zout_l[lax.rem(b, RING), q] = mine if i == ntp - 1 else zin_l[q] + mine
                left_copy(b, i).start()

    def zfin_copies(b):
        s = lax.rem(b, RING)
        dst = gz.at[rows8(z * qrows + b * zrows, zrows)]
        return (pltpu.make_async_copy(zfin.at[s], dst, zfin_s.at[0, s]),
                zdma(zfin.at[s], dst, zfin_s.at[1, s], zag_rr.at[b, 0], z + 1),
                zdma(zfin.at[s], dst, zfin_s.at[2, s], zag_rl.at[b, 0], z - 1))

    def z_final(b):
        load_h = pltpu.make_async_copy(hidden.at[rows8(z * qrows + b * zrows, zrows)], hbuf, h_sem.at[0])
        load_h.start()
        for i in range(ntp):
            @pl.when(z == i)
            def _(i=i):
                if i > 0:
                    right_copy(b, i - 1).wait_recv() if i == ntp - 1 else None
                    load = pltpu.make_async_copy(rs_r.at[b, i - 1], zin_r.at[i - 1], zld.at[0])
                    load.start()
                    load.wait()
                if i < ntp - 1:
                    left_copy(b, i + 1).wait_recv() if i == 0 else None
                    load = pltpu.make_async_copy(rs_l.at[b, i], zin_l.at[i], zld.at[0])
                    load.start()
                    load.wait()
                z_wait_fin(b - RING, b >= RING)
                total = acc[pl.ds(zacc(i, b), zrows), :]
                if i > 0:
                    total = zin_r[i - 1] + total
                if i < ntp - 1:
                    total = total + zin_l[i]
                zfin[lax.rem(b, RING)] = total
        load_h.wait()
        h = hbuf[...].astype(F32)
        centered = h - jnp.mean(h, axis=-1, keepdims=True)
        rstd = lax.rsqrt(jnp.mean(centered * centered, axis=-1, keepdims=True) + 1e-5)
        unit = centered * rstd
        dy = zfin[lax.rem(b, RING)] * affine[0:1, :]
        zfin[lax.rem(b, RING)] = rstd * (dy - jnp.mean(dy, axis=-1, keepdims=True)
                                         - unit * jnp.mean(dy * unit, axis=-1, keepdims=True))
        copies = zfin_copies(b)
        copies[0].start()

        @pl.when(z < ntp - 1)
        def _():
            copies[1].start()

        @pl.when(z > 0)
        def _():
            copies[2].start()

    def z_wait_fin(b, cond):
        @pl.when(cond)
        def _():
            copies = zfin_copies(b)
            copies[0].wait()

            @pl.when(z < ntp - 1)
            def _():
                copies[1].wait_send()

            @pl.when(z > 0)
            def _():
                copies[2].wait_send()

    def zag(b, h, sign, ssem, rsem):
        ref = gz.at[rows8((z - sign * h) * qrows + b * zrows, zrows)]
        return zdma(ref, ref, ssem.at[b, h - 1], rsem.at[b, h], z + sign)

    def z_hop(b, h):
        ref_r = gz.at[rows8((z - h) * qrows + b * zrows, zrows)]
        ref_l = gz.at[rows8((z + h) * qrows + b * zrows, zrows)]

        @pl.when(z >= h)
        def _():
            zdma(ref_r, ref_r, zfw_r.at[b, 0], zag_rr.at[b, h - 1], z).wait_recv()
            if h < ntp - 1:
                @pl.when(z < ntp - 1)
                def _():
                    zag(b, h, 1, zfw_r, zag_rr).start()

        @pl.when(z + h <= ntp - 1)
        def _():
            zdma(ref_l, ref_l, zfw_l.at[b, 0], zag_rl.at[b, h - 1], z).wait_recv()
            if h < ntp - 1:
                @pl.when(z > 0)
                def _():
                    zag(b, h, -1, zfw_l, zag_rl).start()

    lead, g_first = 18, STEPS
    nz, ng = nc * tiles, nc * ntiles
    fast = tiles * 13 // 7

    def uz(i):
        late = jnp.maximum(i - 1 - lead, 0)
        count = tiles + 1 + lax.div(jnp.minimum(i - 1, lead) * tiles + late * fast, STEPS)
        return jnp.where(i <= 0, 0, jnp.minimum(count, nz))

    def ug(i):
        return jnp.where(i <= 0, 0, jnp.minimum(ntiles + lax.div(jnp.maximum(i - g_first, 0) * ntiles, STEPS), ng))

    lags = (('w', 12, 10), ('f', 24, 18), ('c', 8, 6), ('b', 5, 3), ('d', 11, 9), ('e', 16, 14), ('p', 0, -1), ('a', 1, -1))
    stages = {'w': stage_w, 'f': stage_f, 'e': stage_e, 'd': stage_d, 'c': stage_c, 'b': stage_b, 'a': stage_a,
              'p': load_start}
    z_start = lead + -(-max(nz - (tiles + 1 + lead * tiles // STEPS), 0) * STEPS // fast)
    hop = 3
    steps = max((ncc - 1) * STEPS + 26, z_start + nb + hop * 2 * (ntp - 1))
    share_start()
    zb_copy.start()
    e_copy(0).start()
    l_copy(0).start()

    pos_copy = pltpu.make_async_copy(pos, gbuf, s_sem.at[0])
    pos_copy.start()
    gtile[...] = jnp.zeros_like(gtile)
    pos_copy.wait()
    s_copy(0).start()
    own_copy(0).start()
    d2d_copy(0).start()

    own_copy(0).wait()
    load_start(0)

    def clear(j, carry):
        acc[pl.ds(pl.multiple_of(j * tile, tile), tile), :] = jnp.zeros((tile, d), F32)
        return carry
    lax.fori_loop(0, tiles, clear, 0)
    stage_a(0)
    share_use()

    def one_step(i, carry):
        lax.fori_loop(uz(i), uz(i + 1), z_unit, 0)
        lax.fori_loop(ug(i), ug(i + 1), g_unit, 0)
        for name, lag, first in lags:
            later = (i - lag >= STEPS) & (i - lag < ncc * STEPS) & (lax.rem(i - lag + STEPS * 64, STEPS) == 0)

            @pl.when(later | (i == first))
            def _(name=name, lag=lag, first=first):
                stages[name](jnp.where(i == first, 0, lax.div(i - lag, STEPS)))
        zt = i - z_start

        @pl.when(valid(zt - hop * z, nb))
        def _():
            z_right(zt - hop * z)

        @pl.when(valid(zt - hop * (ntp - 1 - z), nb))
        def _():
            z_left(zt - hop * (ntp - 1 - z))

        @pl.when(valid(zt - hop * (ntp - 1), nb))
        def _():
            z_final(zt - hop * (ntp - 1))
        for h in range(1, ntp):
            @pl.when(valid(zt - hop * (ntp - 1 + h), nb))
            def _(h=h):
                z_hop(zt - hop * (ntp - 1 + h), h)
        return carry
    lax.fori_loop(0, steps, one_step, 0)

    share_end()

    for k in range(max(ncc - RING, 0), ncc):
        rs1_copy(k).wait_send()
        rs2_copy(k).wait_send()
        for i, c in enumerate(fin_copies(k)):
            c.wait() if i == 0 else c.wait_send()
        for c in fwd_copies(k):
            c.wait_send()
        last_copy(k).wait_send()
    for b in range(max(nb - RING, 0), nb):
        for i in range(ntp - 1):
            @pl.when(z == i)
            def _(i=i, b=b):
                right_copy(b, i).wait_send()
        for i in range(1, ntp):
            @pl.when(z == i)
            def _(i=i, b=b):
                left_copy(b, i).wait_send()
        z_wait_fin(b, z >= 0)

    def drain(b, carry):
        for h in range(1, ntp - 1):
            @pl.when((z >= h) & (z < ntp - 1))
            def _(h=h):
                zag(b, h, 1, zfw_r, zag_rr).wait_send()

            @pl.when((z + h <= ntp - 1) & (z > 0))
            def _(h=h):
                zag(b, h, -1, zfw_l, zag_rl).wait_send()
        return carry
    lax.fori_loop(0, nb, drain, 0)


def gradients(ntp, ndp, zb, stats, mask, lab, affine, hidden, embed, logits, scatter, pos, chunk, tile, zrows):
    tokens, d = zb.shape
    vocab_loc = embed.shape[0]
    nc = vocab_loc // chunk
    ncc = nc + 1
    half, quarter, eighth = chunk // 2, chunk // 4, chunk // 8
    tiles = tokens // tile
    nb = tokens // ntp // zrows
    vm = pl.BlockSpec(memory_space=pltpu.VMEM)
    hbm = pl.BlockSpec(memory_space=pl.ANY)
    dma = lambda *s: pltpu.SemaphoreType.DMA(s)
    vf = lambda *s: pltpu.VMEM(s, F32)
    sds = lambda *s: jax.ShapeDtypeStruct(s, F32)
    flops = 2 * tokens * d * vocab_loc
    rows = lambda a: a.reshape(tiles, 1, tile)
    res = pl.pallas_call(
        functools.partial(grad_kernel, ntp, ndp, chunk, tile, zrows),
        out_shape=(sds(vocab_loc + chunk, d), sds(8, 128), sds(tokens, d), sds(ncc, half, d), sds(ncc, half, d),
                   sds(nb, ntp - 1, zrows, d), sds(nb, ntp - 1, zrows, d), jax.ShapeDtypeStruct((nc, chunk, tokens), BF16)),
        in_specs=[vm] * 4 + [hbm] * 6,
        out_specs=(hbm, vm) + (hbm,) * 6,
        scratch_shapes=[
            pltpu.VMEM((tokens, d), BF16), vf(tiles, 1, tile), vf(tiles, 1, tile), vf(ntp, tiles, 8, tile), vf(ndp, 8, 128), vf(ndp, 8, 128),
            vf(2, chunk, tokens),
            pltpu.VMEM((2, chunk, d), BF16), pltpu.VMEM((2, chunk, tokens), BF16), pltpu.VMEM((2, tile, chunk), BF16),
            pltpu.VMEM((zrows, d), BF16), pltpu.VMEM((chunk, tokens), BF16), vf(chunk, d),
            vf(tokens, d), vf(chunk, d), vf(half, d), vf(half, d),
            vf(RING, half, d), vf(RING, quarter, d), vf(RING, eighth, d), vf(SLOTS, quarter, d), vf(SLOTS, eighth, d),
            vf(ntp - 1, zrows, d), vf(ntp - 1, zrows, d), vf(RING, ntp - 1, zrows, d), vf(RING, ntp - 1, zrows, d),
            vf(RING, zrows, d),
            dma(ntp - 1), dma(ntp), dma(ndp - 1), dma(ndp), dma(ndp - 1), dma(ndp), dma(1), dma(2),
            dma(2), dma(2), dma(1), dma(1), dma(1), dma(1), dma(1), dma(ncc), dma(2), dma(RING), dma(SLOTS), dma(RING), dma(SLOTS), dma(4, RING),
            dma(ncc), dma(2, ncc), dma(3, RING), dma(3, ncc),
            dma(1), dma(RING), dma(RING), dma(nb), dma(nb), dma(3, RING), dma(nb, ntp - 1), dma(nb, ntp - 1),
            dma(nb, ntp - 1), dma(nb, ntp - 1),
        ],
        compiler_params=pltpu.CompilerParams(vmem_limit_bytes=VMEM_LIMIT, has_side_effects=True),
        cost_estimate=pl.CostEstimate(flops=2 * flops, bytes_accessed=4 * vocab_loc * (4 * d + tokens),
                                      transcendentals=tokens * vocab_loc),
        name='gradients',
    )(stats, rows(mask), rows(lab), affine, zb, hidden, embed, logits, scatter, pos)
    return res[:3]


def finish_kernel(grads, pos_in, rows, gh_in, pos_table, grad_out, pos_out, embed_out, gh_out, ring, in_sem, out_sem):
    i, n = pl.program_id(0), pl.num_programs(0)
    slots, size = ring.shape[0], ring.shape[1]
    ahead = slots - 2

    def block(k):
        return pl.ds(pl.multiple_of(k * size, 8), size)

    def take(k):
        return pltpu.make_async_copy(grads.at[block(k)], ring.at[lax.rem(k, slots)], in_sem.at[lax.rem(k, slots)])

    def give(k):
        return pltpu.make_async_copy(ring.at[lax.rem(k, slots)], grad_out.at[block(k)], out_sem.at[lax.rem(k, slots)])

    @pl.when(i == 0)
    def _():
        def first(k, carry):
            take(k).start()
            return carry
        lax.fori_loop(0, jnp.minimum(ahead, n), first, 0)

    @pl.when(i >= 2)
    def _():
        give(i - 2).wait()

    @pl.when(i + ahead < n)
    def _():
        take(i + ahead).start()
    take(i).wait()
    give(i).start()
    pos_out[...] = pos_in[...]
    embed_out[...] = (rows[...] + pos_table[...].astype(F32)).astype(BF16)
    gh_out[...] = gh_in[...].astype(BF16)

    @pl.when(i == n - 1)
    def _():
        @pl.when(i >= 1)
        def _():
            give(i - 1).wait()
        give(i).wait()


def finish(grads, rows, grad_h, pos_table, vocab_loc):
    tokens, d = grad_h.shape
    ctx = pos_table.shape[0]
    n = tokens // 64
    big, mid, small = vocab_loc // n, 64, ctx // n
    at = lambda r, f=lambda i: i: pl.BlockSpec((r, d), lambda i: (f(i), 0))
    return pl.pallas_call(
        finish_kernel,
        grid=(n,),
        in_specs=[pl.BlockSpec(memory_space=pl.ANY), at(small, lambda i: vocab_loc // small + i), at(mid), at(mid), at(mid, lambda i: lax.rem(i, ctx // mid))],
        out_specs=(pl.BlockSpec(memory_space=pl.ANY), at(small), at(mid), at(mid)),
        scratch_shapes=[pltpu.VMEM((8, big, d), F32), pltpu.SemaphoreType.DMA((8,)), pltpu.SemaphoreType.DMA((8,))],
        out_shape=(jax.ShapeDtypeStruct((vocab_loc, d), F32), jax.ShapeDtypeStruct((ctx, d), F32),
                   jax.ShapeDtypeStruct((tokens, d), BF16), jax.ShapeDtypeStruct((tokens, d), BF16)),
        compiler_params=pltpu.CompilerParams(vmem_limit_bytes=VMEM_LIMIT),
        cost_estimate=pl.CostEstimate(flops=tokens * d, bytes_accessed=8 * vocab_loc * d, transcendentals=0),
        name='finish',
    )(grads, grads, rows, grad_h, pos_table)


def solution(mesh):
    ntp, ndp = mesh.shape['tp'], mesh.shape['dp']

    def device_fn(tokens, labels, lossmask, hidden, grad_x0, embed_loc, pos_table, ln_gain, ln_bias):
        vocab_loc, d = embed_loc.shape
        batch, ctx = tokens.shape
        ntok = batch * ctx
        chunk1, chunk, tile, zrows = sizes(ntok, vocab_loc)
        shard_start = lax.axis_index('tp') * vocab_loc
        tok_local = (tokens - shard_start).reshape(1, ntok)
        lab_local = (labels - shard_start).reshape(1, ntok)
        tok_here = (tok_local >= 0) & (tok_local < vocab_loc)
        hidden2 = hidden.reshape(ntok, d)
        affine = jnp.stack([ln_gain, ln_bias])
        zb, stats, logits, rows, scatter, pos = token_stats(hidden2, affine, lab_local, tok_local, tok_here,
                                                            grad_x0.reshape(ntok, d), embed_loc, chunk1, tile, ctx)
        rows = lax.psum(rows, 'tp')
        grads, loss, grad_h = gradients(ntp, ndp, zb, stats, lossmask.astype(F32), lab_local, affine, hidden2, embed_loc,
                                        logits, scatter, pos, chunk, tile, zrows)
        grad_embed, grad_pos, embed_out, grad_hidden = finish(grads, rows, grad_h, pos_table, vocab_loc)
        mean_loss = loss[0, 0]
        embed_out = embed_out.reshape(batch, ctx, d)
        grad_hidden = grad_hidden.reshape(batch, ctx, d)
        return mean_loss, embed_out, grad_hidden, grad_embed, grad_pos

    row_spec = P('dp', None)
    act_spec = P('dp', None, None)
    return jax.shard_map(device_fn, mesh=mesh, in_specs=(row_spec, row_spec, row_spec, act_spec, act_spec, P('tp', None), P(None, None), P(None), P(None)), out_specs=(P(), act_spec, act_spec, P('tp', None), P(None, None)), check_vma=False)
```

```python
import functools

import jax
import jax.numpy as jnp
from jax import lax
from jax.experimental import pallas as pl
from jax.experimental.pallas import tpu as pltpu
from jax.sharding import PartitionSpec as P

MESH = pl.DeviceIdType.MESH
F32 = jnp.float32
BF16 = jnp.bfloat16
NT = (((1,), (1,)), ((), ()))
RING = 4
SLOTS = 8
STEPS = 2
VMEM_LIMIT = 66_000_000


def sizes(tokens, vocab_loc):
    if vocab_loc % 448 == 0 and tokens % 1792 == 0:
        return (928 if vocab_loc % 928 == 0 else 448), 448, 256, 32
    return 64, 64, 128, 8


def stats_kernel(chunk, tile, ctx, starts, order, skey, hidden, affine, lab, dx, embed,
                 zb_out, stats, logits_out, rows_out, scatter, pos_out, zb, pos, m_ref, s_ref, l_ref, dx_f32, dx_in, dx_sem, out_sem):
    step = pl.program_id(0)
    tokens, d = hidden.shape
    tiles = tokens // tile
    early = (pltpu.make_async_copy(zb, zb_out, out_sem.at[0]), pltpu.make_async_copy(pos, pos_out, out_sem.at[1]))

    @pl.when(step == 0)
    def _():
        def dx_copy(j):
            rows = pl.ds(pl.multiple_of(j * tile, tile), tile)
            return pltpu.make_async_copy(dx.at[rows], dx_in.at[lax.rem(j, 2)], dx_sem.at[lax.rem(j, 2)])
        dx_copy(0).start()

        def norm(j, carry):
            rows = pl.ds(pl.multiple_of(j * tile, tile), tile)
            dx_copy(j).wait()

            @pl.when(j + 1 < tiles)
            def _():
                dx_copy(j + 1).start()
            dx_f32[rows, :] = dx_in[lax.rem(j, 2)].astype(F32)
            h = hidden[rows, :].astype(F32)
            centered = h - jnp.mean(h, axis=-1, keepdims=True)
            var = jnp.mean(centered * centered, axis=-1, keepdims=True)
            zb[rows, :] = (centered * lax.rsqrt(var + 1e-5) * affine[0:1, :] + affine[1:2, :]).astype(BF16)
            rows_out[rows, :] = jnp.zeros((tile, d), F32)
            return carry
        lax.fori_loop(0, tiles, norm, 0)

        def pos_rows(j, carry):
            n = ctx // 8
            pos[pl.ds(pl.multiple_of(j * n, 8), n), :] = functools.reduce(jnp.add, [
                dx_f32[pl.ds(pl.multiple_of(b * ctx + j * n, 8), n), :] for b in range(tokens // ctx)])
            return carry
        lax.fori_loop(0, 8, pos_rows, 0)
        for c in early:
            c.start()
        m_ref[...] = jnp.full_like(m_ref, -jnp.inf)
        s_ref[...] = jnp.zeros_like(s_ref)
        l_ref[...] = jnp.zeros_like(l_ref)

    ids = lax.broadcasted_iota(jnp.int32, (chunk, tile), 0) + step * chunk

    def product(j):
        cols = slice(j * tile, (j + 1) * tile)
        logits_out[:, cols] = lax.dot_general(embed[...], zb[cols, :], NT, preferred_element_type=F32)

    product(0)
    band = -(-chunk // tiles // 8) * 8
    for j in range(tiles):
        cols = slice(j * tile, (j + 1) * tile)
        if j + 1 < tiles:
            product(j + 1)
        if j * band < chunk:
            scatter[j * band:min((j + 1) * band, chunk), :] = jnp.zeros((min(band, chunk - j * band), d), F32)
        logits = logits_out[:, cols]
        m_old = m_ref[:, cols]
        m_new = jnp.maximum(m_old, jnp.max(logits, axis=0, keepdims=True))
        m_ref[:, cols] = m_new
        s_ref[:, cols] = s_ref[:, cols] * jnp.exp(m_old - m_new) + jnp.sum(jnp.exp(logits - m_new), axis=0, keepdims=True)
        l_ref[:, cols] += jnp.sum(jnp.where(ids == lab[:, cols], logits, 0.0), axis=0, keepdims=True)

    first_tok, end_tok = starts[step], starts[step + 1]

    def token_row(i):
        real = i < end_tok
        i = jnp.where(real, i, 0)
        row = jnp.where(real, skey[i] - step * chunk, 0)
        group = lax.div(row, 16) * 16
        block = embed[pl.ds(pl.multiple_of(group, 16), 16), :].astype(F32)
        pick = lax.broadcasted_iota(jnp.int32, (16, 1), 0) == row - group
        rows_out[pl.ds(jnp.where(real, order[i], tokens), 1), :] = jnp.sum(jnp.where(pick, block, 0.0), axis=0, keepdims=True)
        scatter[pl.ds(row, 1), :] += jnp.where(real, dx_f32[pl.ds(order[i], 1), :], 0.0)

    def token_rows(n, carry):
        for u in range(4):
            token_row(first_tok + n * 4 + u)
        return carry
    lax.fori_loop(0, lax.div(end_tok - first_tok + 3, 4), token_rows, 0)

    @pl.when(step == pl.num_programs(0) - 1)
    def _():
        for c in early:
            c.wait()
        for j in range(tiles):
            cols = slice(j * tile, (j + 1) * tile)
            stats[j, 0:1, :] = m_ref[:, cols] + jnp.log(s_ref[:, cols])
            stats[j, 1:2, :] = l_ref[:, cols]
            stats[j, 2:8, :] = jnp.zeros((6, tile), F32)


def token_stats(hidden, affine, lab, tok, here, dx, embed, chunk, tile, ctx):
    tokens, d = hidden.shape
    vocab_loc = embed.shape[0]
    steps = vocab_loc // chunk
    key = jnp.where(here, tok, vocab_loc).reshape(tokens)
    skey, order = lax.sort_key_val(key, lax.iota(jnp.int32, tokens))
    bounds = lax.iota(jnp.int32, steps + 1) * chunk
    starts = jnp.sum((key[None, :] < bounds[:, None]).astype(jnp.int32), axis=1)
    whole = pl.BlockSpec(memory_space=pltpu.VMEM)
    return pl.pallas_call(
        functools.partial(stats_kernel, chunk, tile, ctx),
        grid_spec=pltpu.PrefetchScalarGridSpec(
            num_scalar_prefetch=3,
            grid=(steps,),
            in_specs=[whole, whole, whole, pl.BlockSpec(memory_space=pl.ANY), pl.BlockSpec((chunk, d), lambda i, *_: (i, 0))],
            out_specs=(pl.BlockSpec(memory_space=pl.ANY), whole, pl.BlockSpec((chunk, tokens), lambda i, *_: (i, 0)), whole,
                       pl.BlockSpec((chunk, d), lambda i, *_: (i, 0)), pl.BlockSpec(memory_space=pl.ANY)),
            scratch_shapes=[pltpu.VMEM((tokens, d), BF16), pltpu.VMEM((ctx, d), F32)] + [pltpu.VMEM((1, tokens), F32)] * 3 + [pltpu.VMEM((tokens, d), F32), pltpu.VMEM((2, tile, d), BF16),
                                                               pltpu.SemaphoreType.DMA((2,)), pltpu.SemaphoreType.DMA((2,))]),
        out_shape=(jax.ShapeDtypeStruct((tokens, d), BF16), jax.ShapeDtypeStruct((tokens // tile, 8, tile), F32),
                   jax.ShapeDtypeStruct((vocab_loc, tokens), F32), jax.ShapeDtypeStruct((tokens + 8, d), F32),
                   jax.ShapeDtypeStruct((vocab_loc, d), F32), jax.ShapeDtypeStruct((ctx, d), F32)),
        compiler_params=pltpu.CompilerParams(vmem_limit_bytes=VMEM_LIMIT),
        cost_estimate=pl.CostEstimate(flops=2 * tokens * d * vocab_loc, bytes_accessed=6 * embed.size + 4 * vocab_loc * tokens,
                                      transcendentals=tokens * vocab_loc),
        name='token_stats',
    )(starts, order, skey, hidden, affine, lab, dx, embed)


def grad_kernel(ntp, ndp, chunk, tile, zrows,
                stats, mask, lab, affine, zb_hbm, hidden, embed, logits, scatter, pos,
                out, loss, gz, own, d2d, rs_r, rs_l, gsave,
                zb, lse, wgt, st_in, cnt_in, loss_in, lbuf, ebuf, gz_t, gtile, hbuf, gt, sbuf, acc, gbuf, ld_own, ld_d2d, s1, s2, fin, rs1, rs2, zin_r, zin_l, zfin_r, zfin_l, zout_r, zout_l, zfin,
                st_s, st_r, cnt_s, cnt_r, loss_s, loss_r, zb_sem, l_sem, e_sem, gs_sem, gl_sem, h_sem, s_sem, own_sem, d2d_s, d2d_r, ld_sem, rs1_s, rs1_r, rs2_s, rs2_r, fin_s, ag1_r, ag2_r, fwd_s, part_r,
                zld, zrs_sr, zrs_sl, zrs_rr, zrs_rl, zfin_s, zag_rr, zag_rl, zfw_r, zfw_l):
    tokens, d = zb_hbm.shape
    vocab_loc = embed.shape[0]
    nc = vocab_loc // chunk
    ncc = nc + 1
    tiles = tokens // tile
    ntile = 256 if d % 256 == 0 and d > 256 else 128
    ntiles = d // ntile
    half, quarter, eighth = chunk // 2, chunk // 4, chunk // 8
    dp, z = lax.axis_index('dp'), lax.axis_index('tp')
    core = lax.rem(dp, 2)
    xpos = lax.rem(lax.div(dp, 2), 2)
    ypos = lax.div(dp, 4)
    partner = dp + 1 - 2 * core
    x_nbr = dp + 2 - 4 * xpos
    y_nbr = dp + 4 - 8 * ypos

    def place(k):
        odd = lax.rem(k, 2)
        n1 = x_nbr + (y_nbr - x_nbr) * odd
        n2 = y_nbr + (x_nbr - y_nbr) * odd
        a1 = xpos + (ypos - xpos) * odd
        a2 = ypos + (xpos - ypos) * odd
        return n1, n2, a1, a2

    def rdma(src, dst, ssem, rsem, dev):
        return pltpu.make_async_remote_copy(src_ref=src, dst_ref=dst, send_sem=ssem, recv_sem=rsem,
                                            device_id={'dp': dev}, device_id_type=MESH)

    def zdma(src, dst, ssem, rsem, dev):
        return pltpu.make_async_remote_copy(src_ref=src, dst_ref=dst, send_sem=ssem, recv_sem=rsem,
                                            device_id={'tp': dev}, device_id_type=MESH)

    def row0(c):
        return lax.rem(c + nc, ncc) * chunk

    def rows8(start, n):
        return pl.ds(pl.multiple_of(start, 8), n)

    def valid(k, limit):
        return (k >= 0) & (k < limit)

    def e_copy(k):
        return pltpu.make_async_copy(embed.at[rows8(k * chunk, chunk)], ebuf.at[lax.rem(k, 2)], e_sem.at[lax.rem(k, 2)])

    def l_copy(k):
        return pltpu.make_async_copy(logits.at[rows8(k * chunk, chunk)], lbuf.at[lax.rem(k, 2)], l_sem.at[lax.rem(k, 2)])

    def gs_copy(k):
        b = lax.rem(k, 2)
        return pltpu.make_async_copy(gz_t.at[b], gsave.at[k], gs_sem.at[b])

    def gl_copy(k):
        return pltpu.make_async_copy(gsave.at[k], gt, gl_sem.at[0])

    def own_copy(k):
        return pltpu.make_async_copy(gbuf.at[rows8(core * half, half)], own.at[k], own_sem.at[0])

    def d2d_copy(k):
        return rdma(gbuf.at[rows8((1 - core) * half, half)], d2d.at[k], d2d_s.at[0], d2d_r.at[k], partner)

    def rs1_copy(k):
        n1, _, a1, _ = place(k)
        b, r = lax.rem(k, RING), lax.rem(k, SLOTS)
        return rdma(s1.at[b, rows8((1 - a1) * quarter, quarter)], rs1.at[r], rs1_s.at[b], rs1_r.at[r], n1)

    def rs2_copy(k):
        _, n2, _, a2 = place(k)
        b, r = lax.rem(k, RING), lax.rem(k, SLOTS)
        return rdma(s2.at[b, rows8((1 - a2) * eighth, eighth)], rs2.at[r], rs2_s.at[b], rs2_r.at[r], n2)

    def fin_copies(k):
        n1, n2, a1, a2 = place(k)
        b = lax.rem(k, RING)
        dst = out.at[rows8(row0(k) + core * half + a1 * quarter + a2 * eighth, eighth)]
        src = fin.at[b]
        return (pltpu.make_async_copy(src, dst, fin_s.at[0, b]),
                rdma(src, dst, fin_s.at[1, b], ag1_r.at[k], n2),
                rdma(src, dst, fin_s.at[2, b], ag2_r.at[0, k], n1),
                rdma(src, dst, fin_s.at[3, b], part_r.at[0, k], partner))

    def fwd_copies(k):
        n1, _, a1, a2 = place(k)
        b = lax.rem(k, RING)
        ref = out.at[rows8(row0(k) + core * half + a1 * quarter + (1 - a2) * eighth, eighth)]
        return (rdma(ref, ref, fwd_s.at[0, b], ag2_r.at[1, k], n1),
                rdma(ref, ref, fwd_s.at[1, b], part_r.at[1, k], partner))

    def last_copy(k):
        _, _, a1, _ = place(k)
        ref = out.at[rows8(row0(k) + core * half + (1 - a1) * quarter, quarter)]
        return rdma(ref, ref, fwd_s.at[2, lax.rem(k, RING)], part_r.at[2, k], partner)

    def peer(i, n, me):
        return lax.rem(me + i, n)

    def st_copy(i, src_of):
        return zdma(st_in.at[z], st_in.at[src_of], st_s.at[i - 1], st_r.at[src_of], peer(i, ntp, z))

    def tile_copy(buf, ssem, rsem, i, src_of):
        return rdma(buf.at[dp], buf.at[src_of], ssem.at[i - 1], rsem.at[src_of], peer(i, ndp, dp))

    def share_start():
        st_in[z] = stats[...]
        for i in range(1, ntp):
            st_copy(i, z).start()
        cnt_in[dp] = jnp.broadcast_to(jnp.sum(jnp.sum(mask[...], axis=0), axis=-1, keepdims=True), (8, 128))
        for i in range(1, ndp):
            tile_copy(cnt_in, cnt_s, cnt_r, i, dp).start()

    def in_order_sum(buf):
        total = buf[0]
        for i in range(1, ndp):
            total = total + buf[i]
        return total[0:1, 0:1]

    def share_use():
        for i in range(1, ndp):
            tile_copy(cnt_in, cnt_s, cnt_r, i, peer(i, ndp, dp)).wait_recv()
        for i in range(1, ntp):
            st_copy(i, peer(i, ntp, z)).wait_recv()
        count = in_order_sum(cnt_in)
        part = jnp.zeros((1, tile), F32)
        for j in range(tiles):
            shard = [st_in[q, j] for q in range(ntp)]
            top = functools.reduce(jnp.maximum, [a[0:1] for a in shard])
            total = functools.reduce(jnp.add, [jnp.exp(a[0:1] - top) for a in shard])
            lse_j = top + jnp.log(total)
            lse[j] = lse_j
            wgt[j] = mask[j] / count
            part = part + mask[j] * (lse_j - functools.reduce(jnp.add, [a[1:2] for a in shard]))
        loss_in[dp] = jnp.broadcast_to(jnp.sum(part, axis=-1, keepdims=True), (8, 128))
        for i in range(1, ndp):
            tile_copy(loss_in, loss_s, loss_r, i, dp).start()

    def share_end():
        for i in range(1, ndp):
            tile_copy(loss_in, loss_s, loss_r, i, peer(i, ndp, dp)).wait_recv()
        loss[...] = jnp.broadcast_to(in_order_sum(loss_in) / in_order_sum(cnt_in), (8, 128))
        for i in range(1, ndp):
            tile_copy(cnt_in, cnt_s, cnt_r, i, dp).wait_send()
            tile_copy(loss_in, loss_s, loss_r, i, dp).wait_send()
        for i in range(1, ntp):
            st_copy(i, z).wait_send()

    zb_copy = pltpu.make_async_copy(zb_hbm, zb, zb_sem.at[0])

    def s_copy(k):
        return pltpu.make_async_copy(scatter.at[rows8(k * chunk, chunk)], sbuf, s_sem.at[0])

    def z_product(u):
        k, j = lax.div(u, tiles), lax.rem(u, tiles)
        cols = pl.ds(pl.multiple_of(j * tile, tile), tile)
        acc[cols, :] += jnp.dot(gtile[lax.rem(u, 2)], ebuf[lax.rem(k, 2)], preferred_element_type=F32)

    def z_unit(u, carry):
        k, j = lax.div(u, tiles), lax.rem(u, tiles)
        slot = lax.rem(k, 2)

        @pl.when(j == 0)
        def _():
            e_copy(k).wait()
            l_copy(k).wait()

            @pl.when(k >= 2)
            def _():
                gs_copy(k - 1).wait()
        z_product(jnp.maximum(u - 1, 0) + jnp.where(u == 0, 1, 0))
        cols = pl.ds(pl.multiple_of(j * tile, tile), tile)
        ids = lax.broadcasted_iota(jnp.int32, (chunk, tile), 0) + k * chunk
        hit = jnp.where(ids == lab[j], 1.0, 0.0)
        g = ((jnp.exp(lbuf[slot, :, cols] - lse[j]) - hit) * wgt[j]).astype(BF16)
        gz_t[slot, :, cols] = g
        gtile[lax.rem(u, 2)] = g.T

        @pl.when((j == 0) & (k + 1 < nc))
        def _():
            e_copy(k + 1).start()
            l_copy(k + 1).start()

        @pl.when(j == tiles - 1)
        def _():
            gs_copy(k).start()

            @pl.when((k == 0) | (k == nc - 1))
            def _():
                gs_copy(k).wait()

        @pl.when(u == nc * tiles - 1)
        def _():
            z_product(u)
        return carry

    def g_unit(u, carry):
        k, n = lax.div(u, ntiles), lax.rem(u, ntiles)

        @pl.when(n == 0)
        def _():
            gl_copy(k).start()

            @pl.when(k >= 1)
            def _():
                own_copy(k).wait()
            d2d_copy(k).wait_send()
            s_copy(k).wait()

            @pl.when(k == 0)
            def _():
                zb_copy.wait()
            gl_copy(k).wait()
        cols = pl.ds(pl.multiple_of(n * ntile, ntile), ntile)
        gbuf[:, cols] = sbuf[:, cols] + jnp.dot(gt[...], zb[:, cols], preferred_element_type=F32)

        @pl.when(n == ntiles - 1)
        def _():
            own_copy(k + 1).start()
            d2d_copy(k + 1).start()

            @pl.when(k + 1 < nc)
            def _():
                s_copy(k + 1).start()

            @pl.when(k == nc - 1)
            def _():
                own_copy(k + 1).wait()
                d2d_copy(k + 1).wait_send()
        return carry

    def load_start(k):
        d2d_copy(k).wait_recv()
        pltpu.make_async_copy(own.at[k], ld_own, ld_sem.at[0]).start()
        pltpu.make_async_copy(d2d.at[k], ld_d2d, ld_sem.at[1]).start()

    def stage_a(k):
        pltpu.make_async_copy(own.at[k], ld_own, ld_sem.at[0]).wait()
        pltpu.make_async_copy(d2d.at[k], ld_d2d, ld_sem.at[1]).wait()

        @pl.when(k >= RING)
        def _():
            rs1_copy(k - RING).wait_send()
        b = lax.rem(k, RING)

        def add(i, c):
            r = rows8(i * eighth, eighth)
            s1[b, r, :] = ld_own[r, :] + ld_d2d[r, :]
            return c
        lax.fori_loop(0, half // eighth, add, 0)
        rs1_copy(k).start()

    def stage_b(k):
        _, _, a1, _ = place(k)
        rs1_copy(k).wait_recv()

        @pl.when(k >= RING)
        def _():
            rs2_copy(k - RING).wait_send()
        b, r = lax.rem(k, RING), lax.rem(k, SLOTS)

        def add(i, c):
            s2[b, rows8(i * eighth, eighth), :] = (s1[b, rows8(a1 * quarter + i * eighth, eighth), :]
                                                   + rs1[r, rows8(i * eighth, eighth), :])
            return c
        lax.fori_loop(0, quarter // eighth, add, 0)
        rs2_copy(k).start()

    def stage_c(k):
        _, _, _, a2 = place(k)
        rs2_copy(k).wait_recv()

        @pl.when(k >= RING)
        def _():
            for i, c in enumerate(fin_copies(k - RING)):
                c.wait() if i == 0 else c.wait_send()
        b, r = lax.rem(k, RING), lax.rem(k, SLOTS)
        fin[b] = s2[b, rows8(a2 * eighth, eighth), :] + rs2[r]
        for c in fin_copies(k):
            c.start()

    def stage_d(k):
        fin_copies(k)[1].wait_recv()

        @pl.when(k >= RING)
        def _():
            for c in fwd_copies(k - RING):
                c.wait_send()
        for c in fwd_copies(k):
            c.start()

    def stage_w(k):
        fin_copies(k)[2].wait_recv()

    def stage_e(k):
        fwd_copies(k)[0].wait_recv()

        @pl.when(k >= RING)
        def _():
            last_copy(k - RING).wait_send()
        last_copy(k).start()

    def stage_f(k):
        fin_copies(k)[3].wait_recv()
        fwd_copies(k)[1].wait_recv()
        last_copy(k).wait_recv()

    nb = tokens // ntp // zrows
    qrows = tokens // ntp

    def zacc(q, b):
        return pl.multiple_of(q * qrows + b * zrows, 8)

    def right_copy(b, i, src=None):
        n = ntp - 1 - i
        s = zout_r.at[lax.rem(b, RING), pl.ds(i, n)] if src is None else src
        return zdma(s, rs_r.at[b, pl.ds(i, n)], zrs_sr.at[lax.rem(b, RING)], zrs_rr.at[b], i + 1)

    def left_copy(b, i):
        return zdma(zout_l.at[lax.rem(b, RING), pl.ds(0, i)], rs_l.at[b, pl.ds(0, i)], zrs_sl.at[lax.rem(b, RING)],
                    zrs_rl.at[b], i - 1)

    def right_load(b, i):
        n = ntp - 1 - i
        return pltpu.make_async_copy(rs_r.at[b, pl.ds(i, n)], zin_r.at[pl.ds(i, n)], zld.at[0])

    def left_load(b, i):
        return pltpu.make_async_copy(rs_l.at[b, pl.ds(0, i)], zin_l.at[pl.ds(0, i)], zld.at[1])

    def final_loads(b, i):
        loads = [pltpu.make_async_copy(hidden.at[rows8(z * qrows + b * zrows, zrows)], hbuf, h_sem.at[0])]
        if i > 0:
            loads.append(pltpu.make_async_copy(rs_r.at[b, i - 1], zfin_r, zld.at[2]))
        if i < ntp - 1:
            loads.append(pltpu.make_async_copy(rs_l.at[b, i], zfin_l, zld.at[3]))
        return loads

    def z_right_head(b):
        for i in range(1, ntp - 1):
            @pl.when(z == i)
            def _(i=i):
                right_copy(b, i - 1).wait_recv()
                right_load(b, i).start()

    def z_left_head(b):
        for i in range(1, ntp - 1):
            @pl.when(z == i)
            def _(i=i):
                left_copy(b, i + 1).wait_recv()
                left_load(b, i).start()

    def z_final_head(b):
        for i in range(ntp):
            @pl.when(z == i)
            def _(i=i):
                if i == ntp - 1:
                    right_copy(b, i - 1).wait_recv()
                if i == 0:
                    left_copy(b, i + 1).wait_recv()
                for c in final_loads(b, i):
                    c.start()

    def z_right(b):
        for i in range(ntp - 1):
            @pl.when(z == i)
            def _(i=i):
                n = ntp - 1 - i
                if i > 0:
                    right_load(b, i).wait()

                @pl.when(b >= RING)
                def _():
                    right_copy(b - RING, i).wait_send()
                for q in range(i + 1, ntp):
                    mine = acc[pl.ds(zacc(q, b), zrows), :]
                    zout_r[lax.rem(b, RING), q - 1] = mine if i == 0 else zin_r[q - 1] + mine
                right_copy(b, i).start()

    def z_left(b):
        for i in range(1, ntp):
            @pl.when(z == i)
            def _(i=i):
                if i < ntp - 1:
                    left_load(b, i).wait()

                @pl.when(b >= RING)
                def _():
                    left_copy(b - RING, i).wait_send()
                for q in range(i):
                    mine = acc[pl.ds(zacc(q, b), zrows), :]
                    zout_l[lax.rem(b, RING), q] = mine if i == ntp - 1 else zin_l[q] + mine
                left_copy(b, i).start()

    def zfin_copies(b):
        s = lax.rem(b, RING)
        dst = gz.at[rows8(z * qrows + b * zrows, zrows)]
        return (pltpu.make_async_copy(zfin.at[s], dst, zfin_s.at[0, s]),
                zdma(zfin.at[s], dst, zfin_s.at[1, s], zag_rr.at[b, 0], z + 1),
                zdma(zfin.at[s], dst, zfin_s.at[2, s], zag_rl.at[b, 0], z - 1))

    def z_final(b):
        for i in range(ntp):
            @pl.when(z == i)
            def _(i=i):
                for c in final_loads(b, i):
                    c.wait()
                z_wait_fin(b - RING, b >= RING)
                total = acc[pl.ds(zacc(i, b), zrows), :]
                if i > 0:
                    total = zfin_r[...] + total
                if i < ntp - 1:
                    total = total + zfin_l[...]
                zfin[lax.rem(b, RING)] = total
        h = hbuf[...].astype(F32)
        centered = h - jnp.mean(h, axis=-1, keepdims=True)
        rstd = lax.rsqrt(jnp.mean(centered * centered, axis=-1, keepdims=True) + 1e-5)
        unit = centered * rstd
        dy = zfin[lax.rem(b, RING)] * affine[0:1, :]
        zfin[lax.rem(b, RING)] = rstd * (dy - jnp.mean(dy, axis=-1, keepdims=True)
                                         - unit * jnp.mean(dy * unit, axis=-1, keepdims=True))
        copies = zfin_copies(b)
        copies[0].start()

        @pl.when(z < ntp - 1)
        def _():
            copies[1].start()

        @pl.when(z > 0)
        def _():
            copies[2].start()

    def z_wait_fin(b, cond):
        @pl.when(cond)
        def _():
            copies = zfin_copies(b)
            copies[0].wait()

            @pl.when(z < ntp - 1)
            def _():
                copies[1].wait_send()

            @pl.when(z > 0)
            def _():
                copies[2].wait_send()

    def zag(b, h, sign, ssem, rsem):
        ref = gz.at[rows8((z - sign * h) * qrows + b * zrows, zrows)]
        return zdma(ref, ref, ssem.at[b, h - 1], rsem.at[b, h], z + sign)

    def z_hop(b, h):
        ref_r = gz.at[rows8((z - h) * qrows + b * zrows, zrows)]
        ref_l = gz.at[rows8((z + h) * qrows + b * zrows, zrows)]

        @pl.when(z >= h)
        def _():
            zdma(ref_r, ref_r, zfw_r.at[b, 0], zag_rr.at[b, h - 1], z).wait_recv()
            if h < ntp - 1:
                @pl.when(z < ntp - 1)
                def _():
                    zag(b, h, 1, zfw_r, zag_rr).start()

        @pl.when(z + h <= ntp - 1)
        def _():
            zdma(ref_l, ref_l, zfw_l.at[b, 0], zag_rl.at[b, h - 1], z).wait_recv()
            if h < ntp - 1:
                @pl.when(z > 0)
                def _():
                    zag(b, h, -1, zfw_l, zag_rl).start()

    lead, g_first = 18, STEPS
    nz, ng = nc * tiles, nc * ntiles
    fast = tiles * 13 // 7

    def uz(i):
        late = jnp.maximum(i - 1 - lead, 0)
        count = tiles + 1 + lax.div(jnp.minimum(i - 1, lead) * tiles + late * fast, STEPS)
        return jnp.where(i <= 0, 0, jnp.minimum(count, nz))

    def ug(i):
        return jnp.where(i <= 0, 0, jnp.minimum(ntiles + lax.div(jnp.maximum(i - g_first, 0) * ntiles, STEPS), ng))

    lags = (('w', 12, 10), ('f', 24, 18), ('c', 8, 6), ('b', 5, 3), ('d', 11, 9), ('e', 16, 14), ('p', 0, -1), ('a', 1, -1))
    stages = {'w': stage_w, 'f': stage_f, 'e': stage_e, 'd': stage_d, 'c': stage_c, 'b': stage_b, 'a': stage_a,
              'p': load_start}
    z_start = lead + -(-max(nz - (tiles + 1 + lead * tiles // STEPS), 0) * STEPS // fast)
    hop = 3
    steps = max((ncc - 1) * STEPS + 26, z_start + nb + hop * 2 * (ntp - 1))
    share_start()
    zb_copy.start()
    e_copy(0).start()
    l_copy(0).start()

    pos_copy = pltpu.make_async_copy(pos, gbuf, s_sem.at[0])
    pos_copy.start()
    gtile[...] = jnp.zeros_like(gtile)
    pos_copy.wait()
    s_copy(0).start()
    own_copy(0).start()
    d2d_copy(0).start()

    own_copy(0).wait()
    load_start(0)

    def clear(j, carry):
        acc[pl.ds(pl.multiple_of(j * tile, tile), tile), :] = jnp.zeros((tile, d), F32)
        return carry
    lax.fori_loop(0, tiles, clear, 0)
    stage_a(0)
    share_use()

    def one_step(i, carry):
        zt = i - z_start
        right_b, left_b, final_b = zt - hop * z, zt - hop * (ntp - 1 - z), zt - hop * (ntp - 1)

        def z_stages(*stage_of):
            for b, stage in zip((right_b, left_b, final_b), stage_of):
                @pl.when(valid(b, nb))
                def _(b=b, stage=stage):
                    stage(b)
        z_stages(z_right_head, z_left_head, z_final_head)
        lax.fori_loop(uz(i), uz(i + 1), z_unit, 0)
        lax.fori_loop(ug(i), ug(i + 1), g_unit, 0)
        for name, lag, first in lags:
            later = (i - lag >= STEPS) & (i - lag < ncc * STEPS) & (lax.rem(i - lag + STEPS * 64, STEPS) == 0)

            @pl.when(later | (i == first))
            def _(name=name, lag=lag, first=first):
                stages[name](jnp.where(i == first, 0, lax.div(i - lag, STEPS)))
        z_stages(z_right, z_left, z_final)
        for h in range(1, ntp):
            @pl.when(valid(zt - hop * (ntp - 1 + h), nb))
            def _(h=h):
                z_hop(zt - hop * (ntp - 1 + h), h)
        return carry
    lax.fori_loop(0, steps, one_step, 0)

    share_end()

    for k in range(max(ncc - RING, 0), ncc):
        rs1_copy(k).wait_send()
        rs2_copy(k).wait_send()
        for i, c in enumerate(fin_copies(k)):
            c.wait() if i == 0 else c.wait_send()
        for c in fwd_copies(k):
            c.wait_send()
        last_copy(k).wait_send()
    for b in range(max(nb - RING, 0), nb):
        for i in range(ntp - 1):
            @pl.when(z == i)
            def _(i=i, b=b):
                right_copy(b, i).wait_send()
        for i in range(1, ntp):
            @pl.when(z == i)
            def _(i=i, b=b):
                left_copy(b, i).wait_send()
        z_wait_fin(b, z >= 0)

    def drain(b, carry):
        for h in range(1, ntp - 1):
            @pl.when((z >= h) & (z < ntp - 1))
            def _(h=h):
                zag(b, h, 1, zfw_r, zag_rr).wait_send()

            @pl.when((z + h <= ntp - 1) & (z > 0))
            def _(h=h):
                zag(b, h, -1, zfw_l, zag_rl).wait_send()
        return carry
    lax.fori_loop(0, nb, drain, 0)


def gradients(ntp, ndp, zb, stats, mask, lab, affine, hidden, embed, logits, scatter, pos, chunk, tile, zrows):
    tokens, d = zb.shape
    vocab_loc = embed.shape[0]
    nc = vocab_loc // chunk
    ncc = nc + 1
    half, quarter, eighth = chunk // 2, chunk // 4, chunk // 8
    tiles = tokens // tile
    nb = tokens // ntp // zrows
    vm = pl.BlockSpec(memory_space=pltpu.VMEM)
    hbm = pl.BlockSpec(memory_space=pl.ANY)
    dma = lambda *s: pltpu.SemaphoreType.DMA(s)
    vf = lambda *s: pltpu.VMEM(s, F32)
    sds = lambda *s: jax.ShapeDtypeStruct(s, F32)
    flops = 2 * tokens * d * vocab_loc
    rows = lambda a: a.reshape(tiles, 1, tile)
    res = pl.pallas_call(
        functools.partial(grad_kernel, ntp, ndp, chunk, tile, zrows),
        out_shape=(sds(vocab_loc + chunk, d), sds(8, 128), sds(tokens, d), sds(ncc, half, d), sds(ncc, half, d),
                   sds(nb, ntp - 1, zrows, d), sds(nb, ntp - 1, zrows, d), jax.ShapeDtypeStruct((nc, chunk, tokens), BF16)),
        in_specs=[vm] * 4 + [hbm] * 6,
        out_specs=(hbm, vm) + (hbm,) * 6,
        scratch_shapes=[
            pltpu.VMEM((tokens, d), BF16), vf(tiles, 1, tile), vf(tiles, 1, tile), vf(ntp, tiles, 8, tile), vf(ndp, 8, 128), vf(ndp, 8, 128),
            vf(2, chunk, tokens),
            pltpu.VMEM((2, chunk, d), BF16), pltpu.VMEM((2, chunk, tokens), BF16), pltpu.VMEM((2, tile, chunk), BF16),
            pltpu.VMEM((zrows, d), BF16), pltpu.VMEM((chunk, tokens), BF16), vf(chunk, d),
            vf(tokens, d), vf(chunk, d), vf(half, d), vf(half, d),
            vf(RING, half, d), vf(RING, quarter, d), vf(RING, eighth, d), vf(SLOTS, quarter, d), vf(SLOTS, eighth, d),
            vf(ntp - 1, zrows, d), vf(ntp - 1, zrows, d), vf(zrows, d), vf(zrows, d), vf(RING, ntp - 1, zrows, d), vf(RING, ntp - 1, zrows, d),
            vf(RING, zrows, d),
            dma(ntp - 1), dma(ntp), dma(ndp - 1), dma(ndp), dma(ndp - 1), dma(ndp), dma(1), dma(2),
            dma(2), dma(2), dma(1), dma(1), dma(1), dma(1), dma(1), dma(ncc), dma(2), dma(RING), dma(SLOTS), dma(RING), dma(SLOTS), dma(4, RING),
            dma(ncc), dma(2, ncc), dma(3, RING), dma(3, ncc),
            dma(4), dma(RING), dma(RING), dma(nb), dma(nb), dma(3, RING), dma(nb, ntp - 1), dma(nb, ntp - 1),
            dma(nb, ntp - 1), dma(nb, ntp - 1),
        ],
        compiler_params=pltpu.CompilerParams(vmem_limit_bytes=VMEM_LIMIT, has_side_effects=True),
        cost_estimate=pl.CostEstimate(flops=2 * flops, bytes_accessed=4 * vocab_loc * (4 * d + tokens),
                                      transcendentals=tokens * vocab_loc),
        name='gradients',
    )(stats, rows(mask), rows(lab), affine, zb, hidden, embed, logits, scatter, pos)
    return res[:3]


def finish_kernel(grads, pos_in, rows, gh_in, pos_table, grad_out, pos_out, embed_out, gh_out, ring, in_sem, out_sem):
    i, n = pl.program_id(0), pl.num_programs(0)
    slots, size = ring.shape[0], ring.shape[1]
    ahead = slots - 2

    def block(k):
        return pl.ds(pl.multiple_of(k * size, 8), size)

    def take(k):
        return pltpu.make_async_copy(grads.at[block(k)], ring.at[lax.rem(k, slots)], in_sem.at[lax.rem(k, slots)])

    def give(k):
        return pltpu.make_async_copy(ring.at[lax.rem(k, slots)], grad_out.at[block(k)], out_sem.at[lax.rem(k, slots)])

    @pl.when(i == 0)
    def _():
        def first(k, carry):
            take(k).start()
            return carry
        lax.fori_loop(0, jnp.minimum(ahead, n), first, 0)

    @pl.when(i >= 2)
    def _():
        give(i - 2).wait()

    @pl.when(i + ahead < n)
    def _():
        take(i + ahead).start()
    take(i).wait()
    give(i).start()
    pos_out[...] = pos_in[...]
    embed_out[...] = (rows[...] + pos_table[...].astype(F32)).astype(BF16)
    gh_out[...] = gh_in[...].astype(BF16)

    @pl.when(i == n - 1)
    def _():
        @pl.when(i >= 1)
        def _():
            give(i - 1).wait()
        give(i).wait()


def finish(grads, rows, grad_h, pos_table, vocab_loc):
    tokens, d = grad_h.shape
    ctx = pos_table.shape[0]
    n = tokens // 64
    big, mid, small = vocab_loc // n, 64, ctx // n
    at = lambda r, f=lambda i: i: pl.BlockSpec((r, d), lambda i: (f(i), 0))
    return pl.pallas_call(
        finish_kernel,
        grid=(n,),
        in_specs=[pl.BlockSpec(memory_space=pl.ANY), at(small, lambda i: vocab_loc // small + i), at(mid), at(mid), at(mid, lambda i: lax.rem(i, ctx // mid))],
        out_specs=(pl.BlockSpec(memory_space=pl.ANY), at(small), at(mid), at(mid)),
        scratch_shapes=[pltpu.VMEM((8, big, d), F32), pltpu.SemaphoreType.DMA((8,)), pltpu.SemaphoreType.DMA((8,))],
        out_shape=(jax.ShapeDtypeStruct((vocab_loc, d), F32), jax.ShapeDtypeStruct((ctx, d), F32),
                   jax.ShapeDtypeStruct((tokens, d), BF16), jax.ShapeDtypeStruct((tokens, d), BF16)),
        compiler_params=pltpu.CompilerParams(vmem_limit_bytes=VMEM_LIMIT),
        cost_estimate=pl.CostEstimate(flops=tokens * d, bytes_accessed=8 * vocab_loc * d, transcendentals=0),
        name='finish',
    )(grads, grads, rows, grad_h, pos_table)


def solution(mesh):
    ntp, ndp = mesh.shape['tp'], mesh.shape['dp']

    def device_fn(tokens, labels, lossmask, hidden, grad_x0, embed_loc, pos_table, ln_gain, ln_bias):
        vocab_loc, d = embed_loc.shape
        batch, ctx = tokens.shape
        ntok = batch * ctx
        chunk1, chunk, tile, zrows = sizes(ntok, vocab_loc)
        shard_start = lax.axis_index('tp') * vocab_loc
        tok_local = (tokens - shard_start).reshape(1, ntok)
        lab_local = (labels - shard_start).reshape(1, ntok)
        tok_here = (tok_local >= 0) & (tok_local < vocab_loc)
        hidden2 = hidden.reshape(ntok, d)
        affine = jnp.stack([ln_gain, ln_bias])
        zb, stats, logits, rows, scatter, pos = token_stats(hidden2, affine, lab_local, tok_local, tok_here,
                                                            grad_x0.reshape(ntok, d), embed_loc, chunk1, tile, ctx)
        rows = lax.psum(rows, 'tp')
        grads, loss, grad_h = gradients(ntp, ndp, zb, stats, lossmask.astype(F32), lab_local, affine, hidden2, embed_loc,
                                        logits, scatter, pos, chunk, tile, zrows)
        grad_embed, grad_pos, embed_out, grad_hidden = finish(grads, rows, grad_h, pos_table, vocab_loc)
        mean_loss = loss[0, 0]
        embed_out = embed_out.reshape(batch, ctx, d)
        grad_hidden = grad_hidden.reshape(batch, ctx, d)
        return mean_loss, embed_out, grad_hidden, grad_embed, grad_pos

    row_spec = P('dp', None)
    act_spec = P('dp', None, None)
    return jax.shard_map(device_fn, mesh=mesh, in_specs=(row_spec, row_spec, row_spec, act_spec, act_spec, P('tp', None), P(None, None), P(None), P(None)), out_specs=(P(), act_spec, act_spec, P('tp', None), P(None, None)), check_vma=False)
```

```python
import functools

import jax
import jax.numpy as jnp
from jax import lax
from jax.experimental import pallas as pl
from jax.experimental.pallas import tpu as pltpu
from jax.sharding import PartitionSpec as P

MESH = pl.DeviceIdType.MESH
F32 = jnp.float32
BF16 = jnp.bfloat16
NT = (((1,), (1,)), ((), ()))
RING = 4
SLOTS = 8
STEPS = 2
VMEM_LIMIT = 66_000_000


def sizes(tokens, vocab_loc):
    if vocab_loc % 448 == 0 and tokens % 1792 == 0:
        return (928 if vocab_loc % 928 == 0 else 448), 448, 256, 32
    return 64, 64, 128, 8


def stats_kernel(chunk, tile, starts, order, skey, hidden, affine, lab, dx, embed,
                 zb_out, stats, logits_out, rows_out, scatter, zb, m_ref, s_ref, l_ref, dx_f32, dx_in, dx_sem, out_sem):
    step = pl.program_id(0)
    tokens, d = hidden.shape
    tiles = tokens // tile
    early = pltpu.make_async_copy(zb, zb_out, out_sem.at[0])

    @pl.when(step == 0)
    def _():
        def dx_copy(j):
            rows = pl.ds(pl.multiple_of(j * tile, tile), tile)
            return pltpu.make_async_copy(dx.at[rows], dx_in.at[lax.rem(j, 2)], dx_sem.at[lax.rem(j, 2)])
        dx_copy(0).start()

        def norm(j, carry):
            rows = pl.ds(pl.multiple_of(j * tile, tile), tile)
            dx_copy(j).wait()

            @pl.when(j + 1 < tiles)
            def _():
                dx_copy(j + 1).start()
            dx_f32[rows, :] = dx_in[lax.rem(j, 2)].astype(F32)
            h = hidden[rows, :].astype(F32)
            centered = h - jnp.mean(h, axis=-1, keepdims=True)
            var = jnp.mean(centered * centered, axis=-1, keepdims=True)
            zb[rows, :] = (centered * lax.rsqrt(var + 1e-5) * affine[0:1, :] + affine[1:2, :]).astype(BF16)
            rows_out[rows, :] = jnp.zeros((tile, d), F32)
            return carry
        lax.fori_loop(0, tiles, norm, 0)

        early.start()
        m_ref[...] = jnp.full_like(m_ref, -jnp.inf)
        s_ref[...] = jnp.zeros_like(s_ref)
        l_ref[...] = jnp.zeros_like(l_ref)

    ids = lax.broadcasted_iota(jnp.int32, (chunk, tile), 0) + step * chunk

    def product(j):
        cols = slice(j * tile, (j + 1) * tile)
        logits_out[:, cols] = lax.dot_general(embed[...], zb[cols, :], NT, preferred_element_type=F32)

    product(0)
    band = -(-chunk // tiles // 8) * 8
    for j in range(tiles):
        cols = slice(j * tile, (j + 1) * tile)
        if j + 1 < tiles:
            product(j + 1)
        if j * band < chunk:
            scatter[j * band:min((j + 1) * band, chunk), :] = jnp.zeros((min(band, chunk - j * band), d), F32)
        logits = logits_out[:, cols]
        m_old = m_ref[:, cols]
        m_new = jnp.maximum(m_old, jnp.max(logits, axis=0, keepdims=True))
        m_ref[:, cols] = m_new
        s_ref[:, cols] = s_ref[:, cols] * jnp.exp(m_old - m_new) + jnp.sum(jnp.exp(logits - m_new), axis=0, keepdims=True)
        l_ref[:, cols] += jnp.sum(jnp.where(ids == lab[:, cols], logits, 0.0), axis=0, keepdims=True)

    first_tok, end_tok = starts[step], starts[step + 1]

    def token_row(i):
        real = i < end_tok
        i = jnp.where(real, i, 0)
        row = jnp.where(real, skey[i] - step * chunk, 0)
        group = lax.div(row, 16) * 16
        block = embed[pl.ds(pl.multiple_of(group, 16), 16), :].astype(F32)
        pick = lax.broadcasted_iota(jnp.int32, (16, 1), 0) == row - group
        rows_out[pl.ds(jnp.where(real, order[i], tokens), 1), :] = jnp.sum(jnp.where(pick, block, 0.0), axis=0, keepdims=True)
        scatter[pl.ds(row, 1), :] += jnp.where(real, dx_f32[pl.ds(order[i], 1), :], 0.0)

    def token_rows(n, carry):
        for u in range(4):
            token_row(first_tok + n * 4 + u)
        return carry
    lax.fori_loop(0, lax.div(end_tok - first_tok + 3, 4), token_rows, 0)

    @pl.when(step == pl.num_programs(0) - 1)
    def _():
        early.wait()
        for j in range(tiles):
            cols = slice(j * tile, (j + 1) * tile)
            stats[j, 0:1, :] = m_ref[:, cols] + jnp.log(s_ref[:, cols])
            stats[j, 1:2, :] = l_ref[:, cols]
            stats[j, 2:8, :] = jnp.zeros((6, tile), F32)


def token_stats(hidden, affine, lab, tok, here, dx, embed, chunk, tile):
    tokens, d = hidden.shape
    vocab_loc = embed.shape[0]
    steps = vocab_loc // chunk
    key = jnp.where(here, tok, vocab_loc).reshape(tokens)
    skey, order = lax.sort_key_val(key, lax.iota(jnp.int32, tokens))
    bounds = lax.iota(jnp.int32, steps + 1) * chunk
    starts = jnp.sum((key[None, :] < bounds[:, None]).astype(jnp.int32), axis=1)
    whole = pl.BlockSpec(memory_space=pltpu.VMEM)
    return pl.pallas_call(
        functools.partial(stats_kernel, chunk, tile),
        grid_spec=pltpu.PrefetchScalarGridSpec(
            num_scalar_prefetch=3,
            grid=(steps,),
            in_specs=[whole, whole, whole, pl.BlockSpec(memory_space=pl.ANY), pl.BlockSpec((chunk, d), lambda i, *_: (i, 0))],
            out_specs=(pl.BlockSpec(memory_space=pl.ANY), whole, pl.BlockSpec((chunk, tokens), lambda i, *_: (i, 0)), whole,
                       pl.BlockSpec((chunk, d), lambda i, *_: (i, 0))),
            scratch_shapes=[pltpu.VMEM((tokens, d), BF16)] + [pltpu.VMEM((1, tokens), F32)] * 3 + [pltpu.VMEM((tokens, d), F32), pltpu.VMEM((2, tile, d), BF16),
                                                               pltpu.SemaphoreType.DMA((2,)), pltpu.SemaphoreType.DMA((1,))]),
        out_shape=(jax.ShapeDtypeStruct((tokens, d), BF16), jax.ShapeDtypeStruct((tokens // tile, 8, tile), F32),
                   jax.ShapeDtypeStruct((vocab_loc, tokens), F32), jax.ShapeDtypeStruct((tokens + 8, d), F32),
                   jax.ShapeDtypeStruct((vocab_loc, d), F32)),
        compiler_params=pltpu.CompilerParams(vmem_limit_bytes=VMEM_LIMIT),
        cost_estimate=pl.CostEstimate(flops=2 * tokens * d * vocab_loc, bytes_accessed=6 * embed.size + 4 * vocab_loc * tokens,
                                      transcendentals=tokens * vocab_loc),
        name='token_stats',
    )(starts, order, skey, hidden, affine, lab, dx, embed)


def grad_kernel(ntp, ndp, chunk, tile, zrows,
                stats, mask, lab, affine, zb_hbm, hidden, embed, logits, scatter,
                out, loss, gz, own, d2d, rs_r, rs_l, gsave,
                zb, lse, wgt, st_in, cnt_in, loss_in, lbuf, ebuf, gz_t, gtile, hbuf, gt, sbuf, acc, gbuf, ld_own, ld_d2d, s1, s2, fin, rs1, rs2, zin_r, zin_l, zfin_r, zfin_l, zout_r, zout_l, zfin,
                st_s, st_r, cnt_s, cnt_r, loss_s, loss_r, zb_sem, l_sem, e_sem, gs_sem, gl_sem, h_sem, s_sem, own_sem, d2d_s, d2d_r, ld_sem, rs1_s, rs1_r, rs2_s, rs2_r, fin_s, ag1_r, ag2_r, fwd_s, part_r,
                zld, zrs_sr, zrs_sl, zrs_rr, zrs_rl, zfin_s, zag_rr, zag_rl, zfw_r, zfw_l):
    tokens, d = zb_hbm.shape
    vocab_loc = embed.shape[0]
    nc = vocab_loc // chunk
    tiles = tokens // tile
    ntile = 256 if d % 256 == 0 and d > 256 else 128
    ntiles = d // ntile
    half, quarter, eighth = chunk // 2, chunk // 4, chunk // 8
    dp, z = lax.axis_index('dp'), lax.axis_index('tp')
    core = lax.rem(dp, 2)
    xpos = lax.rem(lax.div(dp, 2), 2)
    ypos = lax.div(dp, 4)
    partner = dp + 1 - 2 * core
    x_nbr = dp + 2 - 4 * xpos
    y_nbr = dp + 4 - 8 * ypos

    def place(k):
        odd = lax.rem(k, 2)
        n1 = x_nbr + (y_nbr - x_nbr) * odd
        n2 = y_nbr + (x_nbr - y_nbr) * odd
        a1 = xpos + (ypos - xpos) * odd
        a2 = ypos + (xpos - ypos) * odd
        return n1, n2, a1, a2

    def rdma(src, dst, ssem, rsem, dev):
        return pltpu.make_async_remote_copy(src_ref=src, dst_ref=dst, send_sem=ssem, recv_sem=rsem,
                                            device_id={'dp': dev}, device_id_type=MESH)

    def zdma(src, dst, ssem, rsem, dev):
        return pltpu.make_async_remote_copy(src_ref=src, dst_ref=dst, send_sem=ssem, recv_sem=rsem,
                                            device_id={'tp': dev}, device_id_type=MESH)

    def rows8(start, n):
        return pl.ds(pl.multiple_of(start, 8), n)

    def valid(k, limit):
        return (k >= 0) & (k < limit)

    def e_copy(k):
        return pltpu.make_async_copy(embed.at[rows8(k * chunk, chunk)], ebuf.at[lax.rem(k, 2)], e_sem.at[lax.rem(k, 2)])

    def l_copy(k):
        return pltpu.make_async_copy(logits.at[rows8(k * chunk, chunk)], lbuf.at[lax.rem(k, 2)], l_sem.at[lax.rem(k, 2)])

    def gs_copy(k):
        b = lax.rem(k, 2)
        return pltpu.make_async_copy(gz_t.at[b], gsave.at[k], gs_sem.at[b])

    def gl_copy(k):
        return pltpu.make_async_copy(gsave.at[k], gt, gl_sem.at[0])

    def own_copy(k):
        return pltpu.make_async_copy(gbuf.at[rows8(core * half, half)], own.at[k], own_sem.at[0])

    def d2d_copy(k):
        return rdma(gbuf.at[rows8((1 - core) * half, half)], d2d.at[k], d2d_s.at[0], d2d_r.at[k], partner)

    def rs1_copy(k):
        n1, _, a1, _ = place(k)
        b, r = lax.rem(k, RING), lax.rem(k, SLOTS)
        return rdma(s1.at[b, rows8((1 - a1) * quarter, quarter)], rs1.at[r], rs1_s.at[b], rs1_r.at[r], n1)

    def rs2_copy(k):
        _, n2, _, a2 = place(k)
        b, r = lax.rem(k, RING), lax.rem(k, SLOTS)
        return rdma(s2.at[b, rows8((1 - a2) * eighth, eighth)], rs2.at[r], rs2_s.at[b], rs2_r.at[r], n2)

    def fin_copies(k):
        n1, n2, a1, a2 = place(k)
        b = lax.rem(k, RING)
        dst = out.at[rows8(k * chunk + core * half + a1 * quarter + a2 * eighth, eighth)]
        src = fin.at[b]
        return (pltpu.make_async_copy(src, dst, fin_s.at[0, b]),
                rdma(src, dst, fin_s.at[1, b], ag1_r.at[k], n2),
                rdma(src, dst, fin_s.at[2, b], ag2_r.at[0, k], n1),
                rdma(src, dst, fin_s.at[3, b], part_r.at[0, k], partner))

    def fwd_copies(k):
        n1, _, a1, a2 = place(k)
        b = lax.rem(k, RING)
        ref = out.at[rows8(k * chunk + core * half + a1 * quarter + (1 - a2) * eighth, eighth)]
        return (rdma(ref, ref, fwd_s.at[0, b], ag2_r.at[1, k], n1),
                rdma(ref, ref, fwd_s.at[1, b], part_r.at[1, k], partner))

    def last_copy(k):
        _, _, a1, _ = place(k)
        ref = out.at[rows8(k * chunk + core * half + (1 - a1) * quarter, quarter)]
        return rdma(ref, ref, fwd_s.at[2, lax.rem(k, RING)], part_r.at[2, k], partner)

    def peer(i, n, me):
        return lax.rem(me + i, n)

    def st_copy(i, src_of):
        return zdma(st_in.at[z], st_in.at[src_of], st_s.at[i - 1], st_r.at[src_of], peer(i, ntp, z))

    def tile_copy(buf, ssem, rsem, i, src_of):
        return rdma(buf.at[dp], buf.at[src_of], ssem.at[i - 1], rsem.at[src_of], peer(i, ndp, dp))

    def share_start():
        st_in[z] = stats[...]
        for i in range(1, ntp):
            st_copy(i, z).start()
        cnt_in[dp] = jnp.broadcast_to(jnp.sum(jnp.sum(mask[...], axis=0), axis=-1, keepdims=True), (8, 128))
        for i in range(1, ndp):
            tile_copy(cnt_in, cnt_s, cnt_r, i, dp).start()

    def in_order_sum(buf):
        total = buf[0]
        for i in range(1, ndp):
            total = total + buf[i]
        return total[0:1, 0:1]

    def share_use():
        for i in range(1, ndp):
            tile_copy(cnt_in, cnt_s, cnt_r, i, peer(i, ndp, dp)).wait_recv()
        for i in range(1, ntp):
            st_copy(i, peer(i, ntp, z)).wait_recv()
        count = in_order_sum(cnt_in)
        part = jnp.zeros((1, tile), F32)
        for j in range(tiles):
            shard = [st_in[q, j] for q in range(ntp)]
            top = functools.reduce(jnp.maximum, [a[0:1] for a in shard])
            total = functools.reduce(jnp.add, [jnp.exp(a[0:1] - top) for a in shard])
            lse_j = top + jnp.log(total)
            lse[j] = lse_j
            wgt[j] = mask[j] / count
            part = part + mask[j] * (lse_j - functools.reduce(jnp.add, [a[1:2] for a in shard]))
        loss_in[dp] = jnp.broadcast_to(jnp.sum(part, axis=-1, keepdims=True), (8, 128))
        for i in range(1, ndp):
            tile_copy(loss_in, loss_s, loss_r, i, dp).start()

    def share_end():
        for i in range(1, ndp):
            tile_copy(loss_in, loss_s, loss_r, i, peer(i, ndp, dp)).wait_recv()
        loss[...] = jnp.broadcast_to(in_order_sum(loss_in) / in_order_sum(cnt_in), (8, 128))
        for i in range(1, ndp):
            tile_copy(cnt_in, cnt_s, cnt_r, i, dp).wait_send()
            tile_copy(loss_in, loss_s, loss_r, i, dp).wait_send()
        for i in range(1, ntp):
            st_copy(i, z).wait_send()

    zb_copy = pltpu.make_async_copy(zb_hbm, zb, zb_sem.at[0])

    def s_copy(k):
        return pltpu.make_async_copy(scatter.at[rows8(k * chunk, chunk)], sbuf, s_sem.at[0])

    def z_product(u):
        k, j = lax.div(u, tiles), lax.rem(u, tiles)
        cols = pl.ds(pl.multiple_of(j * tile, tile), tile)
        acc[cols, :] += jnp.dot(gtile[lax.rem(u, 2)], ebuf[lax.rem(k, 2)], preferred_element_type=F32)

    def z_unit(u, carry):
        k, j = lax.div(u, tiles), lax.rem(u, tiles)
        slot = lax.rem(k, 2)

        @pl.when(j == 0)
        def _():
            e_copy(k).wait()
            l_copy(k).wait()

            @pl.when(k >= 2)
            def _():
                gs_copy(k - 1).wait()
        z_product(jnp.maximum(u - 1, 0) + jnp.where(u == 0, 1, 0))
        cols = pl.ds(pl.multiple_of(j * tile, tile), tile)
        ids = lax.broadcasted_iota(jnp.int32, (chunk, tile), 0) + k * chunk
        hit = jnp.where(ids == lab[j], 1.0, 0.0)
        g = ((jnp.exp(lbuf[slot, :, cols] - lse[j]) - hit) * wgt[j]).astype(BF16)
        gz_t[slot, :, cols] = g
        gtile[lax.rem(u, 2)] = g.T

        @pl.when((j == 0) & (k + 1 < nc))
        def _():
            e_copy(k + 1).start()
            l_copy(k + 1).start()

        @pl.when(j == tiles - 1)
        def _():
            gs_copy(k).start()

            @pl.when((k == 0) | (k == nc - 1))
            def _():
                gs_copy(k).wait()

        @pl.when(u == nc * tiles - 1)
        def _():
            z_product(u)
        return carry

    def g_unit(u, carry):
        k, n = lax.div(u, ntiles), lax.rem(u, ntiles)

        @pl.when(n == 0)
        def _():
            gl_copy(k).start()

            @pl.when(k >= 1)
            def _():
                d2d_copy(k - 1).wait_send()
            s_copy(k).wait()

            @pl.when(k == 0)
            def _():
                zb_copy.wait()
            gl_copy(k).wait()
        cols = pl.ds(pl.multiple_of(n * ntile, ntile), ntile)
        gbuf[:, cols] = sbuf[:, cols] + jnp.dot(gt[...], zb[:, cols], preferred_element_type=F32)

        @pl.when(n == ntiles - 1)
        def _():
            own_copy(k).start()
            d2d_copy(k).start()

            @pl.when(k + 1 < nc)
            def _():
                s_copy(k + 1).start()

            @pl.when(k == nc - 1)
            def _():
                d2d_copy(k).wait_send()
        return carry

    def load_start(k):
        own_copy(k).wait()
        d2d_copy(k).wait_recv()
        pltpu.make_async_copy(own.at[k], ld_own, ld_sem.at[0]).start()
        pltpu.make_async_copy(d2d.at[k], ld_d2d, ld_sem.at[1]).start()

    def stage_a(k):
        pltpu.make_async_copy(own.at[k], ld_own, ld_sem.at[0]).wait()
        pltpu.make_async_copy(d2d.at[k], ld_d2d, ld_sem.at[1]).wait()

        @pl.when(k >= RING)
        def _():
            rs1_copy(k - RING).wait_send()
        b = lax.rem(k, RING)

        def add(i, c):
            r = rows8(i * eighth, eighth)
            s1[b, r, :] = ld_own[r, :] + ld_d2d[r, :]
            return c
        lax.fori_loop(0, half // eighth, add, 0)
        rs1_copy(k).start()

    def stage_b(k):
        _, _, a1, _ = place(k)
        rs1_copy(k).wait_recv()

        @pl.when(k >= RING)
        def _():
            rs2_copy(k - RING).wait_send()
        b, r = lax.rem(k, RING), lax.rem(k, SLOTS)

        def add(i, c):
            s2[b, rows8(i * eighth, eighth), :] = (s1[b, rows8(a1 * quarter + i * eighth, eighth), :]
                                                   + rs1[r, rows8(i * eighth, eighth), :])
            return c
        lax.fori_loop(0, quarter // eighth, add, 0)
        rs2_copy(k).start()

    def stage_c(k):
        _, _, _, a2 = place(k)
        rs2_copy(k).wait_recv()

        @pl.when(k >= RING)
        def _():
            for i, c in enumerate(fin_copies(k - RING)):
                c.wait() if i == 0 else c.wait_send()
        b, r = lax.rem(k, RING), lax.rem(k, SLOTS)
        fin[b] = s2[b, rows8(a2 * eighth, eighth), :] + rs2[r]
        for c in fin_copies(k):
            c.start()

    def stage_d(k):
        fin_copies(k)[1].wait_recv()

        @pl.when(k >= RING)
        def _():
            for c in fwd_copies(k - RING):
                c.wait_send()
        for c in fwd_copies(k):
            c.start()

    def stage_w(k):
        fin_copies(k)[2].wait_recv()

    def stage_e(k):
        fwd_copies(k)[0].wait_recv()

        @pl.when(k >= RING)
        def _():
            last_copy(k - RING).wait_send()
        last_copy(k).start()

    def stage_f(k):
        fin_copies(k)[3].wait_recv()
        fwd_copies(k)[1].wait_recv()
        last_copy(k).wait_recv()

    nb = tokens // ntp // zrows
    qrows = tokens // ntp

    def zacc(q, b):
        return pl.multiple_of(q * qrows + b * zrows, 8)

    def right_copy(b, i, src=None):
        n = ntp - 1 - i
        s = zout_r.at[lax.rem(b, RING), pl.ds(i, n)] if src is None else src
        return zdma(s, rs_r.at[b, pl.ds(i, n)], zrs_sr.at[lax.rem(b, RING)], zrs_rr.at[b], i + 1)

    def left_copy(b, i):
        return zdma(zout_l.at[lax.rem(b, RING), pl.ds(0, i)], rs_l.at[b, pl.ds(0, i)], zrs_sl.at[lax.rem(b, RING)],
                    zrs_rl.at[b], i - 1)

    def right_load(b, i):
        n = ntp - 1 - i
        return pltpu.make_async_copy(rs_r.at[b, pl.ds(i, n)], zin_r.at[pl.ds(i, n)], zld.at[0])

    def left_load(b, i):
        return pltpu.make_async_copy(rs_l.at[b, pl.ds(0, i)], zin_l.at[pl.ds(0, i)], zld.at[1])

    def final_loads(b, i):
        loads = [pltpu.make_async_copy(hidden.at[rows8(z * qrows + b * zrows, zrows)], hbuf, h_sem.at[0])]
        if i > 0:
            loads.append(pltpu.make_async_copy(rs_r.at[b, i - 1], zfin_r, zld.at[2]))
        if i < ntp - 1:
            loads.append(pltpu.make_async_copy(rs_l.at[b, i], zfin_l, zld.at[3]))
        return loads

    def z_right_head(b):
        for i in range(1, ntp - 1):
            @pl.when(z == i)
            def _(i=i):
                right_copy(b, i - 1).wait_recv()
                right_load(b, i).start()

    def z_left_head(b):
        for i in range(1, ntp - 1):
            @pl.when(z == i)
            def _(i=i):
                left_copy(b, i + 1).wait_recv()
                left_load(b, i).start()

    def z_final_head(b):
        for i in range(ntp):
            @pl.when(z == i)
            def _(i=i):
                if i == ntp - 1:
                    right_copy(b, i - 1).wait_recv()
                if i == 0:
                    left_copy(b, i + 1).wait_recv()
                for c in final_loads(b, i):
                    c.start()

    def z_right(b):
        for i in range(ntp - 1):
            @pl.when(z == i)
            def _(i=i):
                n = ntp - 1 - i
                if i > 0:
                    right_load(b, i).wait()

                @pl.when(b >= RING)
                def _():
                    right_copy(b - RING, i).wait_send()
                for q in range(i + 1, ntp):
                    mine = acc[pl.ds(zacc(q, b), zrows), :]
                    zout_r[lax.rem(b, RING), q - 1] = mine if i == 0 else zin_r[q - 1] + mine
                right_copy(b, i).start()

    def z_left(b):
        for i in range(1, ntp):
            @pl.when(z == i)
            def _(i=i):
                if i < ntp - 1:
                    left_load(b, i).wait()

                @pl.when(b >= RING)
                def _():
                    left_copy(b - RING, i).wait_send()
                for q in range(i):
                    mine = acc[pl.ds(zacc(q, b), zrows), :]
                    zout_l[lax.rem(b, RING), q] = mine if i == ntp - 1 else zin_l[q] + mine
                left_copy(b, i).start()

    def zfin_copies(b):
        s = lax.rem(b, RING)
        dst = gz.at[rows8(z * qrows + b * zrows, zrows)]
        return (pltpu.make_async_copy(zfin.at[s], dst, zfin_s.at[0, s]),
                zdma(zfin.at[s], dst, zfin_s.at[1, s], zag_rr.at[b, 0], z + 1),
                zdma(zfin.at[s], dst, zfin_s.at[2, s], zag_rl.at[b, 0], z - 1))

    def z_final(b):
        for i in range(ntp):
            @pl.when(z == i)
            def _(i=i):
                for c in final_loads(b, i):
                    c.wait()
                z_wait_fin(b - RING, b >= RING)
                total = acc[pl.ds(zacc(i, b), zrows), :]
                if i > 0:
                    total = zfin_r[...] + total
                if i < ntp - 1:
                    total = total + zfin_l[...]
                zfin[lax.rem(b, RING)] = total
        h = hbuf[...].astype(F32)
        centered = h - jnp.mean(h, axis=-1, keepdims=True)
        rstd = lax.rsqrt(jnp.mean(centered * centered, axis=-1, keepdims=True) + 1e-5)
        unit = centered * rstd
        dy = zfin[lax.rem(b, RING)] * affine[0:1, :]
        zfin[lax.rem(b, RING)] = rstd * (dy - jnp.mean(dy, axis=-1, keepdims=True)
                                         - unit * jnp.mean(dy * unit, axis=-1, keepdims=True))
        copies = zfin_copies(b)
        copies[0].start()

        @pl.when(z < ntp - 1)
        def _():
            copies[1].start()

        @pl.when(z > 0)
        def _():
            copies[2].start()

    def z_wait_fin(b, cond):
        @pl.when(cond)
        def _():
            copies = zfin_copies(b)
            copies[0].wait()

            @pl.when(z < ntp - 1)
            def _():
                copies[1].wait_send()

            @pl.when(z > 0)
            def _():
                copies[2].wait_send()

    def zag(b, h, sign, ssem, rsem):
        ref = gz.at[rows8((z - sign * h) * qrows + b * zrows, zrows)]
        return zdma(ref, ref, ssem.at[b, h - 1], rsem.at[b, h], z + sign)

    def z_hop(b, h):
        ref_r = gz.at[rows8((z - h) * qrows + b * zrows, zrows)]
        ref_l = gz.at[rows8((z + h) * qrows + b * zrows, zrows)]

        @pl.when(z >= h)
        def _():
            zdma(ref_r, ref_r, zfw_r.at[b, 0], zag_rr.at[b, h - 1], z).wait_recv()
            if h < ntp - 1:
                @pl.when(z < ntp - 1)
                def _():
                    zag(b, h, 1, zfw_r, zag_rr).start()

        @pl.when(z + h <= ntp - 1)
        def _():
            zdma(ref_l, ref_l, zfw_l.at[b, 0], zag_rl.at[b, h - 1], z).wait_recv()
            if h < ntp - 1:
                @pl.when(z > 0)
                def _():
                    zag(b, h, -1, zfw_l, zag_rl).start()

    lead, g_first = 18, STEPS
    nz, ng = nc * tiles, nc * ntiles
    fast = tiles * 13 // 7

    def uz(i):
        late = jnp.maximum(i - 1 - lead, 0)
        count = tiles + 1 + lax.div(jnp.minimum(i - 1, lead) * tiles + late * fast, STEPS)
        return jnp.where(i <= 0, 0, jnp.minimum(count, nz))

    def ug(i):
        return jnp.where(i <= 0, 0, jnp.minimum(ntiles + lax.div(jnp.maximum(i - g_first, 0) * ntiles, STEPS), ng))

    lags = (('w', 13, 11), ('f', 25, 20), ('c', 9, 7), ('b', 6, 4), ('d', 12, 10), ('e', 17, 15), ('p', 1, 0), ('a', 2, 1))
    stages = {'w': stage_w, 'f': stage_f, 'e': stage_e, 'd': stage_d, 'c': stage_c, 'b': stage_b, 'a': stage_a,
              'p': load_start}
    z_start = lead + -(-max(nz - (tiles + 1 + lead * tiles // STEPS), 0) * STEPS // fast)
    hop = 3
    steps = max((nc - 1) * STEPS + 27, z_start + nb + hop * 2 * (ntp - 1))
    share_start()
    zb_copy.start()
    e_copy(0).start()
    l_copy(0).start()

    gtile[...] = jnp.zeros_like(gtile)
    s_copy(0).start()

    def clear(j, carry):
        acc[pl.ds(pl.multiple_of(j * tile, tile), tile), :] = jnp.zeros((tile, d), F32)
        return carry
    lax.fori_loop(0, tiles, clear, 0)
    share_use()

    def one_step(i, carry):
        zt = i - z_start
        right_b, left_b, final_b = zt - hop * z, zt - hop * (ntp - 1 - z), zt - hop * (ntp - 1)

        def z_stages(*stage_of):
            for b, stage in zip((right_b, left_b, final_b), stage_of):
                @pl.when(valid(b, nb))
                def _(b=b, stage=stage):
                    stage(b)
        z_stages(z_right_head, z_left_head, z_final_head)
        lax.fori_loop(uz(i), uz(i + 1), z_unit, 0)
        lax.fori_loop(ug(i), ug(i + 1), g_unit, 0)
        for name, lag, first in lags:
            later = (i - lag >= STEPS) & (i - lag < nc * STEPS) & (lax.rem(i - lag + STEPS * 64, STEPS) == 0)

            @pl.when(later | (i == first))
            def _(name=name, lag=lag, first=first):
                stages[name](jnp.where(i == first, 0, lax.div(i - lag, STEPS)))
        z_stages(z_right, z_left, z_final)
        for h in range(1, ntp):
            @pl.when(valid(zt - hop * (ntp - 1 + h), nb))
            def _(h=h):
                z_hop(zt - hop * (ntp - 1 + h), h)
        return carry
    lax.fori_loop(0, steps, one_step, 0)

    share_end()

    for k in range(max(nc - RING, 0), nc):
        rs1_copy(k).wait_send()
        rs2_copy(k).wait_send()
        for i, c in enumerate(fin_copies(k)):
            c.wait() if i == 0 else c.wait_send()
        for c in fwd_copies(k):
            c.wait_send()
        last_copy(k).wait_send()
    for b in range(max(nb - RING, 0), nb):
        for i in range(ntp - 1):
            @pl.when(z == i)
            def _(i=i, b=b):
                right_copy(b, i).wait_send()
        for i in range(1, ntp):
            @pl.when(z == i)
            def _(i=i, b=b):
                left_copy(b, i).wait_send()
        z_wait_fin(b, z >= 0)

    def drain(b, carry):
        for h in range(1, ntp - 1):
            @pl.when((z >= h) & (z < ntp - 1))
            def _(h=h):
                zag(b, h, 1, zfw_r, zag_rr).wait_send()

            @pl.when((z + h <= ntp - 1) & (z > 0))
            def _(h=h):
                zag(b, h, -1, zfw_l, zag_rl).wait_send()
        return carry
    lax.fori_loop(0, nb, drain, 0)


def gradients(ntp, ndp, zb, stats, mask, lab, affine, hidden, embed, logits, scatter, chunk, tile, zrows):
    tokens, d = zb.shape
    vocab_loc = embed.shape[0]
    nc = vocab_loc // chunk
    half, quarter, eighth = chunk // 2, chunk // 4, chunk // 8
    tiles = tokens // tile
    nb = tokens // ntp // zrows
    vm = pl.BlockSpec(memory_space=pltpu.VMEM)
    hbm = pl.BlockSpec(memory_space=pl.ANY)
    dma = lambda *s: pltpu.SemaphoreType.DMA(s)
    vf = lambda *s: pltpu.VMEM(s, F32)
    sds = lambda *s: jax.ShapeDtypeStruct(s, F32)
    rows = lambda a: a.reshape(tiles, 1, tile)
    res = pl.pallas_call(
        functools.partial(grad_kernel, ntp, ndp, chunk, tile, zrows),
        out_shape=(sds(vocab_loc, d), sds(8, 128), sds(tokens, d), sds(nc, half, d), sds(nc, half, d),
                   sds(nb, ntp - 1, zrows, d), sds(nb, ntp - 1, zrows, d), jax.ShapeDtypeStruct((nc, chunk, tokens), BF16)),
        in_specs=[vm] * 4 + [hbm] * 5,
        out_specs=(hbm, vm) + (hbm,) * 6,
        scratch_shapes=[
            pltpu.VMEM((tokens, d), BF16), vf(tiles, 1, tile), vf(tiles, 1, tile), vf(ntp, tiles, 8, tile), vf(ndp, 8, 128), vf(ndp, 8, 128),
            vf(2, chunk, tokens),
            pltpu.VMEM((2, chunk, d), BF16), pltpu.VMEM((2, chunk, tokens), BF16), pltpu.VMEM((2, tile, chunk), BF16),
            pltpu.VMEM((zrows, d), BF16), pltpu.VMEM((chunk, tokens), BF16), vf(chunk, d),
            vf(tokens, d), vf(chunk, d), vf(half, d), vf(half, d),
            vf(RING, half, d), vf(RING, quarter, d), vf(RING, eighth, d), vf(SLOTS, quarter, d), vf(SLOTS, eighth, d),
            vf(ntp - 1, zrows, d), vf(ntp - 1, zrows, d), vf(zrows, d), vf(zrows, d), vf(RING, ntp - 1, zrows, d), vf(RING, ntp - 1, zrows, d),
            vf(RING, zrows, d),
            dma(ntp - 1), dma(ntp), dma(ndp - 1), dma(ndp), dma(ndp - 1), dma(ndp), dma(1), dma(2),
            dma(2), dma(2), dma(1), dma(1), dma(1), dma(1), dma(1), dma(nc), dma(2), dma(RING), dma(SLOTS), dma(RING), dma(SLOTS), dma(4, RING),
            dma(nc), dma(2, nc), dma(3, RING), dma(3, nc),
            dma(4), dma(RING), dma(RING), dma(nb), dma(nb), dma(3, RING), dma(nb, ntp - 1), dma(nb, ntp - 1),
            dma(nb, ntp - 1), dma(nb, ntp - 1),
        ],
        compiler_params=pltpu.CompilerParams(vmem_limit_bytes=VMEM_LIMIT, has_side_effects=True),
        cost_estimate=pl.CostEstimate(flops=4 * tokens * d * vocab_loc, bytes_accessed=4 * vocab_loc * (4 * d + tokens),
                                      transcendentals=tokens * vocab_loc),
        name='gradients',
    )(stats, rows(mask), rows(lab), affine, zb, hidden, embed, logits, scatter)
    return res[:3]


def finish_kernel(grads, rows, gh_in, pos_table, grad_out, embed_out, gh_out, ring, in_sem, out_sem):
    i, n = pl.program_id(0), pl.num_programs(0)
    slots, size = ring.shape[0], ring.shape[1]
    ahead = slots - 2

    def block(k):
        return pl.ds(pl.multiple_of(k * size, 8), size)

    def take(k):
        return pltpu.make_async_copy(grads.at[block(k)], ring.at[lax.rem(k, slots)], in_sem.at[lax.rem(k, slots)])

    def give(k):
        return pltpu.make_async_copy(ring.at[lax.rem(k, slots)], grad_out.at[block(k)], out_sem.at[lax.rem(k, slots)])

    @pl.when(i == 0)
    def _():
        def first(k, carry):
            take(k).start()
            return carry
        lax.fori_loop(0, jnp.minimum(ahead, n), first, 0)

    @pl.when(i >= 2)
    def _():
        give(i - 2).wait()

    @pl.when(i + ahead < n)
    def _():
        take(i + ahead).start()
    take(i).wait()
    give(i).start()
    embed_out[...] = (rows[...] + pos_table[...].astype(F32)).astype(BF16)
    gh_out[...] = gh_in[...].astype(BF16)

    @pl.when(i == n - 1)
    def _():
        @pl.when(i >= 1)
        def _():
            give(i - 1).wait()
        give(i).wait()


def finish(grads, rows, grad_h, pos_table, vocab_loc):
    tokens, d = grad_h.shape
    ctx = pos_table.shape[0]
    n = tokens // 64
    big, mid = vocab_loc // n, 64
    at = lambda r, f=lambda i: i: pl.BlockSpec((r, d), lambda i: (f(i), 0))
    return pl.pallas_call(
        finish_kernel,
        grid=(n,),
        in_specs=[pl.BlockSpec(memory_space=pl.ANY), at(mid), at(mid), at(mid, lambda i: lax.rem(i, ctx // mid))],
        out_specs=(pl.BlockSpec(memory_space=pl.ANY), at(mid), at(mid)),
        scratch_shapes=[pltpu.VMEM((8, big, d), F32), pltpu.SemaphoreType.DMA((8,)), pltpu.SemaphoreType.DMA((8,))],
        out_shape=(jax.ShapeDtypeStruct((vocab_loc, d), F32),
                   jax.ShapeDtypeStruct((tokens, d), BF16), jax.ShapeDtypeStruct((tokens, d), BF16)),
        compiler_params=pltpu.CompilerParams(vmem_limit_bytes=VMEM_LIMIT),
        cost_estimate=pl.CostEstimate(flops=tokens * d, bytes_accessed=8 * vocab_loc * d, transcendentals=0),
        name='finish',
    )(grads, rows, grad_h, pos_table)


def solution(mesh):
    ntp, ndp = mesh.shape['tp'], mesh.shape['dp']

    def device_fn(tokens, labels, lossmask, hidden, grad_x0, embed_loc, pos_table, ln_gain, ln_bias):
        vocab_loc, d = embed_loc.shape
        batch, ctx = tokens.shape
        ntok = batch * ctx
        chunk1, chunk, tile, zrows = sizes(ntok, vocab_loc)
        shard_start = lax.axis_index('tp') * vocab_loc
        tok_local = (tokens - shard_start).reshape(1, ntok)
        lab_local = (labels - shard_start).reshape(1, ntok)
        tok_here = (tok_local >= 0) & (tok_local < vocab_loc)
        hidden2, pos_part = lax.optimization_barrier((hidden.reshape(ntok, d), jnp.sum(grad_x0.astype(F32), axis=0)))
        grad_pos = lax.psum(pos_part, 'dp')
        affine = jnp.stack([ln_gain, ln_bias])
        zb, stats, logits, rows, scatter = token_stats(hidden2, affine, lab_local, tok_local, tok_here,
                                                            grad_x0.reshape(ntok, d), embed_loc, chunk1, tile)
        rows, grad_pos = lax.optimization_barrier((rows, grad_pos))
        rows = lax.psum(rows, 'tp')
        grads, loss, grad_h = gradients(ntp, ndp, zb, stats, lossmask.astype(F32), lab_local, affine, hidden2, embed_loc,
                                        logits, scatter, chunk, tile, zrows)
        grad_embed, embed_out, grad_hidden = finish(grads, rows, grad_h, pos_table, vocab_loc)
        mean_loss = loss[0, 0]
        embed_out = embed_out.reshape(batch, ctx, d)
        grad_hidden = grad_hidden.reshape(batch, ctx, d)
        return mean_loss, embed_out, grad_hidden, grad_embed, grad_pos

    row_spec = P('dp', None)
    act_spec = P('dp', None, None)
    return jax.shard_map(device_fn, mesh=mesh, in_specs=(row_spec, row_spec, row_spec, act_spec, act_spec, P('tp', None), P(None, None), P(None), P(None)), out_specs=(P(), act_spec, act_spec, P('tp', None), P(None, None)), check_vma=False)
```
